8 devices in a mesh: q: 8 (over z, y, x, core).
Axes of the slice: x: 2, y: 2, z: 1, core: 2. Of those that a mesh axis runs over, the one named last changes fastest.
Arguments:
- state_in: float32 [2, 1048576], P(None, 'q')
- unitaries: float32 [2, 20, 2, 2], replicated
- cz_pairs: int32 [10, 2], replicated
Outputs:
- output 1: float32 [2, 1048576], P(None, 'q')
- output 2: float32 [20], replicated
All inputs are finite; a program needn't handle non-finite values.
Results may differ from the reference program's by a relative error of at most 0.001.
Values sent between devices are 32-bit elements.
A program may use at most 1 GiB of HBM per device.

```python
import math
import jax
import jax.numpy as jnp
from jax import lax

QUBITS = 20
NUM_PAIRS = QUBITS // 2
STATE_SIZE = 2 ** QUBITS


def u3_gates(theta_angle, phi_angle, lam_angle):
    cos_half = jnp.cos(0.5 * theta_angle)
    sin_half = jnp.sin(0.5 * theta_angle)
    zero_part = jnp.zeros_like(cos_half)
    real_part = jnp.stack([
        jnp.stack([cos_half, -jnp.cos(lam_angle) * sin_half], axis=-1),
        jnp.stack([jnp.cos(phi_angle) * sin_half, jnp.cos(phi_angle + lam_angle) * cos_half], axis=-1)], axis=-2)
    imag_part = jnp.stack([
        jnp.stack([zero_part, -jnp.sin(lam_angle) * sin_half], axis=-1),
        jnp.stack([jnp.sin(phi_angle) * sin_half, jnp.sin(phi_angle + lam_angle) * cos_half], axis=-1)], axis=-2)
    return jnp.stack([real_part, imag_part])


def product_envelope(zero_weight, env_angle):
    env_re = jnp.ones((1,), jnp.float32)
    env_im = jnp.zeros((1,), jnp.float32)
    for qubit_pos in range(QUBITS):
        amp_zero = jnp.sqrt(2.0 * zero_weight[qubit_pos])
        amp_one = jnp.sqrt(2.0 * (1.0 - zero_weight[qubit_pos]))
        fac_re = jnp.stack([amp_zero, amp_one * jnp.cos(env_angle[qubit_pos])])
        fac_im = jnp.stack([jnp.zeros_like(amp_zero), amp_one * jnp.sin(env_angle[qubit_pos])])
        next_re = (env_re[:, None] * fac_re[None, :] - env_im[:, None] * fac_im[None, :]).reshape(-1)
        next_im = (env_re[:, None] * fac_im[None, :] + env_im[:, None] * fac_re[None, :]).reshape(-1)
        env_re = next_re
        env_im = next_im
    return env_re, env_im


def setup_inputs(seed: int = 0) -> dict:
    root_key = jax.random.key(seed)
    key_amp, key_bias, key_theta, key_phase, key_pairs, key_env = jax.random.split(root_key, 6)
    zero_weight = jax.random.uniform(key_bias, (QUBITS,), jnp.float32, 0.15, 0.85)
    env_angle = jax.random.uniform(key_env, (QUBITS,), jnp.float32, 0.0, 2.0 * math.pi)
    env_re, env_im = product_envelope(zero_weight, env_angle)
    noise = 0.6 * jax.random.normal(key_amp, (2, STATE_SIZE), jnp.float32)
    base_re = 1.0 + noise[0]
    base_im = noise[1]
    amplitudes = jnp.stack([env_re * base_re - env_im * base_im, env_re * base_im + env_im * base_re])
    amplitudes = amplitudes * lax.rsqrt(jnp.mean(jnp.sum(amplitudes * amplitudes, axis=0)))
    theta_angle = jax.random.uniform(key_theta, (QUBITS,), jnp.float32, 0.35 * math.pi, 0.65 * math.pi)
    phase_angle = jax.random.uniform(key_phase, (2, QUBITS), jnp.float32, 0.0, 2.0 * math.pi)
    unitaries = u3_gates(theta_angle, phase_angle[0], phase_angle[1])
    cz_pairs = jax.random.permutation(key_pairs, QUBITS)[: 2 * NUM_PAIRS].reshape(NUM_PAIRS, 2).astype(jnp.int32)
    return {'state_in': amplitudes, 'unitaries': unitaries, 'cz_pairs': cz_pairs}


def mix_pair(first, second, coef_a, coef_b):
    out_re = coef_a[0] * first[0] - coef_a[1] * first[1] + coef_b[0] * second[0] - coef_b[1] * second[1]
    out_im = coef_a[0] * first[1] + coef_a[1] * first[0] + coef_b[0] * second[1] + coef_b[1] * second[0]
    return jnp.stack([out_re, out_im])


def apply_gate(state, bit_pos, gate_mat):
    view = state.reshape(2, 2 ** bit_pos, 2, -1)
    zero_half = view[:, :, 0, :]
    one_half = view[:, :, 1, :]
    new_zero = mix_pair(zero_half, one_half, gate_mat[:, 0, 0], gate_mat[:, 0, 1])
    new_one = mix_pair(zero_half, one_half, gate_mat[:, 1, 0], gate_mat[:, 1, 1])
    return jnp.stack([new_zero, new_one], axis=2).reshape(state.shape)


def pair_signs(flat_index, cz_pairs):
    parity = jnp.zeros_like(flat_index)
    for pair_pos in range(NUM_PAIRS):
        shift_a = QUBITS - 1 - cz_pairs[pair_pos, 0]
        shift_b = QUBITS - 1 - cz_pairs[pair_pos, 1]
        parity = parity ^ ((flat_index >> shift_a) & (flat_index >> shift_b) & 1)
    return (1 - 2 * parity).astype(jnp.float32)


def reference(state_in, unitaries, cz_pairs):
    state = state_in
    for qubit_pos in range(QUBITS):
        state = apply_gate(state, qubit_pos, unitaries[:, qubit_pos])
    flat_index = lax.iota(jnp.int32, STATE_SIZE)
    state = state * pair_signs(flat_index, cz_pairs)[None, :]
    density = state[0] * state[0] + state[1] * state[1]
    halves = [jnp.sum(density.reshape(2 ** qubit_pos, 2, -1), axis=(0, 2)) for qubit_pos in range(QUBITS)]
    z_expect = jnp.stack([bit_sums[0] - bit_sums[1] for bit_sums in halves]) / STATE_SIZE
    return state, z_expect
```

```python
import jax
import jax.numpy as jnp
from jax import lax
from jax.experimental import pallas as pl
from jax.experimental.pallas import tpu as pltpu
from jax.sharding import PartitionSpec as P

MESH = pl.DeviceIdType.MESH
F32 = jnp.float32
ROWS = 128
CHUNK = 2 * ROWS
CHUNKS = 4
PIECES = 4
PROWS = ROWS // PIECES
DEVICES = 8


def cmul2(coef_a, first, coef_b, second):
    re = coef_a[0] * first[0] - coef_a[1] * first[1] + coef_b[0] * second[0] - coef_b[1] * second[1]
    im = coef_a[0] * first[1] + coef_a[1] * first[0] + coef_b[0] * second[1] + coef_b[1] * second[0]
    return re, im


def kernel(X, u_ref, cz_ref, OUT, z_ref,
           RB, XP, RP, S, R2, T, SG, GM, KM, XC, ZC, TP, V, VR,
           s1s, s1r, cps, cpr, fws, fwr, s2s, s2r, zs, zr):
    me = lax.axis_index('q')
    bit_y = me // 4
    bit_x = (me // 2) % 2
    bit_c = me % 2
    dev_y = me + 4 * (1 - 2 * bit_y)
    dev_x = me + 2 * (1 - 2 * bit_x)
    dev_c = me + (1 - 2 * bit_c)
    first_dev = (dev_x, dev_y)
    second_dev = (dev_y, dev_x)

    def remote(src, dst, send, recv, dev):
        return pltpu.make_async_remote_copy(src_ref=src, dst_ref=dst, send_sem=send, recv_sem=recv,
                                            device_id=(dev,), device_id_type=MESH)

    def stage1(half, chunk):
        k = half * CHUNKS + chunk
        rows = pl.ds(k * CHUNK, CHUNK)
        return remote(X.at[rows], RB.at[rows], s1s.at[k], s1r.at[k], first_dev[half])

    def core_copy(half, chunk):
        k = half * CHUNKS + chunk
        rows = pl.ds(k * CHUNK, CHUNK)
        return remote(X.at[rows], XP.at[rows], cps.at[k], cpr.at[k], dev_c)

    def forward(half, chunk):
        k = half * CHUNKS + chunk
        rows = pl.ds(k * CHUNK, CHUNK)
        return remote(RB.at[rows], RP.at[rows], fws.at[k], fwr.at[k], dev_c)

    def stage2(half, chunk, piece):
        k = (half * CHUNKS + chunk) * PIECES + piece
        rows = pl.ds(piece * PROWS, PROWS)
        return remote(S.at[half, chunk, :, rows], R2.at[half, chunk, :, rows], s2s.at[k], s2r.at[k], second_dev[half])

    barrier = pltpu.get_barrier_semaphore()
    for dev in (dev_x, dev_y, dev_c):
        pl.semaphore_signal(barrier, inc=1, device_id=(dev,), device_id_type=MESH)
    pl.semaphore_wait(barrier, 3)

    for chunk in range(CHUNKS):
        for half in range(2):
            stage1(half, chunk).start()
    for chunk in range(CHUNKS):
        for half in range(2):
            core_copy(half, chunk).start()

    def entry(qubit, row, col):
        return u_ref[row * 2 + col, qubit], u_ref[4 + row * 2 + col, qubit]

    lane = lax.broadcasted_iota(jnp.int32, (8, 128), 1)
    sub = lax.broadcasted_iota(jnp.int32, (8, 128), 0)

    def build(t, carry):
        row = sub + 8 * t
        for base, left in ((6, True), (13, False)):
            re = im = None
            for j in range(7):
                shift = 6 - j
                row_bit = ((row >> shift) & 1) == 1
                col_bit = ((lane >> shift) & 1) == 1
                fac = []
                for ri in range(2):
                    u00, u01, u10, u11 = [u_ref[4 * ri + k, base + j] for k in range(4)]
                    if not left:
                        u01, u10 = u10, u01
                    fac.append(jnp.where(row_bit, jnp.where(col_bit, u11, u10), jnp.where(col_bit, u01, u00)))
                if re is None:
                    re, im = fac
                else:
                    re, im = re * fac[0] - im * fac[1], re * fac[1] + im * fac[0]
            low = pl.ds(pl.multiple_of(8 * t, 8), 8)
            high = pl.ds(pl.multiple_of(128 + 8 * t, 8), 8)
            if left:
                GM[low, 0:128] = re
                GM[low, 128:256] = -im
                GM[high, 0:128] = im
                GM[high, 128:256] = re
            else:
                KM[low, 0:128] = re
                KM[low, 128:256] = im
                KM[high, 0:128] = -im
                KM[high, 128:256] = re
        return carry

    lax.fori_loop(0, 16, build, 0)

    num_pairs = cz_ref.shape[1]
    shifts = [(19 - cz_ref[0, k], 19 - cz_ref[1, k]) for k in range(num_pairs)]

    def build_signs(t, carry):
        flat = me * 131072 + (sub + 8 * t) * 128 + lane
        parity = jnp.zeros_like(flat)
        for shift_a, shift_b in shifts:
            parity = parity ^ ((flat >> shift_a) & (flat >> shift_b))
        SG[pl.ds(pl.multiple_of(8 * t, 8), 8), :] = (1 - 2 * (parity & 1)).astype(F32)
        return carry

    lax.fori_loop(0, 128, build_signs, 0)

    def gate_pair(qubit, own_bit):
        return entry(qubit, own_bit, own_bit), entry(qubit, own_bit, 1 - own_bit)

    def scalar_mul(a, b):
        return a[0] * b[0] - a[1] * b[1], a[0] * b[1] + a[1] * b[0]

    coef_y = gate_pair(0, bit_y)
    coef_x = gate_pair(1, bit_x)
    coef_c = gate_pair(2, bit_c)
    stage1_coefs = []
    for coef in (coef_x, coef_y):
        stage1_coefs.append([scalar_mul(coef[0], coef_c[0]), scalar_mul(coef[1], coef_c[0]),
                             scalar_mul(coef[0], coef_c[1]), scalar_mul(coef[1], coef_c[1])])

    for chunk in range(CHUNKS):
        for half in range(2):
            stage1(half, chunk).wait_recv()
            forward(half, chunk).start()
        if chunk:
            for piece in range(PIECES):
                for half in range(2):
                    stage2(half, chunk - 1, piece).start()
        for half in range(2):
            core_copy(half, chunk).wait_recv()
            forward(half, chunk).wait_recv()

        for half in range(2):
            coefs = stage1_coefs[half]
            base = (half * CHUNKS + chunk) * CHUNK

            def combine(t, carry, base=base, coefs=coefs, half=half):
                at = pl.multiple_of(base + 16 * t, 16)
                re = im = None
                for ref, coef in zip((X, RB, XP, RP), coefs):
                    a = ref[pl.ds(at, 8, stride=2), :]
                    b = ref[pl.ds(at + 1, 8, stride=2), :]
                    part_re = coef[0] * a - coef[1] * b
                    part_im = coef[0] * b + coef[1] * a
                    re = part_re if re is None else re + part_re
                    im = part_im if im is None else im + part_im
                XC[pl.ds(pl.multiple_of(8 * t, 8), 8), half * 128:half * 128 + 128] = re
                XC[pl.ds(pl.multiple_of(128 + 8 * t, 8), 8), half * 128:half * 128 + 128] = im
                return carry

            lax.fori_loop(0, 16, combine, 0, unroll=2)
        left = lax.dot(GM[...], XC[...], precision=lax.Precision.HIGHEST, preferred_element_type=F32)
        ZC[0:128, 0:128] = left[0:128, 0:128]
        ZC[0:128, 128:256] = left[128:256, 0:128]
        ZC[128:256, 0:128] = left[0:128, 128:256]
        ZC[128:256, 128:256] = left[128:256, 128:256]
        both = lax.dot(ZC[...], KM[...], precision=lax.Precision.HIGHEST, preferred_element_type=F32)
        S[0, chunk, 0] = both[0:128, 0:128]
        S[0, chunk, 1] = both[0:128, 128:256]
        S[1, chunk, 0] = both[128:256, 0:128]
        S[1, chunk, 1] = both[128:256, 128:256]

    u3 = [entry(3, 0, 0), entry(3, 0, 1), entry(3, 1, 0), entry(3, 1, 1)]
    u4 = [entry(4, 0, 0), entry(4, 0, 1), entry(4, 1, 0), entry(4, 1, 1)]
    u5 = [entry(5, 0, 0), entry(5, 0, 1), entry(5, 1, 0), entry(5, 1, 1)]

    def gate(mat, zero, one):
        return cmul2(mat[0], zero, mat[1], one), cmul2(mat[2], zero, mat[3], one)

    def second_gate(chunk, rows):
        def pair(ref, half):
            return ref[half, chunk, 0, rows, :], ref[half, chunk, 1, rows, :]
        zero = cmul2(coef_y[0], pair(S, 0), coef_y[1], pair(R2, 0))
        one = cmul2(coef_x[0], pair(S, 1), coef_x[1], pair(R2, 1))
        return gate(u3, zero, one)

    def read(half, chunk, rows):
        return T[half, chunk, 0, rows, :], T[half, chunk, 1, rows, :]

    def keep(half, chunk, rows, value):
        T[half, chunk, 0, rows, :] = value[0]
        T[half, chunk, 1, rows, :] = value[1]

    def piece_rows(t):
        return pl.ds(pl.multiple_of(8 * t, 8), 8)

    def step_even(chunk):
        def body(t, carry):
            rows = piece_rows(t)
            both = second_gate(chunk, rows)
            for half in range(2):
                keep(half, chunk, rows, both[half])
            return carry
        return body

    def step_odd(t, carry):
        rows = piece_rows(t)
        both = second_gate(1, rows)
        for half in range(2):
            zero, one = gate(u5, read(half, 0, rows), both[half])
            keep(half, 0, rows, zero)
            keep(half, 1, rows, one)
        return carry

    def step_last(t, sums):
        rows = piece_rows(t)
        both = second_gate(3, rows)
        sums = list(sums)
        total = None
        for half in range(2):
            two, three = gate(u5, read(half, 2, rows), both[half])
            out_0, out_2 = gate(u4, read(half, 0, rows), two)
            out_1, out_3 = gate(u4, read(half, 1, rows), three)
            for chunk, value in enumerate((out_0, out_1, out_2, out_3)):
                block = half * CHUNKS + chunk
                sign = SG[pl.ds(pl.multiple_of(block * ROWS + 8 * t, 8), 8), :]
                re, im = value[0] * sign, value[1] * sign
                at = pl.multiple_of(block * CHUNK + 16 * t, 16)
                OUT[pl.ds(at, 8, stride=2), :] = re
                OUT[pl.ds(at + 1, 8, stride=2), :] = im
                density = re * re + im * im
                sums[block] = sums[block] + density
                total = density if total is None else total + density
        TP[pl.ds(pl.multiple_of(8 * t, 8), 8), :] = total
        return tuple(sums)

    per_piece = PROWS // 8
    sums = tuple(jnp.zeros((8, 128), F32) for _ in range(8))
    for chunk in range(CHUNKS):
        for piece in range(PIECES):
            for half in range(2):
                stage2(half, chunk, piece).wait_recv()
            if chunk == 0 and piece == 0:
                for other in range(PIECES):
                    for half in range(2):
                        stage2(half, CHUNKS - 1, other).start()
            span = (piece * per_piece, (piece + 1) * per_piece)
            if chunk == 3:
                sums = lax.fori_loop(*span, step_last, sums)
            elif chunk == 1:
                lax.fori_loop(*span, step_odd, 0)
            else:
                lax.fori_loop(*span, step_even(chunk), 0)

    def signed(parts, bit):
        acc = None
        for index, part in enumerate(parts):
            if acc is None:
                acc = part
            elif (index >> bit) & 1:
                acc = acc - part
            else:
                acc = acc + part
        return acc

    def fold(part):
        return jnp.sum(part, axis=0, keepdims=True)

    parts = [TP[8 * t:8 * t + 8, :] for t in range(16)]
    total = signed(parts, 10)
    tot_row = fold(total)
    rows = [tot_row] * 3
    rows += [fold(signed(sums, bit)) for bit in (2, 1, 0)]
    rows += [fold(signed(parts, bit)) for bit in (3, 2, 1, 0)]
    rows += [fold(total * (1 - 2 * ((sub >> bit) & 1)).astype(F32)) for bit in (2, 1, 0)]
    lane_row = lane[0:1, :]
    rows += [tot_row * (1 - 2 * ((lane_row >> bit) & 1)).astype(F32) for bit in (6, 5, 4, 3, 2, 1, 0)]
    rows += [jnp.zeros((1, 128), F32)] * 4
    mine = jnp.concatenate(rows, axis=0)
    V[...] = mine

    def z_copy(dist):
        flip_y, flip_x, flip_c = dist // 4, (dist // 2) % 2, dist % 2
        dev = (me + 4 * flip_y * (1 - 2 * bit_y) + 2 * flip_x * (1 - 2 * bit_x) + flip_c * (1 - 2 * bit_c))
        return remote(V, VR.at[dist], zs.at[dist], zr.at[dist], dev)

    for dist in (7, 6, 5, 3, 4, 2, 1):
        z_copy(dist).start()

    for chunk in range(CHUNKS):
        for half in range(2):
            stage1(half, chunk).wait_send()
            core_copy(half, chunk).wait_send()
            forward(half, chunk).wait_send()
            for piece in range(PIECES):
                stage2(half, chunk, piece).wait_send()

    row24 = lax.broadcasted_iota(jnp.int32, (24, 128), 0)
    col24 = lax.broadcasted_iota(jnp.int32, (24, 128), 1)
    own_sign = jnp.where(row24 == 0, 1 - 2 * bit_y, jnp.where(row24 == 1, 1 - 2 * bit_x, jnp.where(row24 == 2, 1 - 2 * bit_c, 1))).astype(F32)
    acc = mine
    for dist in (1, 2, 4, 3, 5, 6, 7):
        z_copy(dist).wait_recv()
        value = VR[dist]
        flips = [k for k, bit in ((0, 4), (1, 2), (2, 1)) if dist & bit]
        mask = row24 == flips[0]
        for k in flips[1:]:
            mask = mask | (row24 == k)
        acc = acc + jnp.where(mask, -value, value)
    acc = acc * own_sign
    column = jnp.sum(acc, axis=1, keepdims=True)
    spread = jnp.where(row24 == col24, column, 0.0)
    z_ref[...] = jnp.sum(spread, axis=0, keepdims=True)[:, 0:20] * (1.0 / (131072 * DEVICES))
    for dist in range(1, DEVICES):
        z_copy(dist).wait_send()


def solution(mesh):
    def local_layer(state_local, unitaries, cz_pairs):
        size = state_local.shape[1]
        rows = 2 * size // 128
        x = state_local.reshape(2, size // 128, 128).transpose(1, 0, 2).reshape(rows, 128)
        u = unitaries.transpose(0, 2, 3, 1).reshape(8, 20)
        cz = cz_pairs.T
        vm = pltpu.VMEM
        dma = pltpu.SemaphoreType.DMA
        out, z = pl.pallas_call(
            kernel,
            out_shape=(jax.ShapeDtypeStruct((rows, 128), F32), jax.ShapeDtypeStruct((1, 20), F32)),
            in_specs=[pl.BlockSpec(memory_space=pltpu.VMEM), pl.BlockSpec(memory_space=pltpu.SMEM), pl.BlockSpec(memory_space=pltpu.SMEM)],
            out_specs=(pl.BlockSpec(memory_space=pltpu.VMEM), pl.BlockSpec(memory_space=pltpu.VMEM)),
            scratch_shapes=[
                vm((rows, 128), F32), vm((rows, 128), F32), vm((rows, 128), F32),
                vm((2, CHUNKS, 2, ROWS, 128), F32), vm((2, CHUNKS, 2, ROWS, 128), F32), vm((2, CHUNKS, 2, ROWS, 128), F32),
                vm((rows // 2, 128), F32),
                vm((256, 256), F32), vm((256, 256), F32), vm((256, 256), F32), vm((256, 256), F32),
                vm((128, 128), F32), vm((24, 128), F32), vm((DEVICES, 24, 128), F32),
                dma((8,)), dma((8,)), dma((8,)), dma((8,)), dma((8,)), dma((8,)),
                dma((8 * PIECES,)), dma((8 * PIECES,)), dma((DEVICES,)), dma((DEVICES,)),
            ],
            compiler_params=pltpu.CompilerParams(collective_id=0, has_side_effects=True, vmem_limit_bytes=40 * 2 ** 20),
        )(x, u, cz)
        state = out.reshape(size // 128, 2, 128).transpose(1, 0, 2).reshape(2, size)
        return state, z.reshape(20)

    return jax.shard_map(local_layer, mesh=mesh, in_specs=(P(None, 'q'), P(), P()), out_specs=(P(None, 'q'), P()), check_vma=False)
```

```python
import jax
import jax.numpy as jnp
from jax import lax
from jax.experimental import pallas as pl
from jax.experimental.pallas import tpu as pltpu
from jax.sharding import PartitionSpec as P

MESH = pl.DeviceIdType.MESH
F32 = jnp.float32
LANES = 128
SUB = 8
TILES = 16
LOW, HIGH = slice(0, LANES), slice(LANES, 2 * LANES)
ROWS = SUB * TILES
CHUNK = 2 * ROWS
CHUNKS = 4
PIECES = (0, 48, 88, 112, 128)
EARLY = 2
DEVICES = 8
QUBITS = 20
scope = jax.named_scope


def cmul(a, b):
    (a_re, a_im), (b_re, b_im) = a, b
    return a_re * b_re - a_im * b_im, a_re * b_im + a_im * b_re


def cadd(a, b):
    (a_re, a_im), (b_re, b_im) = a, b
    return a_re + b_re, a_im + b_im


def conj_mul(a, b):
    (a_re, a_im), (b_re, b_im) = a, b
    return a_re * b_re + a_im * b_im, a_re * b_im - a_im * b_re


def mix(coefs, values):
    total = None
    for coef, value in zip(coefs, values):
        part = cmul(coef, value)
        total = part if total is None else cadd(total, part)
    return total


def gate(mat, zero, one):
    u00, u01, u10, u11 = mat
    return mix((u00, u01), (zero, one)), mix((u10, u11), (zero, one))


def norm(a):
    re, im = a
    return re * re + im * im


def plus_minus(bit):
    return 1 - 2 * bit


def planes(ref, half, chunk, rows):
    return [ref[half, chunk, part, rows, :] for part in range(2)]


def put(ref, half, chunk, rows, value):
    for part in range(2):
        ref[half, chunk, part, rows, :] = value[part]


def tile(t, first=0):
    return pl.ds(pl.multiple_of(first + SUB * t, SUB), SUB)


def kernel(x_hbm, u_hbm, cz_hbm, OUT, z_ref,
           X, u_ref, cz_ref, RB, XP, RP, S, R2, T, SG, GM, KM, XC, ZC, TP, V, VR,
           ld, s1s, s1r, cps, cpr, fws, fwr, s2s, s2r, zs, zr):
    me = lax.axis_index('q')
    bit_y = me // 4
    bit_x = (me // 2) % 2
    bit_c = me % 2
    step_y, step_x, step_c = 4 * plus_minus(bit_y), 2 * plus_minus(bit_x), plus_minus(bit_c)
    dev_y, dev_x, dev_c = me + step_y, me + step_x, me + step_c
    first_dev = (dev_x, dev_y)
    second_dev = (dev_y, dev_x)
    second_bit = (bit_y, bit_x)

    def sent(half, k):
        return k + second_bit[half] * (3 - 2 * k)

    def received(half, k):
        return 3 - k + second_bit[half] * (2 * k - 3)

    def block_rows(half, chunk):
        return pl.ds(pl.multiple_of((half * CHUNKS + chunk) * CHUNK, CHUNK), CHUNK)

    def remote(src, dst, send, recv, dev):
        return pltpu.make_async_remote_copy(src_ref=src, dst_ref=dst, send_sem=send, recv_sem=recv,
                                            device_id=(dev,), device_id_type=MESH)

    def wait_bytes(ref, sem):
        pltpu.make_async_copy(ref, ref, sem).wait()

    def load_copy(half, k):
        rows = block_rows(half, sent(half, k))
        return pltpu.make_async_copy(x_hbm.at[rows], X.at[rows], ld.at[min(k, 1)])

    def stage1(half, k):
        rows = block_rows(half, sent(half, k))
        return remote(X.at[rows], RB.at[rows], s1s, s1r.at[k], first_dev[half])

    def core_copy(half, k):
        rows = block_rows(half, sent(half, k))
        return remote(X.at[rows], XP.at[rows], cps, cpr, dev_c)

    def forward(half, k):
        rows = block_rows(half, sent(half, k))
        return remote(RB.at[rows], RP.at[rows], fws, fwr.at[k], dev_c)

    def stage2(half, k, piece=None):
        chunk = sent(half, k)
        if piece is None:
            return remote(S.at[half, chunk], R2.at[half, chunk], s2s, s2r.at[k], second_dev[half])
        rows = pl.ds(PIECES[piece], PIECES[piece + 1] - PIECES[piece])
        return remote(S.at[half, chunk, :, rows], R2.at[half, chunk, :, rows], s2s, s2r.at[3 + piece], second_dev[half])

    u_copy = pltpu.make_async_copy(u_hbm, u_ref, ld.at[2])
    cz_copy = pltpu.make_async_copy(cz_hbm, cz_ref, ld.at[3])
    for k in range(CHUNKS):
        for half in range(2):
            load_copy(half, k).start()
    u_copy.start()
    cz_copy.start()

    barrier = pltpu.get_barrier_semaphore()
    for dev in (dev_x, dev_y, dev_c):
        pl.semaphore_signal(barrier, inc=1, device_id=(dev,), device_id_type=MESH)
    with scope('bar'):
        pl.semaphore_wait(barrier, 3)

    with scope('w_ld'):
        wait_bytes(X.at[0:2 * CHUNK], ld.at[0])
    for half in range(2):
        stage1(half, 0).start()
    with scope('w_ld'):
        wait_bytes(X.at[0:6 * CHUNK], ld.at[1])
    for k in range(1, CHUNKS):
        for half in range(2):
            stage1(half, k).start()
    for k in range(CHUNKS):
        for half in range(2):
            core_copy(half, k).start()
    u_copy.wait()
    cz_copy.wait()

    def entry(qubit, row, col):
        return u_ref[row * 2 + col, qubit], u_ref[4 + row * 2 + col, qubit]

    def matrix(qubit, flip=0):
        return [entry(qubit, row + flip * plus_minus(row), col + flip * plus_minus(col)) for row in range(2) for col in range(2)]

    lane = lax.broadcasted_iota(jnp.int32, (SUB, LANES), 1)
    sub = lax.broadcasted_iota(jnp.int32, (SUB, LANES), 0)

    def build(t, carry):
        row = sub + SUB * t
        for base, left in ((6, True), (13, False)):
            re = im = None
            for j in range(7):
                shift = 6 - j
                row_bit = ((row >> shift) & 1) == 1
                col_bit = ((lane >> shift) & 1) == 1
                fac = []
                for ri in range(2):
                    u00, u01, u10, u11 = [u_ref[4 * ri + k, base + j] for k in range(4)]
                    if not left:
                        u01, u10 = u10, u01
                    fac.append(jnp.where(row_bit, jnp.where(col_bit, u11, u10), jnp.where(col_bit, u01, u00)))
                if re is None:
                    re, im = fac
                else:
                    re, im = cmul((re, im), fac)
            low, high = tile(t), tile(t, LANES)
            dest, upper, lower = (GM, -im, im) if left else (KM, im, -im)
            dest[low, LOW] = re
            dest[low, HIGH] = upper
            dest[high, LOW] = lower
            dest[high, HIGH] = re
        return carry

    with scope('build'):
        lax.fori_loop(0, TILES, build, 0)

    shifts = [[QUBITS - 1 - cz_ref[side, k] for side in range(2)] for k in range(QUBITS // 2)]

    def build_signs(t, carry):
        flat = (me * DEVICES * ROWS + sub + SUB * t) * LANES + lane
        parity = jnp.zeros_like(flat)
        for shift_a, shift_b in shifts:
            parity = parity ^ ((flat >> shift_a) & (flat >> shift_b))
        SG[tile(t), :] = plus_minus(parity & 1).astype(F32)
        return carry

    with scope('signs'):
        lax.fori_loop(0, DEVICES * TILES, build_signs, 0, unroll=4)

    def strided(ref, at):
        return [ref[pl.ds(at + part, SUB, stride=2), :] for part in range(2)]

    zero_tile = jnp.zeros((SUB, LANES), F32)
    zero_pair = (zero_tile, zero_tile)

    def raw_sums(t, carry):
        total, sums = carry
        value = [strided(X, pl.multiple_of(block * CHUNK + 2 * SUB * t, 2 * SUB)) for block in range(DEVICES)]
        dens = [norm(v) for v in value]
        done = []
        for (diff, cross), bit in zip(sums, (4, 2, 1)):
            for block in range(DEVICES):
                if block & bit:
                    diff = diff - dens[block]
                else:
                    diff = diff + dens[block]
                    cross = cadd(cross, conj_mul(value[block], value[block + bit]))
            done.append((diff, cross))
        for part in dens:
            total = total + part
        return total, tuple(done)

    with scope('raw'):
        raw_total, raw = lax.fori_loop(0, TILES, raw_sums, (zero_tile, ((zero_tile, zero_pair),) * 3))

    def fold(part):
        return jnp.sum(part, axis=0, keepdims=True)

    def pair_weights(mat):
        u00, u01, u10, u11 = mat
        (a_re, a_im), (b_re, b_im) = conj_mul(u00, u01), conj_mul(u10, u11)
        return norm(u00) - norm(u10), norm(u01) - norm(u11), 2 * (a_re - b_re), 2 * (b_im - a_im)

    raw_rows = []
    raw_total = fold(raw_total)
    for qubit, (diff, (re, im)) in zip((3, 4, 5), raw):
        weight_0, weight_1, mix_re, mix_im = pair_weights(matrix(qubit))
        even, odd = raw_total + fold(diff), raw_total - fold(diff)
        raw_rows.append((weight_0 * even + weight_1 * odd) / 2 + mix_re * fold(re) + mix_im * fold(im))

    def gate_pair(qubit, own_bit):
        return entry(qubit, own_bit, own_bit), entry(qubit, own_bit, 1 - own_bit)

    coef_y = gate_pair(0, bit_y)
    coef_x = gate_pair(1, bit_x)
    coef_c = gate_pair(2, bit_c)
    stage1_coefs = [[cmul(top, core) for core in coef_c for top in coef] for coef in (coef_x, coef_y)]

    norms = zero_pair
    for k in range(CHUNKS):
        with scope('w_s1'):
            wait_bytes(RB.at[0:2 * CHUNK], s1r.at[k])
        for half in range(2):
            forward(half, k).start()
        if k:
            for half in range(2):
                stage2(half, k - 1).start()
        if k == 0:
            wait_bytes(XP, cpr)
        with scope('w_fw'):
            wait_bytes(RP.at[0:2 * CHUNK], fwr.at[k])

        for half in range(2):
            coefs = stage1_coefs[half]
            base = (half * CHUNKS + sent(half, k)) * CHUNK

            def combine(t, carry, base=base, coefs=coefs, half=half):
                at = pl.multiple_of(base + 2 * SUB * t, 2 * SUB)
                re, im = mix(coefs, [strided(ref, at) for ref in (X, RB, XP, RP)])
                XC[tile(t), (LOW, HIGH)[half]] = re
                XC[tile(t, LANES), (LOW, HIGH)[half]] = im
                return carry

            with scope('comb'):
                lax.fori_loop(0, TILES, combine, 0, unroll=2)
        with scope('mm'):
            left = lax.dot(GM[...], XC[...], precision=lax.Precision.HIGHEST, preferred_element_type=F32)
            for rows in (LOW, HIGH):
                for cols in (LOW, HIGH):
                    ZC[cols, rows] = left[rows, cols]
            both = lax.dot(ZC[...], KM[...], precision=lax.Precision.HIGHEST, preferred_element_type=F32)
            for half in range(2):
                for part in range(2):
                    S[half, sent(half, k), part] = both[(LOW, HIGH)[half], (LOW, HIGH)[part]]

        def mid_sums(t, sums, k=k):
            dens = [norm(planes(S, half, sent(half, k), tile(t))) for half in range(2)]
            row = dens[0] + dens[1]
            TP[tile(t), :] = row if k == 0 else TP[tile(t), :] + row
            return tuple(a + b for a, b in zip(sums, dens))

        with scope('dens'):
            norms = lax.fori_loop(0, TILES, mid_sums, norms, unroll=2)

    flips = (1 - bit_y, 1 - bit_x)
    u3 = matrix(3)
    u4 = [matrix(4, flip) for flip in flips]
    u5 = [matrix(5, flip) for flip in flips]
    second_coef = (coef_y, coef_x)

    def second_gate(half, k, rows):
        chunk = received(half, k)
        return mix(second_coef[half], (planes(S, half, chunk, rows), planes(R2, half, chunk, rows)))

    def add_cross(k):
        def body(t, cross):
            done = []
            for half in range(2):
                chunk = received(half, k)
                part = conj_mul(planes(S, half, chunk, tile(t)), planes(R2, half, chunk, tile(t)))
                done.append(cadd(cross[half], part))
            return tuple(done)
        return body

    def step_even(k):
        def body(t, carry):
            for half in range(2):
                put(T, half, k, tile(t), second_gate(half, k, tile(t)))
            return carry
        return body

    def step_second(t, carry):
        rows = tile(t)
        for half in range(2):
            pair = gate(u5[half], planes(T, half, 0, rows), second_gate(half, 1, rows))
            for k, value in enumerate(pair):
                put(T, half, k, rows, value)
        return carry

    def step_last(t, carry):
        rows = tile(t)
        for half in range(2):
            upper = gate(u5[half], planes(T, half, 2, rows), second_gate(half, 3, rows))
            pairs = [gate(u4[half], planes(T, half, k, rows), upper[k]) for k in range(2)]
            for k in range(CHUNKS):
                put(T, half, received(half, k), rows, pairs[k % 2][k // 2])
        return carry

    def step_out(t, carry):
        rows = tile(t)
        for chunk in range(CHUNKS):
            for half, done in enumerate(gate(u3, planes(T, 0, chunk, rows), planes(T, 1, chunk, rows))):
                block = half * CHUNKS + chunk
                sign = SG[tile(t, block * ROWS), :]
                at = pl.multiple_of(block * CHUNK + 2 * SUB * t, 2 * SUB)
                for part in range(2):
                    OUT[pl.ds(at + part, SUB, stride=2), :] = done[part] * sign
        return carry

    cross = (zero_pair, zero_pair)
    with scope('w_s2'):
        wait_bytes(R2.at[:, 0], s2r.at[0])
    for piece in range(EARLY):
        for half in range(2):
            stage2(half, 3, piece).start()
    with scope('st0'):
        cross = lax.fori_loop(0, TILES, add_cross(0), cross, unroll=2)
        lax.fori_loop(0, TILES, step_even(0), 0, unroll=2)
    with scope('w_s2'):
        wait_bytes(R2.at[:, 0], s2r.at[1])
    with scope('x1'):
        cross = lax.fori_loop(0, TILES, add_cross(1), cross, unroll=2)

    def signed(parts, bit):
        acc = parts[0]
        for index, part in enumerate(parts[1:], 1):
            acc = acc - part if (index >> bit) & 1 else acc + part
        return acc

    def z_copy(dist):
        dev = me + (dist // 4) * step_y + (dist // 2 % 2) * step_x + (dist % 2) * step_c
        return remote(V, VR.at[dist], zs, zr, dev)

    row_index = lax.broadcasted_iota(jnp.int32, (3 * SUB, LANES), 0)
    col_index = lax.broadcasted_iota(jnp.int32, (3 * SUB, LANES), 1)
    with scope('zsum'):
        signs = [plus_minus(bit).astype(F32) for bit in (bit_y, bit_x, bit_c)]
        norm_rows = [fold(part) for part in norms]
        tot_row = norm_rows[0] + norm_rows[1]
        rows = []
        for half, bit in enumerate(second_bit):
            weight_0, weight_1, mix_re, mix_im = pair_weights(matrix(half))
            re, im = cross[half]
            rows.append(jnp.where(bit == 1, weight_1, weight_0) * norm_rows[half] + mix_re * fold(re)
                        + (mix_im * signs[half]) * fold(im) + signs[half] * norm_rows[1 - half])
        rows += [signs[2] * tot_row] + raw_rows
        parts = [TP[tile(t), :] for t in range(TILES)]
        rows += [fold(signed(parts, bit)) for bit in reversed(range(4))]
        total = norms[0] + norms[1]
        rows += [fold(total * plus_minus((sub >> bit) & 1).astype(F32)) for bit in reversed(range(3))]
        rows += [tot_row * plus_minus((lane[:1] >> bit) & 1).astype(F32) for bit in reversed(range(7))]
        rows += [jnp.zeros_like(tot_row)] * 4
        column = jnp.sum(jnp.concatenate(rows, axis=0), axis=1, keepdims=True)
        mine = jnp.sum(jnp.where(row_index == col_index, column, 0.0), axis=0, keepdims=True)
        V[...] = mine
    with scope('st1'):
        lax.fori_loop(0, TILES, step_second, 0, unroll=2)
    for dist in reversed(range(1, DEVICES)):
        z_copy(dist).start()
    for piece in range(EARLY, len(PIECES) - 1):
        for half in range(2):
            stage2(half, 3, piece).start()
    with scope('w_s2'):
        wait_bytes(R2.at[:, 0], s2r.at[2])
    with scope('st2'):
        lax.fori_loop(0, TILES, step_even(2), 0, unroll=2)

    for piece in range(len(PIECES) - 1):
        low, high = PIECES[piece], PIECES[piece + 1]
        with scope('w_s2'):
            wait_bytes(R2.at[:, 0, :, low:high], s2r.at[3 + piece])
        with scope('tail'):
            lax.fori_loop(low // SUB, high // SUB, step_last, 0)
            lax.fori_loop(low // SUB, high // SUB, step_out, 0)
        if piece == len(PIECES) - 3:
            with scope('w_z'):
                wait_bytes(VR.at[1:DEVICES], zr)
            acc = mine
            for dist in range(1, DEVICES):
                acc = acc + VR[dist]
            z_ref[...] = acc[:, :QUBITS] / 2 ** QUBITS

    with scope('w_send'):
        wait_bytes(X, s1s)
        wait_bytes(X, cps)
        wait_bytes(X, fws)
        wait_bytes(S, s2s)
        wait_bytes(VR.at[1:DEVICES], zs)


def writer(state_ref, z_ref, state_out, z_out, sems):
    copies = [pltpu.make_async_copy(state_ref, state_out, sems.at[0]), pltpu.make_async_copy(z_ref, z_out, sems.at[1])]
    for copy in copies:
        copy.start()
    for copy in copies:
        copy.wait()


def solution(mesh):
    def local_layer(state_local, unitaries, cz_pairs):
        size = state_local.shape[1]
        rows = 2 * size // LANES
        x = state_local.reshape(2, -1, LANES).swapaxes(0, 1).reshape(rows, LANES)
        u = unitaries.transpose(0, 2, 3, 1).reshape(SUB, QUBITS)
        cz = cz_pairs.T
        x, u, cz = [pltpu.with_memory_space_constraint(v, pltpu.HBM) for v in (x, u, cz)]
        vm = pltpu.VMEM
        dma = pltpu.SemaphoreType.DMA
        full = vm((rows, LANES), F32)
        halves = vm((2, CHUNKS, 2, ROWS, LANES), F32)
        square = vm((2 * LANES, 2 * LANES), F32)
        any_spec = pl.BlockSpec(memory_space=pl.ANY)
        shapes = (jax.ShapeDtypeStruct((rows, LANES), F32), jax.ShapeDtypeStruct((1, QUBITS), F32))
        out, z = pl.pallas_call(
            kernel,
            out_shape=shapes,
            in_specs=[pl.BlockSpec(memory_space=pltpu.HBM)] * 3,
            out_specs=(pl.BlockSpec(memory_space=pltpu.VMEM), pl.BlockSpec(memory_space=pltpu.VMEM)),
            scratch_shapes=[
                full, pltpu.SMEM(u.shape, F32), pltpu.SMEM(cz.shape, jnp.int32), full, full, full, halves, halves, halves,
                vm((rows // 2, LANES), F32), square, square, square, square, vm((ROWS, LANES), F32),
                vm((1, LANES), F32), vm((DEVICES, 1, LANES), F32),
                dma((4,)), dma, dma((4,)), dma, dma, dma, dma((4,)), dma, dma((3 + len(PIECES) - 1,)), dma, dma,
            ],
            compiler_params=pltpu.CompilerParams(collective_id=0, has_side_effects=True, vmem_limit_bytes=40 * 2 ** 20),
        )(x, u, cz)
        out, z = pl.pallas_call(
            writer, out_shape=shapes, in_specs=[any_spec] * 2, out_specs=(any_spec,) * 2, scratch_shapes=[dma((2,))],
            compiler_params=pltpu.CompilerParams(vmem_limit_bytes=2 ** 20),
        )(out, z)
        state = out.reshape(-1, 2, LANES).swapaxes(0, 1).reshape(2, size)
        return state, z.reshape(QUBITS)

    return jax.shard_map(local_layer, mesh=mesh, in_specs=(P(None, 'q'), P(), P()), out_specs=(P(None, 'q'), P()), check_vma=False)
```

```python
import jax
import jax.numpy as jnp
from jax import lax
from jax.experimental import pallas as pl
from jax.experimental.pallas import tpu as pltpu
from jax.sharding import PartitionSpec as P

MESH = pl.DeviceIdType.MESH
F32 = jnp.float32
LANES = 128
SUB = 8
TILES = 16
LOW, HIGH = slice(0, LANES), slice(LANES, 2 * LANES)
ROWS = SUB * TILES
CHUNK = 2 * ROWS
CHUNKS = 4
PIECES = (0, 24, 72, 112, 128)
FIRST = CHUNK // 4
EARLY = 1
DEVICES = 8
QUBITS = 20
scope = jax.named_scope


def cmul(a, b):
    (a_re, a_im), (b_re, b_im) = a, b
    return a_re * b_re - a_im * b_im, a_re * b_im + a_im * b_re


def cadd(a, b):
    (a_re, a_im), (b_re, b_im) = a, b
    return a_re + b_re, a_im + b_im


def conj_mul(a, b):
    (a_re, a_im), (b_re, b_im) = a, b
    return a_re * b_re + a_im * b_im, a_re * b_im - a_im * b_re


def mix(coefs, values):
    total = None
    for coef, value in zip(coefs, values):
        part = cmul(coef, value)
        total = part if total is None else cadd(total, part)
    return total


def gate(mat, zero, one):
    u00, u01, u10, u11 = mat
    return mix((u00, u01), (zero, one)), mix((u10, u11), (zero, one))


def norm(a):
    re, im = a
    return re * re + im * im


def plus_minus(bit):
    return 1 - 2 * bit


def planes(ref, half, chunk, rows):
    return [ref[half, chunk, part, rows, :] for part in range(2)]


def put(ref, half, chunk, rows, value):
    for part in range(2):
        ref[half, chunk, part, rows, :] = value[part]


def tile(t, first=0):
    return pl.ds(pl.multiple_of(first + SUB * t, SUB), SUB)


def kernel(x_hbm, u_hbm, cz_hbm, OUT, z_ref,
           BIG, u_ref, cz_ref, S, R2, T, SG, GM, KM, XC, ZC, TP, V, VR,
           ld, sent_sem, s1r, cpr, fwr, s2r, zs, zr):
    X, RB, XP, RP = [BIG.at[part] for part in range(4)]
    me = lax.axis_index('q')
    bit_y = me // 4
    bit_x = (me // 2) % 2
    bit_c = me % 2
    step_y, step_x, step_c = 4 * plus_minus(bit_y), 2 * plus_minus(bit_x), plus_minus(bit_c)
    dev_y, dev_x, dev_c = me + step_y, me + step_x, me + step_c
    first_dev = (dev_x, dev_y)
    second_dev = (dev_y, dev_x)
    second_bit = (bit_y, bit_x)

    def sent(half, k):
        return k + second_bit[half] * (3 - 2 * k)

    def received(half, k):
        return 3 - k + second_bit[half] * (2 * k - 3)

    def block_rows(half, chunk):
        return pl.ds(pl.multiple_of((half * CHUNKS + chunk) * CHUNK, CHUNK), CHUNK)

    def remote(src, dst, send, recv, dev):
        return pltpu.make_async_remote_copy(src_ref=src, dst_ref=dst, send_sem=send, recv_sem=recv,
                                            device_id=(dev,), device_id_type=MESH)

    def wait_bytes(ref, sem):
        pltpu.make_async_copy(ref, ref, sem).wait()

    def part_rows(half, k, part):
        low, size = ((0, FIRST), (FIRST, CHUNK - FIRST))[part] if k == 0 else (0, CHUNK)
        return pl.ds(pl.multiple_of((half * CHUNKS + sent(half, k)) * CHUNK + low, SUB), size)

    def load_copy(half, k, part=0):
        rows = part_rows(half, k, part)
        return pltpu.make_async_copy(x_hbm.at[rows], X.at[rows], ld.at[min(2, k + 1) if k else part])

    def stage1(half, k, part=0):
        rows = part_rows(half, k, part)
        return remote(X.at[rows], RB.at[rows], sent_sem, s1r.at[k], first_dev[half])

    def core_copy(half, k):
        rows = block_rows(half, sent(half, k))
        return remote(X.at[rows], XP.at[rows], sent_sem, cpr, dev_c)

    def forward(half, k):
        rows = block_rows(half, sent(half, k))
        return remote(RB.at[rows], RP.at[rows], sent_sem, fwr.at[k], dev_c)

    def stage2(half, k, piece=None):
        chunk = sent(half, k)
        if piece is None:
            return remote(S.at[half, chunk], R2.at[half, chunk], sent_sem, s2r.at[k], second_dev[half])
        rows = pl.ds(PIECES[piece], PIECES[piece + 1] - PIECES[piece])
        return remote(S.at[half, chunk, :, rows], R2.at[half, chunk, :, rows], sent_sem, s2r.at[3 + piece], second_dev[half])

    u_copy = pltpu.make_async_copy(u_hbm, u_ref, ld.at[3])
    cz_copy = pltpu.make_async_copy(cz_hbm, cz_ref, ld.at[4])
    order = [(k, part) for k in range(CHUNKS) for part in range(1 if k else 2)]
    for k, part in order:
        for half in range(2):
            load_copy(half, k, part).start()
    u_copy.start()
    cz_copy.start()

    barrier = pltpu.get_barrier_semaphore()
    for dev in (dev_x, dev_y, dev_c):
        pl.semaphore_signal(barrier, inc=1, device_id=(dev,), device_id_type=MESH)
    with scope('bar'):
        pl.semaphore_wait(barrier, 3)

    waits = {(0, 0): (0, 2 * FIRST), (0, 1): (1, 2 * (CHUNK - FIRST)), (1, 0): (2, 6 * CHUNK)}
    for k, part in order:
        if (k, part) in waits:
            index, size = waits[k, part]
            with scope('w_ld'):
                wait_bytes(X.at[:size], ld.at[index])
        for half in range(2):
            stage1(half, k, part).start()
    for k in range(CHUNKS):
        for half in range(2):
            core_copy(half, k).start()
    u_copy.wait()
    cz_copy.wait()

    def entry(qubit, row, col):
        return u_ref[row * 2 + col, qubit], u_ref[4 + row * 2 + col, qubit]

    def matrix(qubit, flip=0):
        return [entry(qubit, row + flip * plus_minus(row), col + flip * plus_minus(col)) for row in range(2) for col in range(2)]

    lane = lax.broadcasted_iota(jnp.int32, (SUB, LANES), 1)
    sub = lax.broadcasted_iota(jnp.int32, (SUB, LANES), 0)

    def build(t, carry):
        row = sub + SUB * t
        for base, left in ((6, True), (13, False)):
            re = im = None
            for j in range(7):
                shift = 6 - j
                row_bit = ((row >> shift) & 1) == 1
                col_bit = ((lane >> shift) & 1) == 1
                fac = []
                for ri in range(2):
                    u00, u01, u10, u11 = [u_ref[4 * ri + k, base + j] for k in range(4)]
                    if not left:
                        u01, u10 = u10, u01
                    fac.append(jnp.where(row_bit, jnp.where(col_bit, u11, u10), jnp.where(col_bit, u01, u00)))
                if re is None:
                    re, im = fac
                else:
                    re, im = cmul((re, im), fac)
            low, high = tile(t), tile(t, LANES)
            dest, upper, lower = (GM, -im, im) if left else (KM, im, -im)
            dest[low, LOW] = re
            dest[low, HIGH] = upper
            dest[high, LOW] = lower
            dest[high, HIGH] = re
        return carry

    with scope('build'):
        lax.fori_loop(0, TILES, build, 0)

    shifts = [[QUBITS - 1 - cz_ref[side, k] for side in range(2)] for k in range(QUBITS // 2)]

    def build_signs(t, carry):
        flat = (me * DEVICES * ROWS + sub + SUB * t) * LANES + lane
        parity = jnp.zeros_like(flat)
        for shift_a, shift_b in shifts:
            parity = parity ^ ((flat >> shift_a) & (flat >> shift_b))
        SG[tile(t), :] = plus_minus(parity & 1).astype(F32)
        return carry

    with scope('signs'):
        lax.fori_loop(0, DEVICES * TILES, build_signs, 0, unroll=4)

    def strided(ref, at):
        return [ref[pl.ds(at + part, SUB, stride=2), :] for part in range(2)]

    zero_tile = jnp.zeros((SUB, LANES), F32)
    zero_pair = (zero_tile, zero_tile)

    def raw_sums(t, carry):
        total, sums = carry
        value = [strided(X, pl.multiple_of(block * CHUNK + 2 * SUB * t, 2 * SUB)) for block in range(DEVICES)]
        dens = [norm(v) for v in value]
        done = []
        for (diff, cross), bit in zip(sums, (4, 2, 1)):
            for block in range(DEVICES):
                if block & bit:
                    diff = diff - dens[block]
                else:
                    diff = diff + dens[block]
                    cross = cadd(cross, conj_mul(value[block], value[block + bit]))
            done.append((diff, cross))
        for part in dens:
            total = total + part
        return total, tuple(done)

    with scope('raw'):
        raw_total, raw = lax.fori_loop(0, TILES, raw_sums, (zero_tile, ((zero_tile, zero_pair),) * 3))

    def fold(part):
        return jnp.sum(part, axis=0, keepdims=True)

    def pair_weights(mat):
        u00, u01, u10, u11 = mat
        (a_re, a_im), (b_re, b_im) = conj_mul(u00, u01), conj_mul(u10, u11)
        return norm(u00) - norm(u10), norm(u01) - norm(u11), 2 * (a_re - b_re), 2 * (b_im - a_im)

    raw_rows = []
    raw_total = fold(raw_total)
    for qubit, (diff, (re, im)) in zip((3, 4, 5), raw):
        weight_0, weight_1, mix_re, mix_im = pair_weights(matrix(qubit))
        even, odd = raw_total + fold(diff), raw_total - fold(diff)
        raw_rows.append((weight_0 * even + weight_1 * odd) / 2 + mix_re * fold(re) + mix_im * fold(im))

    def gate_pair(qubit, own_bit):
        return entry(qubit, own_bit, own_bit), entry(qubit, own_bit, 1 - own_bit)

    coef_y = gate_pair(0, bit_y)
    coef_x = gate_pair(1, bit_x)
    coef_c = gate_pair(2, bit_c)
    stage1_coefs = [[cmul(top, core) for core in coef_c for top in coef] for coef in (coef_x, coef_y)]

    norms = zero_pair
    for k in range(CHUNKS):
        with scope('w_s1'):
            wait_bytes(RB.at[0:2 * CHUNK], s1r.at[k])
        for half in range(2):
            forward(half, k).start()
        if k:
            for half in range(2):
                stage2(half, k - 1).start()
        if k == 0:
            wait_bytes(XP, cpr)
        with scope('w_fw'):
            wait_bytes(RP.at[0:2 * CHUNK], fwr.at[k])

        for half in range(2):
            coefs = stage1_coefs[half]
            base = (half * CHUNKS + sent(half, k)) * CHUNK

            def combine(t, carry, base=base, coefs=coefs, half=half):
                at = pl.multiple_of(base + 2 * SUB * t, 2 * SUB)
                re, im = mix(coefs, [strided(ref, at) for ref in (X, RB, XP, RP)])
                XC[tile(t), (LOW, HIGH)[half]] = re
                XC[tile(t, LANES), (LOW, HIGH)[half]] = im
                return carry

            with scope('comb'):
                lax.fori_loop(0, TILES, combine, 0, unroll=2)
        with scope('mm'):
            left = lax.dot(GM[...], XC[...], precision=lax.Precision.HIGHEST, preferred_element_type=F32)
            for rows in (LOW, HIGH):
                for cols in (LOW, HIGH):
                    ZC[cols, rows] = left[rows, cols]
            both = lax.dot(ZC[...], KM[...], precision=lax.Precision.HIGHEST, preferred_element_type=F32)
            for half in range(2):
                for part in range(2):
                    S[half, sent(half, k), part] = both[(LOW, HIGH)[half], (LOW, HIGH)[part]]

        def mid_sums(t, sums, k=k):
            dens = [norm(planes(S, half, sent(half, k), tile(t))) for half in range(2)]
            row = dens[0] + dens[1]
            TP[tile(t), :] = row if k == 0 else TP[tile(t), :] + row
            return tuple(a + b for a, b in zip(sums, dens))

        with scope('dens'):
            norms = lax.fori_loop(0, TILES, mid_sums, norms, unroll=2)

    flips = (1 - bit_y, 1 - bit_x)
    u3 = matrix(3)
    u4 = [matrix(4, flip) for flip in flips]
    u5 = [matrix(5, flip) for flip in flips]
    second_coef = (coef_y, coef_x)

    def weights(k):
        table = {}
        for half in range(2):
            index = received(half, k)
            for chunk in range(CHUNKS):
                inner = cmul(entry(4, chunk // 2, index // 2), entry(5, chunk % 2, index % 2))
                inner = cmul(second_coef[half][1], inner)
                for side in range(2):
                    table[side, chunk, half] = cmul(u3[2 * side + half], inner)
        return table

    def add_cross(k):
        def body(t, cross):
            done = []
            for half in range(2):
                chunk = received(half, k)
                part = conj_mul(planes(S, half, chunk, tile(t)), planes(R2, half, chunk, tile(t)))
                done.append(cadd(cross[half], part))
            return tuple(done)
        return body

    def step_own(t, carry):
        rows = tile(t)
        for half in range(2):
            own, other = second_coef[half]
            value = []
            for k in range(CHUNKS):
                chunk = received(half, k)
                part = cmul(own, planes(S, half, chunk, rows))
                value.append(cadd(part, cmul(other, planes(R2, half, chunk, rows))) if k < 2 else part)
            value = [v for pair in (value[:2], value[2:]) for v in gate(u5[half], *pair)]
            value = [gate(u4[half], value[k], value[k + 2]) for k in range(2)]
            for k in range(CHUNKS):
                put(T, half, received(half, k), rows, value[k % 2][k // 2])
        return carry

    def step_mix(t, carry):
        rows = tile(t)
        for chunk in range(CHUNKS):
            for half, value in enumerate(gate(u3, planes(T, 0, chunk, rows), planes(T, 1, chunk, rows))):
                put(T, half, chunk, rows, value)
        return carry

    def add_received(k, table, store):
        def body(t, carry):
            rows = tile(t)
            other = [planes(R2, half, received(half, k), rows) for half in range(2)]
            for side in range(2):
                for chunk in range(CHUNKS):
                    value = planes(T, side, chunk, rows)
                    for half in range(2):
                        value = cadd(value, cmul(table[side, chunk, half], other[half]))
                    store(side, chunk, t, value)
            return carry
        return body

    def store_partial(side, chunk, t, value):
        put(T, side, chunk, tile(t), value)

    def store_out(side, chunk, t, value):
        block = side * CHUNKS + chunk
        sign = SG[tile(t, block * ROWS), :]
        at = pl.multiple_of(block * CHUNK + 2 * SUB * t, 2 * SUB)
        for part in range(2):
            OUT[pl.ds(at + part, SUB, stride=2), :] = value[part] * sign

    tables = {k: weights(k) for k in (2, 3)}
    cross = (zero_pair, zero_pair)
    with scope('w_s2'):
        wait_bytes(R2.at[:, 0], s2r.at[0])
    for piece in range(EARLY):
        for half in range(2):
            stage2(half, 3, piece).start()
    with scope('x0'):
        cross = lax.fori_loop(0, TILES, add_cross(0), cross, unroll=2)
    with scope('w_s2'):
        wait_bytes(R2.at[:, 0], s2r.at[1])
    with scope('x1'):
        cross = lax.fori_loop(0, TILES, add_cross(1), cross, unroll=2)

    def signed(parts, bit):
        acc = parts[0]
        for index, part in enumerate(parts[1:], 1):
            acc = acc - part if (index >> bit) & 1 else acc + part
        return acc

    def z_copy(dist):
        dev = me + (dist // 4) * step_y + (dist // 2 % 2) * step_x + (dist % 2) * step_c
        return remote(V, VR.at[dist], zs, zr, dev)

    row_index = lax.broadcasted_iota(jnp.int32, (3 * SUB, LANES), 0)
    col_index = lax.broadcasted_iota(jnp.int32, (3 * SUB, LANES), 1)
    with scope('zsum'):
        signs = [plus_minus(bit).astype(F32) for bit in (bit_y, bit_x, bit_c)]
        norm_rows = [fold(part) for part in norms]
        tot_row = norm_rows[0] + norm_rows[1]
        rows = []
        for half, bit in enumerate(second_bit):
            weight_0, weight_1, mix_re, mix_im = pair_weights(matrix(half))
            re, im = cross[half]
            rows.append(jnp.where(bit == 1, weight_1, weight_0) * norm_rows[half] + mix_re * fold(re)
                        + (mix_im * signs[half]) * fold(im) + signs[half] * norm_rows[1 - half])
        rows += [signs[2] * tot_row] + raw_rows
        parts = [TP[tile(t), :] for t in range(TILES)]
        rows += [fold(signed(parts, bit)) for bit in reversed(range(4))]
        total = norms[0] + norms[1]
        rows += [fold(total * plus_minus((sub >> bit) & 1).astype(F32)) for bit in reversed(range(3))]
        rows += [tot_row * plus_minus((lane[:1] >> bit) & 1).astype(F32) for bit in reversed(range(7))]
        rows += [jnp.zeros_like(tot_row)] * 4
        column = jnp.sum(jnp.concatenate(rows, axis=0), axis=1, keepdims=True)
        mine = jnp.sum(jnp.where(row_index == col_index, column, 0.0), axis=0, keepdims=True)
        V[...] = mine
    for dist in reversed(range(1, DEVICES)):
        z_copy(dist).start()
    for piece in range(EARLY, len(PIECES) - 1):
        for half in range(2):
            stage2(half, 3, piece).start()
    with scope('own'):
        lax.fori_loop(0, TILES, step_own, 0)
        lax.fori_loop(0, TILES, step_mix, 0)
    with scope('w_s2'):
        wait_bytes(R2.at[:, 0], s2r.at[2])
    with scope('st2'):
        lax.fori_loop(0, TILES, add_received(2, tables[2], store_partial), 0)

    for piece in range(len(PIECES) - 1):
        low, high = PIECES[piece], PIECES[piece + 1]
        with scope('w_s2'):
            wait_bytes(R2.at[:, 0, :, low:high], s2r.at[3 + piece])
        with scope('tail'):
            lax.fori_loop(low // SUB, high // SUB, add_received(3, tables[3], store_out), 0)
        if piece == len(PIECES) - 3:
            with scope('w_z'):
                wait_bytes(VR.at[1:DEVICES], zr)
            acc = mine
            for dist in range(1, DEVICES):
                acc = acc + VR[dist]
            z_ref[...] = acc[:, :QUBITS] / 2 ** QUBITS

    with scope('w_send'):
        wait_bytes(BIG, sent_sem)
        wait_bytes(VR.at[1:DEVICES], zs)


def writer(state_ref, z_ref, state_out, z_out, sems):
    copies = [pltpu.make_async_copy(state_ref, state_out, sems.at[0]), pltpu.make_async_copy(z_ref, z_out, sems.at[1])]
    for copy in copies:
        copy.start()
    for copy in copies:
        copy.wait()


def solution(mesh):
    def local_layer(state_local, unitaries, cz_pairs):
        size = state_local.shape[1]
        rows = 2 * size // LANES
        x = state_local.reshape(2, -1, LANES).swapaxes(0, 1).reshape(rows, LANES)
        u = unitaries.transpose(0, 2, 3, 1).reshape(SUB, QUBITS)
        cz = cz_pairs.T
        x, u, cz = [pltpu.with_memory_space_constraint(v, pltpu.HBM) for v in (x, u, cz)]
        vm = pltpu.VMEM
        dma = pltpu.SemaphoreType.DMA
        halves = vm((2, CHUNKS, 2, ROWS, LANES), F32)
        square = vm((2 * LANES, 2 * LANES), F32)
        any_spec = pl.BlockSpec(memory_space=pl.ANY)
        shapes = (jax.ShapeDtypeStruct((rows, LANES), F32), jax.ShapeDtypeStruct((1, QUBITS), F32))
        out, z = pl.pallas_call(
            kernel,
            out_shape=shapes,
            in_specs=[pl.BlockSpec(memory_space=pltpu.HBM)] * 3,
            out_specs=(pl.BlockSpec(memory_space=pltpu.VMEM), pl.BlockSpec(memory_space=pltpu.VMEM)),
            scratch_shapes=[
                vm((4, rows, LANES), F32), pltpu.SMEM(u.shape, F32), pltpu.SMEM(cz.shape, jnp.int32), halves, halves, halves,
                vm((rows // 2, LANES), F32), square, square, square, square, vm((ROWS, LANES), F32),
                vm((1, LANES), F32), vm((DEVICES, 1, LANES), F32),
                dma((5,)), dma, dma((4,)), dma, dma((4,)), dma((3 + len(PIECES) - 1,)), dma, dma,
            ],
            compiler_params=pltpu.CompilerParams(collective_id=0, has_side_effects=True, vmem_limit_bytes=40 * 2 ** 20),
        )(x, u, cz)
        out, z = pl.pallas_call(
            writer, out_shape=shapes, in_specs=[any_spec] * 2, out_specs=(any_spec,) * 2, scratch_shapes=[dma((2,))],
            compiler_params=pltpu.CompilerParams(vmem_limit_bytes=2 ** 20),
        )(out, z)
        state = out.reshape(-1, 2, LANES).swapaxes(0, 1).reshape(2, size)
        return state, z.reshape(QUBITS)

    return jax.shard_map(local_layer, mesh=mesh, in_specs=(P(None, 'q'), P(), P()), out_specs=(P(None, 'q'), P()), check_vma=False)
```

```python
import jax
import jax.numpy as jnp
from jax import lax
from jax.experimental import pallas as pl
from jax.experimental.pallas import tpu as pltpu
from jax.sharding import PartitionSpec as P

MESH = pl.DeviceIdType.MESH
F32 = jnp.float32
LANES = 128
SUB = 8
TILES = 16
LOW, HIGH = slice(0, LANES), slice(LANES, 2 * LANES)
ROWS = SUB * TILES
CHUNK = 2 * ROWS
CHUNKS = 4
PIECES = (0, 24, 40, 72, 104, 128)
FIRST = CHUNK // 4
EARLY = 1
HELD = 2
DEVICES = 8
QUBITS = 20
scope = jax.named_scope


def cmul(a, b):
    (a_re, a_im), (b_re, b_im) = a, b
    return a_re * b_re - a_im * b_im, a_re * b_im + a_im * b_re


def cadd(a, b):
    (a_re, a_im), (b_re, b_im) = a, b
    return a_re + b_re, a_im + b_im


def conj_mul(a, b):
    (a_re, a_im), (b_re, b_im) = a, b
    return a_re * b_re + a_im * b_im, a_re * b_im - a_im * b_re


def mix(coefs, values):
    total = None
    for coef, value in zip(coefs, values):
        part = cmul(coef, value)
        total = part if total is None else cadd(total, part)
    return total


def gate(mat, zero, one):
    u00, u01, u10, u11 = mat
    return mix((u00, u01), (zero, one)), mix((u10, u11), (zero, one))


def norm(a):
    re, im = a
    return re * re + im * im


def plus_minus(bit):
    return 1 - 2 * bit


def planes(ref, half, chunk, rows):
    return [ref[half, chunk, part, rows, :] for part in range(2)]


def put(ref, half, chunk, rows, value):
    for part in range(2):
        ref[half, chunk, part, rows, :] = value[part]


def tile(t, first=0):
    return pl.ds(pl.multiple_of(first + SUB * t, SUB), SUB)


def kernel(x_hbm, u_hbm, cz_hbm, OUT, z_ref,
           BIG, u_ref, cz_ref, S, R2, T, SG, GM, KM, XC, ZC, TP, V, VR,
           ld, sent_sem, s1r, cpr, fwr, s2r, zs, zr):
    X, RB, XP, RP = [BIG.at[part] for part in range(4)]
    me = lax.axis_index('q')
    bit_y = me // 4
    bit_x = (me // 2) % 2
    bit_c = me % 2
    step_y, step_x, step_c = 4 * plus_minus(bit_y), 2 * plus_minus(bit_x), plus_minus(bit_c)
    dev_y, dev_x, dev_c = me + step_y, me + step_x, me + step_c
    first_dev = (dev_x, dev_y)
    second_dev = (dev_y, dev_x)
    second_bit = (bit_y, bit_x)

    def sent(half, k):
        return k + second_bit[half] * (3 - 2 * k)

    def received(half, k):
        return 3 - k + second_bit[half] * (2 * k - 3)

    def block_rows(half, chunk):
        return pl.ds(pl.multiple_of((half * CHUNKS + chunk) * CHUNK, CHUNK), CHUNK)

    def remote(src, dst, send, recv, dev):
        return pltpu.make_async_remote_copy(src_ref=src, dst_ref=dst, send_sem=send, recv_sem=recv,
                                            device_id=(dev,), device_id_type=MESH)

    def wait_bytes(ref, sem):
        pltpu.make_async_copy(ref, ref, sem).wait()

    def part_rows(half, k, part):
        low, size = ((0, FIRST), (FIRST, CHUNK - FIRST))[part] if k == 0 else (0, CHUNK)
        return pl.ds(pl.multiple_of((half * CHUNKS + sent(half, k)) * CHUNK + low, SUB), size)

    def load_copy(half, k, part=0):
        rows = part_rows(half, k, part)
        return pltpu.make_async_copy(x_hbm.at[rows], X.at[rows], ld.at[min(2, k + 1) if k else part])

    def stage1(half, k, part=0):
        rows = part_rows(half, k, part)
        return remote(X.at[rows], RB.at[rows], sent_sem, s1r.at[k], first_dev[half])

    def core_copy(half, k):
        rows = block_rows(half, sent(half, k))
        return remote(X.at[rows], XP.at[rows], sent_sem, cpr, dev_c)

    def forward(half, k):
        rows = block_rows(half, sent(half, k))
        return remote(RB.at[rows], RP.at[rows], sent_sem, fwr.at[k], dev_c)

    def stage2(half, k, piece=None):
        chunk = sent(half, k)
        if piece is None:
            return remote(S.at[half, chunk], R2.at[half, chunk], sent_sem, s2r.at[k], second_dev[half])
        rows = pl.ds(PIECES[piece], PIECES[piece + 1] - PIECES[piece])
        return remote(S.at[half, chunk, :, rows], R2.at[half, chunk, :, rows], sent_sem, s2r.at[3 + piece], second_dev[half])

    u_copy = pltpu.make_async_copy(u_hbm, u_ref, ld.at[3])
    cz_copy = pltpu.make_async_copy(cz_hbm, cz_ref, ld.at[4])
    barrier = pltpu.get_barrier_semaphore()
    for dev in (dev_x, dev_y, dev_c):
        pl.semaphore_signal(barrier, inc=1, device_id=(dev,), device_id_type=MESH)
    order = [(k, part) for k in range(CHUNKS) for part in range(1 if k else 2)]
    for k, part in order:
        for half in range(2):
            load_copy(half, k, part).start()
    u_copy.start()
    cz_copy.start()

    with scope('bar'):
        pl.semaphore_wait(barrier, 3)

    waits = {(0, 0): (0, 2 * FIRST), (0, 1): (1, 2 * (CHUNK - FIRST)), (1, 0): (2, 6 * CHUNK)}
    for k, part in order:
        if (k, part) in waits:
            index, size = waits[k, part]
            with scope('w_ld'):
                wait_bytes(X.at[:size], ld.at[index])
        for half in range(2):
            stage1(half, k, part).start()
    for k in range(CHUNKS):
        for half in range(2):
            core_copy(half, k).start()
    u_copy.wait()
    cz_copy.wait()

    def entry(qubit, row, col):
        return u_ref[row * 2 + col, qubit], u_ref[4 + row * 2 + col, qubit]

    def matrix(qubit, flip=0):
        return [entry(qubit, row + flip * plus_minus(row), col + flip * plus_minus(col)) for row in range(2) for col in range(2)]

    lane = lax.broadcasted_iota(jnp.int32, (SUB, LANES), 1)
    sub = lax.broadcasted_iota(jnp.int32, (SUB, LANES), 0)

    def build(t, carry):
        row = sub + SUB * t
        for base, left in ((6, True), (13, False)):
            re = im = None
            for j in range(7):
                shift = 6 - j
                row_bit = ((row >> shift) & 1) == 1
                col_bit = ((lane >> shift) & 1) == 1
                fac = []
                for ri in range(2):
                    u00, u01, u10, u11 = [u_ref[4 * ri + k, base + j] for k in range(4)]
                    if not left:
                        u01, u10 = u10, u01
                    fac.append(jnp.where(row_bit, jnp.where(col_bit, u11, u10), jnp.where(col_bit, u01, u00)))
                if re is None:
                    re, im = fac
                else:
                    re, im = cmul((re, im), fac)
            low, high = tile(t), tile(t, LANES)
            dest, upper, lower = (GM, -im, im) if left else (KM, im, -im)
            dest[low, LOW] = re
            dest[low, HIGH] = upper
            dest[high, LOW] = lower
            dest[high, HIGH] = re
        return carry

    with scope('build'):
        lax.fori_loop(0, TILES, build, 0)

    shifts = [[QUBITS - 1 - cz_ref[side, k] for side in range(2)] for k in range(QUBITS // 2)]

    def build_signs(t, carry):
        flat = (me * DEVICES * ROWS + sub + SUB * t) * LANES + lane
        parity = jnp.zeros_like(flat)
        for shift_a, shift_b in shifts:
            parity = parity ^ ((flat >> shift_a) & (flat >> shift_b))
        SG[tile(t), :] = plus_minus(parity & 1).astype(F32)
        return carry

    with scope('signs'):
        lax.fori_loop(0, DEVICES * TILES, build_signs, 0, unroll=4)

    def strided(ref, at):
        return [ref[pl.ds(at + part, SUB, stride=2), :] for part in range(2)]

    zero_tile = jnp.zeros((SUB, LANES), F32)
    zero_pair = (zero_tile, zero_tile)

    def raw_sums(t, carry):
        total, sums = carry
        value = [strided(X, pl.multiple_of(block * CHUNK + 2 * SUB * t, 2 * SUB)) for block in range(DEVICES)]
        dens = [norm(v) for v in value]
        done = []
        for (diff, cross), bit in zip(sums, (4, 2, 1)):
            for block in range(DEVICES):
                if block & bit:
                    diff = diff - dens[block]
                else:
                    diff = diff + dens[block]
                    cross = cadd(cross, conj_mul(value[block], value[block + bit]))
            done.append((diff, cross))
        for part in dens:
            total = total + part
        return total, tuple(done)

    with scope('raw'):
        raw_total, raw = lax.fori_loop(0, TILES, raw_sums, (zero_tile, ((zero_tile, zero_pair),) * 3))

    def fold(part):
        return jnp.sum(part, axis=0, keepdims=True)

    def pair_weights(mat):
        u00, u01, u10, u11 = mat
        (a_re, a_im), (b_re, b_im) = conj_mul(u00, u01), conj_mul(u10, u11)
        return norm(u00) - norm(u10), norm(u01) - norm(u11), 2 * (a_re - b_re), 2 * (b_im - a_im)

    raw_rows = []
    raw_total = fold(raw_total)
    for qubit, (diff, (re, im)) in zip((3, 4, 5), raw):
        weight_0, weight_1, mix_re, mix_im = pair_weights(matrix(qubit))
        even, odd = raw_total + fold(diff), raw_total - fold(diff)
        raw_rows.append((weight_0 * even + weight_1 * odd) / 2 + mix_re * fold(re) + mix_im * fold(im))

    def gate_pair(qubit, own_bit):
        return entry(qubit, own_bit, own_bit), entry(qubit, own_bit, 1 - own_bit)

    coef_y = gate_pair(0, bit_y)
    coef_x = gate_pair(1, bit_x)
    coef_c = gate_pair(2, bit_c)
    stage1_coefs = [[cmul(top, core) for core in coef_c for top in coef] for coef in (coef_x, coef_y)]

    norms = zero_pair
    for k in range(CHUNKS):
        with scope('w_s1'):
            wait_bytes(RB.at[0:2 * CHUNK], s1r.at[k])
        for half in range(2):
            forward(half, k).start()
        if k:
            for half in range(2):
                stage2(half, k - 1).start()
        if k == 0:
            wait_bytes(XP, cpr)
        with scope('w_fw'):
            wait_bytes(RP.at[0:2 * CHUNK], fwr.at[k])

        for half in range(2):
            coefs = stage1_coefs[half]
            base = (half * CHUNKS + sent(half, k)) * CHUNK

            def combine(t, carry, base=base, coefs=coefs, half=half):
                at = pl.multiple_of(base + 2 * SUB * t, 2 * SUB)
                re, im = mix(coefs, [strided(ref, at) for ref in (X, RB, XP, RP)])
                XC[tile(t), (LOW, HIGH)[half]] = re
                XC[tile(t, LANES), (LOW, HIGH)[half]] = im
                return carry

            with scope('comb'):
                lax.fori_loop(0, TILES, combine, 0, unroll=2)
        with scope('mm'):
            left = lax.dot(GM[...], XC[...], precision=lax.Precision.HIGHEST, preferred_element_type=F32)
            for rows in (LOW, HIGH):
                for cols in (LOW, HIGH):
                    ZC[cols, rows] = left[rows, cols]
            both = lax.dot(ZC[...], KM[...], precision=lax.Precision.HIGHEST, preferred_element_type=F32)
            for half in range(2):
                for part in range(2):
                    S[half, sent(half, k), part] = both[(LOW, HIGH)[half], (LOW, HIGH)[part]]

        def mid_sums(t, sums, k=k):
            dens = [norm(planes(S, half, sent(half, k), tile(t))) for half in range(2)]
            row = dens[0] + dens[1]
            TP[tile(t), :] = row if k == 0 else TP[tile(t), :] + row
            return tuple(a + b for a, b in zip(sums, dens))

        with scope('dens'):
            norms = lax.fori_loop(0, TILES, mid_sums, norms, unroll=2)

    flips = (1 - bit_y, 1 - bit_x)
    u3 = matrix(3)
    u4 = [matrix(4, flip) for flip in flips]
    u5 = [matrix(5, flip) for flip in flips]
    second_coef = (coef_y, coef_x)

    def weights(k):
        table = {}
        for half in range(2):
            index = received(half, k)
            for chunk in range(CHUNKS):
                inner = cmul(entry(4, chunk // 2, index // 2), entry(5, chunk % 2, index % 2))
                inner = cmul(second_coef[half][1], inner)
                for side in range(2):
                    table[side, chunk, half] = cmul(u3[2 * side + half], inner)
        return table

    def add_cross(k):
        def body(t, cross):
            done = []
            for half in range(2):
                chunk = received(half, k)
                part = conj_mul(planes(S, half, chunk, tile(t)), planes(R2, half, chunk, tile(t)))
                done.append(cadd(cross[half], part))
            return tuple(done)
        return body

    def step_own(t, carry):
        rows = tile(t)
        for half in range(2):
            own, other = second_coef[half]
            value = []
            for k in range(CHUNKS):
                chunk = received(half, k)
                part = cmul(own, planes(S, half, chunk, rows))
                value.append(cadd(part, cmul(other, planes(R2, half, chunk, rows))) if k < 2 else part)
            value = [v for pair in (value[:2], value[2:]) for v in gate(u5[half], *pair)]
            value = [gate(u4[half], value[k], value[k + 2]) for k in range(2)]
            for k in range(CHUNKS):
                put(T, half, received(half, k), rows, value[k % 2][k // 2])
        return carry

    def step_mix(t, carry):
        rows = tile(t)
        for chunk in range(CHUNKS):
            for half, value in enumerate(gate(u3, planes(T, 0, chunk, rows), planes(T, 1, chunk, rows))):
                put(T, half, chunk, rows, value)
        return carry

    def add_received(k, table, store):
        def body(t, carry):
            rows = tile(t)
            other = [planes(R2, half, received(half, k), rows) for half in range(2)]
            for side in range(2):
                for chunk in range(CHUNKS):
                    value = planes(T, side, chunk, rows)
                    for half in range(2):
                        value = cadd(value, cmul(table[side, chunk, half], other[half]))
                    store(side, chunk, t, value)
            return carry
        return body

    def store_partial(side, chunk, t, value):
        put(T, side, chunk, tile(t), value)

    def store_out(side, chunk, t, value):
        block = side * CHUNKS + chunk
        sign = SG[tile(t, block * ROWS), :]
        at = pl.multiple_of(block * CHUNK + 2 * SUB * t, 2 * SUB)
        for part in range(2):
            OUT[pl.ds(at + part, SUB, stride=2), :] = value[part] * sign

    tables = {k: weights(k) for k in (2, 3)}
    cross = (zero_pair, zero_pair)
    with scope('w_s2'):
        wait_bytes(R2.at[:, 0], s2r.at[0])
    for piece in range(EARLY):
        for half in range(2):
            stage2(half, 3, piece).start()
    with scope('x0'):
        cross = lax.fori_loop(0, TILES, add_cross(0), cross, unroll=2)
    with scope('w_s2'):
        wait_bytes(R2.at[:, 0], s2r.at[1])
    with scope('x1'):
        cross = lax.fori_loop(0, TILES, add_cross(1), cross, unroll=2)

    def signed(parts, bit):
        acc = parts[0]
        for index, part in enumerate(parts[1:], 1):
            acc = acc - part if (index >> bit) & 1 else acc + part
        return acc

    def z_copy(dist):
        dev = me + (dist // 4) * step_y + (dist // 2 % 2) * step_x + (dist % 2) * step_c
        return remote(V, VR.at[dist], zs, zr, dev)

    row_index = lax.broadcasted_iota(jnp.int32, (3 * SUB, LANES), 0)
    col_index = lax.broadcasted_iota(jnp.int32, (3 * SUB, LANES), 1)
    with scope('zsum'):
        signs = [plus_minus(bit).astype(F32) for bit in (bit_y, bit_x, bit_c)]
        norm_rows = [fold(part) for part in norms]
        tot_row = norm_rows[0] + norm_rows[1]
        rows = []
        for half, bit in enumerate(second_bit):
            weight_0, weight_1, mix_re, mix_im = pair_weights(matrix(half))
            re, im = cross[half]
            rows.append(jnp.where(bit == 1, weight_1, weight_0) * norm_rows[half] + mix_re * fold(re)
                        + (mix_im * signs[half]) * fold(im) + signs[half] * norm_rows[1 - half])
        rows += [signs[2] * tot_row] + raw_rows
        parts = [TP[tile(t), :] for t in range(TILES)]
        rows += [fold(signed(parts, bit)) for bit in reversed(range(4))]
        total = norms[0] + norms[1]
        rows += [fold(total * plus_minus((sub >> bit) & 1).astype(F32)) for bit in reversed(range(3))]
        rows += [tot_row * plus_minus((lane[:1] >> bit) & 1).astype(F32) for bit in reversed(range(7))]
        rows += [jnp.zeros_like(tot_row)] * 4
        column = jnp.sum(jnp.concatenate(rows, axis=0), axis=1, keepdims=True)
        mine = jnp.sum(jnp.where(row_index == col_index, column, 0.0), axis=0, keepdims=True)
        V[...] = mine
    for dist in reversed(range(1, DEVICES)):
        z_copy(dist).start()
    def send_pieces(low, high):
        for piece in range(low, high):
            for half in range(2):
                stage2(half, 3, piece).start()

    send_pieces(EARLY, HELD)
    pl.when(bit_c == 0)(lambda: send_pieces(HELD, len(PIECES) - 1))
    with scope('own'):
        lax.fori_loop(0, TILES, step_own, 0)
        lax.fori_loop(0, TILES, step_mix, 0)
    with scope('w_s2'):
        wait_bytes(R2.at[:, 0], s2r.at[2])
    with scope('st2'):
        lax.fori_loop(0, TILES, add_received(2, tables[2], store_partial), 0)

    for piece in range(len(PIECES) - 1):
        low, high = PIECES[piece], PIECES[piece + 1]
        with scope('w_s2'):
            wait_bytes(R2.at[:, 0, :, low:high], s2r.at[3 + piece])
        if piece == 1:
            pl.when(bit_c == 1)(lambda: send_pieces(HELD, len(PIECES) - 1))
        with scope('tail'):
            lax.fori_loop(low // SUB, high // SUB, add_received(3, tables[3], store_out), 0)
        if piece == len(PIECES) - 3:
            with scope('w_z'):
                wait_bytes(VR.at[1:DEVICES], zr)
            acc = mine
            for dist in range(1, DEVICES):
                acc = acc + VR[dist]
            z_ref[...] = acc[:, :QUBITS] / 2 ** QUBITS

    with scope('w_send'):
        wait_bytes(BIG, sent_sem)
        wait_bytes(VR.at[1:DEVICES], zs)


def writer(state_ref, z_ref, state_out, z_out, sems):
    copies = [pltpu.make_async_copy(state_ref, state_out, sems.at[0]), pltpu.make_async_copy(z_ref, z_out, sems.at[1])]
    for copy in copies:
        copy.start()
    for copy in copies:
        copy.wait()


def solution(mesh):
    def local_layer(state_local, unitaries, cz_pairs):
        size = state_local.shape[1]
        rows = 2 * size // LANES
        x = state_local.reshape(2, -1, LANES).swapaxes(0, 1).reshape(rows, LANES)
        u = unitaries.transpose(0, 2, 3, 1).reshape(SUB, QUBITS)
        cz = cz_pairs.T
        x, u, cz = [pltpu.with_memory_space_constraint(v, pltpu.HBM) for v in (x, u, cz)]
        vm = pltpu.VMEM
        dma = pltpu.SemaphoreType.DMA
        halves = vm((2, CHUNKS, 2, ROWS, LANES), F32)
        square = vm((2 * LANES, 2 * LANES), F32)
        any_spec = pl.BlockSpec(memory_space=pl.ANY)
        shapes = (jax.ShapeDtypeStruct((rows, LANES), F32), jax.ShapeDtypeStruct((1, QUBITS), F32))
        out, z = pl.pallas_call(
            kernel,
            out_shape=shapes,
            in_specs=[pl.BlockSpec(memory_space=pltpu.HBM)] * 3,
            out_specs=(pl.BlockSpec(memory_space=pltpu.VMEM), pl.BlockSpec(memory_space=pltpu.VMEM)),
            scratch_shapes=[
                vm((4, rows, LANES), F32), pltpu.SMEM(u.shape, F32), pltpu.SMEM(cz.shape, jnp.int32), halves, halves, halves,
                vm((rows // 2, LANES), F32), square, square, square, square, vm((ROWS, LANES), F32),
                vm((1, LANES), F32), vm((DEVICES, 1, LANES), F32),
                dma((5,)), dma, dma((4,)), dma, dma((4,)), dma((3 + len(PIECES) - 1,)), dma, dma,
            ],
            compiler_params=pltpu.CompilerParams(collective_id=0, has_side_effects=True, vmem_limit_bytes=40 * 2 ** 20),
        )(x, u, cz)
        out, z = pl.pallas_call(
            writer, out_shape=shapes, in_specs=[any_spec] * 2, out_specs=(any_spec,) * 2, scratch_shapes=[dma((2,))],
            compiler_params=pltpu.CompilerParams(vmem_limit_bytes=2 ** 20),
        )(out, z)
        state = out.reshape(-1, 2, LANES).swapaxes(0, 1).reshape(2, size)
        return state, z.reshape(QUBITS)

    return jax.shard_map(local_layer, mesh=mesh, in_specs=(P(None, 'q'), P(), P()), out_specs=(P(None, 'q'), P()), check_vma=False)
```

```python
import jax
import jax.numpy as jnp
from jax import lax
from jax.experimental import pallas as pl
from jax.experimental.pallas import tpu as pltpu
from jax.sharding import PartitionSpec as P

MESH = pl.DeviceIdType.MESH
F32 = jnp.float32
LANES = 128
SUB = 8
TILES = 16
LOW, HIGH = slice(0, LANES), slice(LANES, 2 * LANES)
ROWS = SUB * TILES
CHUNK = 2 * ROWS
CHUNKS = 4
PIECES = (0, 24, 40, 72, 104, 128)
FIRST = CHUNK // 4
EARLY = 1
DEVICES = 8
QUBITS = 20
scope = jax.named_scope


def cmul(a, b):
    (a_re, a_im), (b_re, b_im) = a, b
    return a_re * b_re - a_im * b_im, a_re * b_im + a_im * b_re


def cadd(a, b):
    (a_re, a_im), (b_re, b_im) = a, b
    return a_re + b_re, a_im + b_im


def conj_mul(a, b):
    (a_re, a_im), (b_re, b_im) = a, b
    return a_re * b_re + a_im * b_im, a_re * b_im - a_im * b_re


def mix(coefs, values):
    total = None
    for coef, value in zip(coefs, values):
        part = cmul(coef, value)
        total = part if total is None else cadd(total, part)
    return total


def gate(mat, zero, one):
    u00, u01, u10, u11 = mat
    return mix((u00, u01), (zero, one)), mix((u10, u11), (zero, one))


def norm(a):
    re, im = a
    return re * re + im * im


def plus_minus(bit):
    return 1 - 2 * bit


def planes(ref, half, chunk, rows):
    return [ref[half, chunk, part, rows, :] for part in range(2)]


def put(ref, half, chunk, rows, value):
    for part in range(2):
        ref[half, chunk, part, rows, :] = value[part]


def tile(t, first=0):
    return pl.ds(pl.multiple_of(first + SUB * t, SUB), SUB)


def kernel(x_hbm, u_hbm, cz_hbm, OUT, z_ref,
           BIG, u_ref, cz_ref, S, R2, T, SG, GM, KM, XC, ZC, TP, V, VR,
           ld, sent_sem, s1r, cpr, fwr, s2r, zs, zr, ready):
    X, RB, XP, RP = [BIG.at[part] for part in range(4)]
    me = lax.axis_index('q')
    bit_y = me // 4
    bit_x = (me // 2) % 2
    bit_c = me % 2
    step_y, step_x, step_c = 4 * plus_minus(bit_y), 2 * plus_minus(bit_x), plus_minus(bit_c)
    dev_y, dev_x, dev_c = me + step_y, me + step_x, me + step_c
    first_dev = (dev_x, dev_y)
    second_dev = (dev_y, dev_x)
    second_bit = (bit_y, bit_x)

    def sent(half, k):
        return k + second_bit[half] * (3 - 2 * k)

    def received(half, k):
        return 3 - k + second_bit[half] * (2 * k - 3)

    def block_rows(half, chunk):
        return pl.ds(pl.multiple_of((half * CHUNKS + chunk) * CHUNK, CHUNK), CHUNK)

    def remote(src, dst, send, recv, dev):
        return pltpu.make_async_remote_copy(src_ref=src, dst_ref=dst, send_sem=send, recv_sem=recv,
                                            device_id=(dev,), device_id_type=MESH)

    def wait_bytes(ref, sem):
        pltpu.make_async_copy(ref, ref, sem).wait()

    def part_rows(half, k, part):
        low, size = ((0, FIRST), (FIRST, CHUNK - FIRST))[part] if k == 0 else (0, CHUNK)
        return pl.ds(pl.multiple_of((half * CHUNKS + sent(half, k)) * CHUNK + low, SUB), size)

    def load_copy(half, k, part=0):
        rows = part_rows(half, k, part)
        return pltpu.make_async_copy(x_hbm.at[rows], X.at[rows], ld.at[min(2, k + 1) if k else part])

    def stage1(half, k, part=0):
        rows = part_rows(half, k, part)
        return remote(X.at[rows], RB.at[rows], sent_sem, s1r.at[k], first_dev[half])

    def core_copy(half, k):
        rows = block_rows(half, sent(half, k))
        return remote(X.at[rows], XP.at[rows], sent_sem, cpr, dev_c)

    def forward(half, k):
        rows = block_rows(half, sent(half, k))
        return remote(RB.at[rows], RP.at[rows], sent_sem, fwr.at[k], dev_c)

    def stage2(half, k, piece=None):
        chunk = sent(half, k)
        if piece is None:
            return remote(S.at[half, chunk], R2.at[half, chunk], sent_sem, s2r.at[k], second_dev[half])
        rows = pl.ds(PIECES[piece], PIECES[piece + 1] - PIECES[piece])
        return remote(S.at[half, chunk, :, rows], R2.at[half, chunk, :, rows], sent_sem, s2r.at[3 + piece], second_dev[half])

    u_copy = pltpu.make_async_copy(u_hbm, u_ref, ld.at[3])
    cz_copy = pltpu.make_async_copy(cz_hbm, cz_ref, ld.at[4])
    last_chip = bit_y * bit_x
    beside = bit_y + bit_x - 2 * last_chip
    barrier = pltpu.get_barrier_semaphore()

    def signal(sem, devices):
        for dev in devices:
            pl.semaphore_signal(sem, inc=1, device_id=(dev,), device_id_type=MESH)

    signal(barrier, (dev_c,))
    pl.when(last_chip == 0)(lambda: signal(barrier, (dev_x, dev_y)))
    order = [(k, part) for k in range(CHUNKS) for part in range(1 if k else 2)]
    for k, part in order:
        for half in range(2):
            load_copy(half, k, part).start()
    u_copy.start()
    cz_copy.start()

    waits = {(0, 0): (0, 2 * FIRST), (0, 1): (1, 2 * (CHUNK - FIRST)), (1, 0): (2, 6 * CHUNK)}

    def send_first(halves, wait):
        for k, part in order:
            if wait and (k, part) in waits:
                index, size = waits[k, part]
                wait_bytes(X.at[:size], ld.at[index])
            if k == 0:
                for half in halves:
                    stage1(half, k, part).start()
        pl.when(bit_c == 0)(lambda: send_rest(halves))

    def send_rest(halves):
        for k in range(1, CHUNKS):
            for half in halves:
                stage1(half, k).start()

    def send_beside(half):
        send_first((half,), True)
        with scope('w_rdy'):
            pl.semaphore_wait(ready, 1)
        send_first((1 - half,), False)

    with scope('bar'):
        pl.when(beside == 1)(lambda: pl.semaphore_wait(barrier, 2))
        pl.when(beside == 0)(lambda: pl.semaphore_wait(barrier, 3))
    pl.when(last_chip == 1)(lambda: signal(ready, (dev_x, dev_y)))
    with scope('first'):
        pl.when(beside == 0)(lambda: send_first((0, 1), True))
        pl.when(beside * bit_x == 1)(lambda: send_beside(0))
        pl.when(beside * bit_y == 1)(lambda: send_beside(1))
    for k in range(CHUNKS):
        for half in range(2):
            core_copy(half, k).start()
    u_copy.wait()
    cz_copy.wait()

    def entry(qubit, row, col):
        return u_ref[row * 2 + col, qubit], u_ref[4 + row * 2 + col, qubit]

    def matrix(qubit, flip=0):
        return [entry(qubit, row + flip * plus_minus(row), col + flip * plus_minus(col)) for row in range(2) for col in range(2)]

    lane = lax.broadcasted_iota(jnp.int32, (SUB, LANES), 1)
    sub = lax.broadcasted_iota(jnp.int32, (SUB, LANES), 0)

    def build(t, carry):
        row = sub + SUB * t
        for base, left in ((6, True), (13, False)):
            re = im = None
            for j in range(7):
                shift = 6 - j
                row_bit = ((row >> shift) & 1) == 1
                col_bit = ((lane >> shift) & 1) == 1
                fac = []
                for ri in range(2):
                    u00, u01, u10, u11 = [u_ref[4 * ri + k, base + j] for k in range(4)]
                    if not left:
                        u01, u10 = u10, u01
                    fac.append(jnp.where(row_bit, jnp.where(col_bit, u11, u10), jnp.where(col_bit, u01, u00)))
                if re is None:
                    re, im = fac
                else:
                    re, im = cmul((re, im), fac)
            low, high = tile(t), tile(t, LANES)
            dest, upper, lower = (GM, -im, im) if left else (KM, im, -im)
            dest[low, LOW] = re
            dest[low, HIGH] = upper
            dest[high, LOW] = lower
            dest[high, HIGH] = re
        return carry

    with scope('build'):
        lax.fori_loop(0, TILES, build, 0)

    shifts = [[QUBITS - 1 - cz_ref[side, k] for side in range(2)] for k in range(QUBITS // 2)]

    def build_signs(t, carry):
        flat = (me * DEVICES * ROWS + sub + SUB * t) * LANES + lane
        parity = jnp.zeros_like(flat)
        for shift_a, shift_b in shifts:
            parity = parity ^ ((flat >> shift_a) & (flat >> shift_b))
        SG[tile(t), :] = plus_minus(parity & 1).astype(F32)
        return carry

    with scope('signs'):
        lax.fori_loop(0, DEVICES * TILES, build_signs, 0, unroll=4)

    def strided(ref, at):
        return [ref[pl.ds(at + part, SUB, stride=2), :] for part in range(2)]

    zero_tile = jnp.zeros((SUB, LANES), F32)
    zero_pair = (zero_tile, zero_tile)

    def raw_sums(t, carry):
        total, sums = carry
        value = [strided(X, pl.multiple_of(block * CHUNK + 2 * SUB * t, 2 * SUB)) for block in range(DEVICES)]
        dens = [norm(v) for v in value]
        done = []
        for (diff, cross), bit in zip(sums, (4, 2, 1)):
            for block in range(DEVICES):
                if block & bit:
                    diff = diff - dens[block]
                else:
                    diff = diff + dens[block]
                    cross = cadd(cross, conj_mul(value[block], value[block + bit]))
            done.append((diff, cross))
        for part in dens:
            total = total + part
        return total, tuple(done)

    with scope('raw'):
        raw_total, raw = lax.fori_loop(0, TILES, raw_sums, (zero_tile, ((zero_tile, zero_pair),) * 3))

    def fold(part):
        return jnp.sum(part, axis=0, keepdims=True)

    def pair_weights(mat):
        u00, u01, u10, u11 = mat
        (a_re, a_im), (b_re, b_im) = conj_mul(u00, u01), conj_mul(u10, u11)
        return norm(u00) - norm(u10), norm(u01) - norm(u11), 2 * (a_re - b_re), 2 * (b_im - a_im)

    raw_rows = []
    raw_total = fold(raw_total)
    for qubit, (diff, (re, im)) in zip((3, 4, 5), raw):
        weight_0, weight_1, mix_re, mix_im = pair_weights(matrix(qubit))
        even, odd = raw_total + fold(diff), raw_total - fold(diff)
        raw_rows.append((weight_0 * even + weight_1 * odd) / 2 + mix_re * fold(re) + mix_im * fold(im))

    def gate_pair(qubit, own_bit):
        return entry(qubit, own_bit, own_bit), entry(qubit, own_bit, 1 - own_bit)

    coef_y = gate_pair(0, bit_y)
    coef_x = gate_pair(1, bit_x)
    coef_c = gate_pair(2, bit_c)
    stage1_coefs = [[cmul(top, core) for core in coef_c for top in coef] for coef in (coef_x, coef_y)]

    norms = zero_pair
    for k in range(CHUNKS):
        with scope('w_s1'):
            wait_bytes(RB.at[0:2 * CHUNK], s1r.at[k])
        for half in range(2):
            forward(half, k).start()
        if k == 0:
            pl.when(bit_c == 1)(lambda: send_rest((0, 1)))
        else:
            for half in range(2):
                stage2(half, k - 1).start()
        if k == 0:
            wait_bytes(XP, cpr)
        with scope('w_fw'):
            wait_bytes(RP.at[0:2 * CHUNK], fwr.at[k])

        for half in range(2):
            coefs = stage1_coefs[half]
            base = (half * CHUNKS + sent(half, k)) * CHUNK

            def combine(t, carry, base=base, coefs=coefs, half=half):
                at = pl.multiple_of(base + 2 * SUB * t, 2 * SUB)
                re, im = mix(coefs, [strided(ref, at) for ref in (X, RB, XP, RP)])
                XC[tile(t), (LOW, HIGH)[half]] = re
                XC[tile(t, LANES), (LOW, HIGH)[half]] = im
                return carry

            with scope('comb'):
                lax.fori_loop(0, TILES, combine, 0, unroll=2)
        with scope('mm'):
            left = lax.dot(GM[...], XC[...], precision=lax.Precision.HIGHEST, preferred_element_type=F32)
            for rows in (LOW, HIGH):
                for cols in (LOW, HIGH):
                    ZC[cols, rows] = left[rows, cols]
            both = lax.dot(ZC[...], KM[...], precision=lax.Precision.HIGHEST, preferred_element_type=F32)
            for half in range(2):
                for part in range(2):
                    S[half, sent(half, k), part] = both[(LOW, HIGH)[half], (LOW, HIGH)[part]]

        def mid_sums(t, sums, k=k):
            dens = [norm(planes(S, half, sent(half, k), tile(t))) for half in range(2)]
            row = dens[0] + dens[1]
            TP[tile(t), :] = row if k == 0 else TP[tile(t), :] + row
            return tuple(a + b for a, b in zip(sums, dens))

        with scope('dens'):
            norms = lax.fori_loop(0, TILES, mid_sums, norms, unroll=2)

    flips = (1 - bit_y, 1 - bit_x)
    u3 = matrix(3)
    u4 = [matrix(4, flip) for flip in flips]
    u5 = [matrix(5, flip) for flip in flips]
    second_coef = (coef_y, coef_x)

    def weights(k):
        table = {}
        for half in range(2):
            index = received(half, k)
            for chunk in range(CHUNKS):
                inner = cmul(entry(4, chunk // 2, index // 2), entry(5, chunk % 2, index % 2))
                inner = cmul(second_coef[half][1], inner)
                for side in range(2):
                    table[side, chunk, half] = cmul(u3[2 * side + half], inner)
        return table

    def add_cross(k):
        def body(t, cross):
            done = []
            for half in range(2):
                chunk = received(half, k)
                part = conj_mul(planes(S, half, chunk, tile(t)), planes(R2, half, chunk, tile(t)))
                done.append(cadd(cross[half], part))
            return tuple(done)
        return body

    def step_own(t, carry):
        rows = tile(t)
        for half in range(2):
            own, other = second_coef[half]
            value = []
            for k in range(CHUNKS):
                chunk = received(half, k)
                part = cmul(own, planes(S, half, chunk, rows))
                value.append(cadd(part, cmul(other, planes(R2, half, chunk, rows))) if k < 2 else part)
            value = [v for pair in (value[:2], value[2:]) for v in gate(u5[half], *pair)]
            value = [gate(u4[half], value[k], value[k + 2]) for k in range(2)]
            for k in range(CHUNKS):
                put(T, half, received(half, k), rows, value[k % 2][k // 2])
        return carry

    def step_mix(t, carry):
        rows = tile(t)
        for chunk in range(CHUNKS):
            for half, value in enumerate(gate(u3, planes(T, 0, chunk, rows), planes(T, 1, chunk, rows))):
                put(T, half, chunk, rows, value)
        return carry

    def add_received(k, table, store):
        def body(t, carry):
            rows = tile(t)
            other = [planes(R2, half, received(half, k), rows) for half in range(2)]
            for side in range(2):
                for chunk in range(CHUNKS):
                    value = planes(T, side, chunk, rows)
                    for half in range(2):
                        value = cadd(value, cmul(table[side, chunk, half], other[half]))
                    store(side, chunk, t, value)
            return carry
        return body

    def store_partial(side, chunk, t, value):
        put(T, side, chunk, tile(t), value)

    def store_out(side, chunk, t, value):
        block = side * CHUNKS + chunk
        sign = SG[tile(t, block * ROWS), :]
        at = pl.multiple_of(block * CHUNK + 2 * SUB * t, 2 * SUB)
        for part in range(2):
            OUT[pl.ds(at + part, SUB, stride=2), :] = value[part] * sign

    tables = {k: weights(k) for k in (2, 3)}
    cross = (zero_pair, zero_pair)
    with scope('w_s2'):
        wait_bytes(R2.at[:, 0], s2r.at[0])
    for piece in range(EARLY):
        for half in range(2):
            stage2(half, 3, piece).start()
    with scope('x0'):
        cross = lax.fori_loop(0, TILES, add_cross(0), cross, unroll=2)
    with scope('w_s2'):
        wait_bytes(R2.at[:, 0], s2r.at[1])
    with scope('x1'):
        cross = lax.fori_loop(0, TILES, add_cross(1), cross, unroll=2)

    def signed(parts, bit):
        acc = parts[0]
        for index, part in enumerate(parts[1:], 1):
            acc = acc - part if (index >> bit) & 1 else acc + part
        return acc

    def z_copy(dist):
        dev = me + (dist // 4) * step_y + (dist // 2 % 2) * step_x + (dist % 2) * step_c
        return remote(V, VR.at[dist], zs, zr, dev)

    row_index = lax.broadcasted_iota(jnp.int32, (3 * SUB, LANES), 0)
    col_index = lax.broadcasted_iota(jnp.int32, (3 * SUB, LANES), 1)
    with scope('zsum'):
        signs = [plus_minus(bit).astype(F32) for bit in (bit_y, bit_x, bit_c)]
        norm_rows = [fold(part) for part in norms]
        tot_row = norm_rows[0] + norm_rows[1]
        rows = []
        for half, bit in enumerate(second_bit):
            weight_0, weight_1, mix_re, mix_im = pair_weights(matrix(half))
            re, im = cross[half]
            rows.append(jnp.where(bit == 1, weight_1, weight_0) * norm_rows[half] + mix_re * fold(re)
                        + (mix_im * signs[half]) * fold(im) + signs[half] * norm_rows[1 - half])
        rows += [signs[2] * tot_row] + raw_rows
        parts = [TP[tile(t), :] for t in range(TILES)]
        rows += [fold(signed(parts, bit)) for bit in reversed(range(4))]
        total = norms[0] + norms[1]
        rows += [fold(total * plus_minus((sub >> bit) & 1).astype(F32)) for bit in reversed(range(3))]
        rows += [tot_row * plus_minus((lane[:1] >> bit) & 1).astype(F32) for bit in reversed(range(7))]
        rows += [jnp.zeros_like(tot_row)] * 4
        column = jnp.sum(jnp.concatenate(rows, axis=0), axis=1, keepdims=True)
        mine = jnp.sum(jnp.where(row_index == col_index, column, 0.0), axis=0, keepdims=True)
        V[...] = mine
    for dist in reversed(range(1, DEVICES)):
        z_copy(dist).start()
    def send_pieces(low, high):
        for piece in range(low, high):
            for half in range(2):
                stage2(half, 3, piece).start()

    send_pieces(EARLY, len(PIECES) - 1)
    with scope('own'):
        lax.fori_loop(0, TILES, step_own, 0)
        lax.fori_loop(0, TILES, step_mix, 0)
    with scope('w_s2'):
        wait_bytes(R2.at[:, 0], s2r.at[2])
    with scope('st2'):
        lax.fori_loop(0, TILES, add_received(2, tables[2], store_partial), 0)

    for piece in range(len(PIECES) - 1):
        low, high = PIECES[piece], PIECES[piece + 1]
        with scope('w_s2'):
            wait_bytes(R2.at[:, 0, :, low:high], s2r.at[3 + piece])
        with scope('tail'):
            lax.fori_loop(low // SUB, high // SUB, add_received(3, tables[3], store_out), 0)
        if piece == len(PIECES) - 3:
            with scope('w_z'):
                wait_bytes(VR.at[1:DEVICES], zr)
            acc = mine
            for dist in range(1, DEVICES):
                acc = acc + VR[dist]
            z_ref[...] = acc[:, :QUBITS] / 2 ** QUBITS

    with scope('w_send'):
        wait_bytes(BIG, sent_sem)
        wait_bytes(VR.at[1:DEVICES], zs)


def writer(state_ref, z_ref, state_out, z_out, sems):
    copies = [pltpu.make_async_copy(state_ref, state_out, sems.at[0]), pltpu.make_async_copy(z_ref, z_out, sems.at[1])]
    for copy in copies:
        copy.start()
    for copy in copies:
        copy.wait()


def solution(mesh):
    def local_layer(state_local, unitaries, cz_pairs):
        size = state_local.shape[1]
        rows = 2 * size // LANES
        x = state_local.reshape(2, -1, LANES).swapaxes(0, 1).reshape(rows, LANES)
        u = unitaries.transpose(0, 2, 3, 1).reshape(SUB, QUBITS)
        cz = cz_pairs.T
        x, u, cz = [pltpu.with_memory_space_constraint(v, pltpu.HBM) for v in (x, u, cz)]
        vm = pltpu.VMEM
        dma = pltpu.SemaphoreType.DMA
        halves = vm((2, CHUNKS, 2, ROWS, LANES), F32)
        square = vm((2 * LANES, 2 * LANES), F32)
        any_spec = pl.BlockSpec(memory_space=pl.ANY)
        shapes = (jax.ShapeDtypeStruct((rows, LANES), F32), jax.ShapeDtypeStruct((1, QUBITS), F32))
        out, z = pl.pallas_call(
            kernel,
            out_shape=shapes,
            in_specs=[pl.BlockSpec(memory_space=pltpu.HBM)] * 3,
            out_specs=(pl.BlockSpec(memory_space=pltpu.VMEM), pl.BlockSpec(memory_space=pltpu.VMEM)),
            scratch_shapes=[
                vm((4, rows, LANES), F32), pltpu.SMEM(u.shape, F32), pltpu.SMEM(cz.shape, jnp.int32), halves, halves, halves,
                vm((rows // 2, LANES), F32), square, square, square, square, vm((ROWS, LANES), F32),
                vm((1, LANES), F32), vm((DEVICES, 1, LANES), F32),
                dma((5,)), dma, dma((4,)), dma, dma((4,)), dma((3 + len(PIECES) - 1,)), dma, dma, pltpu.SemaphoreType.REGULAR,
            ],
            compiler_params=pltpu.CompilerParams(collective_id=0, has_side_effects=True, vmem_limit_bytes=40 * 2 ** 20),
        )(x, u, cz)
        out, z = pl.pallas_call(
            writer, out_shape=shapes, in_specs=[any_spec] * 2, out_specs=(any_spec,) * 2, scratch_shapes=[dma((2,))],
            compiler_params=pltpu.CompilerParams(vmem_limit_bytes=2 ** 20),
        )(out, z)
        state = out.reshape(-1, 2, LANES).swapaxes(0, 1).reshape(2, size)
        return state, z.reshape(QUBITS)

    return jax.shard_map(local_layer, mesh=mesh, in_specs=(P(None, 'q'), P(), P()), out_specs=(P(None, 'q'), P()), check_vma=False)
```

```python
import jax
import jax.numpy as jnp
from jax import lax
from jax.experimental import pallas as pl
from jax.experimental.pallas import tpu as pltpu
from jax.sharding import PartitionSpec as P

MESH = pl.DeviceIdType.MESH
F32 = jnp.float32
LANES = 128
SUB = 8
TILES = 16
LOW, HIGH = slice(0, LANES), slice(LANES, 2 * LANES)
ROWS = SUB * TILES
CHUNK = 2 * ROWS
CHUNKS = 4
PIECES = (0, 16, 64, 112, 128)
FIRST = CHUNK // 4
EARLY = 0
DEVICES = 8
CHIPS = 4
QUBITS = 20
scope = jax.named_scope


def cmul(a, b):
    (a_re, a_im), (b_re, b_im) = a, b
    return a_re * b_re - a_im * b_im, a_re * b_im + a_im * b_re


def cadd(a, b):
    (a_re, a_im), (b_re, b_im) = a, b
    return a_re + b_re, a_im + b_im


def conj_mul(a, b):
    (a_re, a_im), (b_re, b_im) = a, b
    return a_re * b_re + a_im * b_im, a_re * b_im - a_im * b_re


def mix(coefs, values):
    total = None
    for coef, value in zip(coefs, values):
        part = cmul(coef, value)
        total = part if total is None else cadd(total, part)
    return total


def gate(mat, zero, one):
    u00, u01, u10, u11 = mat
    return mix((u00, u01), (zero, one)), mix((u10, u11), (zero, one))


def norm(a):
    re, im = a
    return re * re + im * im


def plus_minus(bit):
    return 1 - 2 * bit


def planes(ref, half, chunk, rows):
    return [ref[half, chunk, part, rows, :] for part in range(2)]


def put(ref, half, chunk, rows, value):
    for part in range(2):
        ref[half, chunk, part, rows, :] = value[part]


def tile(t, first=0):
    return pl.ds(pl.multiple_of(first + SUB * t, SUB), SUB)


def kernel(x_hbm, u_hbm, cz_hbm, OUT, z_ref,
           BIG, u_ref, cz_ref, S, R2, T, SG, GM, KM, XC, ZC, TP, V, VP, VR, V7,
           ld, sent_sem, s1r, cpr, fwr, s2r, zs, zr, zp, ready):
    X, RB, XP, RP = [BIG.at[part] for part in range(4)]
    me = lax.axis_index('q')
    bit_y = me // 4
    bit_x = (me // 2) % 2
    bit_c = me % 2
    step_y, step_x, step_c = 4 * plus_minus(bit_y), 2 * plus_minus(bit_x), plus_minus(bit_c)
    dev_y, dev_x, dev_c = me + step_y, me + step_x, me + step_c
    first_dev = (dev_x, dev_y)
    second_dev = (dev_y, dev_x)
    second_bit = (bit_y, bit_x)

    def sent(half, k):
        return k + second_bit[half] * (3 - 2 * k)

    def received(half, k):
        return 3 - k + second_bit[half] * (2 * k - 3)

    def block_rows(half, chunk):
        return pl.ds(pl.multiple_of((half * CHUNKS + chunk) * CHUNK, CHUNK), CHUNK)

    def remote(src, dst, send, recv, dev):
        return pltpu.make_async_remote_copy(src_ref=src, dst_ref=dst, send_sem=send, recv_sem=recv,
                                            device_id=(dev,), device_id_type=MESH)

    def wait_bytes(ref, sem):
        pltpu.make_async_copy(ref, ref, sem).wait()

    def part_rows(half, k, part):
        low, size = ((0, FIRST), (FIRST, CHUNK - FIRST))[part] if k == 0 else (0, CHUNK)
        return pl.ds(pl.multiple_of((half * CHUNKS + sent(half, k)) * CHUNK + low, SUB), size)

    def load_copy(half, k, part=0):
        rows = part_rows(half, k, part)
        return pltpu.make_async_copy(x_hbm.at[rows], X.at[rows], ld.at[min(2, k + 1) if k else part])

    def stage1(half, k, part=0):
        rows = part_rows(half, k, part)
        return remote(X.at[rows], RB.at[rows], sent_sem, s1r.at[k], first_dev[half])

    def core_copy(half, k):
        rows = block_rows(half, sent(half, k))
        return remote(X.at[rows], XP.at[rows], sent_sem, cpr, dev_c)

    def forward(half, k):
        rows = block_rows(half, sent(half, k))
        return remote(RB.at[rows], RP.at[rows], sent_sem, fwr.at[k], dev_c)

    def stage2(half, k, piece=None):
        chunk = sent(half, k)
        if piece is None:
            return remote(S.at[half, chunk], R2.at[half, chunk], sent_sem, s2r.at[k], second_dev[half])
        rows = pl.ds(PIECES[piece], PIECES[piece + 1] - PIECES[piece])
        return remote(S.at[half, chunk, :, rows], R2.at[half, chunk, :, rows], sent_sem, s2r.at[3 + piece], second_dev[half])

    u_copy = pltpu.make_async_copy(u_hbm, u_ref, ld.at[3])
    cz_copy = pltpu.make_async_copy(cz_hbm, cz_ref, ld.at[4])
    last_chip = bit_y * bit_x
    beside = bit_y + bit_x - 2 * last_chip
    barrier = pltpu.get_barrier_semaphore()

    def signal(sem, devices):
        for dev in devices:
            pl.semaphore_signal(sem, inc=1, device_id=(dev,), device_id_type=MESH)

    signal(barrier, (dev_c,))
    pl.when(last_chip == 0)(lambda: signal(barrier, (dev_x, dev_y)))
    order = [(k, part) for k in range(CHUNKS) for part in range(1 if k else 2)]
    for k, part in order:
        for half in range(2):
            load_copy(half, k, part).start()
    u_copy.start()
    cz_copy.start()

    waits = {(0, 0): (0, 2 * FIRST), (0, 1): (1, 2 * (CHUNK - FIRST)), (1, 0): (2, 6 * CHUNK)}

    def send_first(halves, wait):
        for k, part in order:
            if wait and (k, part) in waits:
                index, size = waits[k, part]
                wait_bytes(X.at[:size], ld.at[index])
            if k == 0:
                for half in halves:
                    stage1(half, k, part).start()
        pl.when(bit_c == 0)(lambda: send_rest(halves))

    def send_rest(halves):
        for k in range(1, CHUNKS):
            for half in halves:
                stage1(half, k).start()

    def send_beside(half):
        send_first((half,), True)
        with scope('w_rdy'):
            pl.semaphore_wait(ready, 1)
        send_first((1 - half,), False)

    with scope('bar'):
        pl.when(beside == 1)(lambda: pl.semaphore_wait(barrier, 2))
        pl.when(beside == 0)(lambda: pl.semaphore_wait(barrier, 3))
    pl.when(last_chip == 1)(lambda: signal(ready, (dev_x, dev_y)))
    with scope('first'):
        pl.when(beside == 0)(lambda: send_first((0, 1), True))
        pl.when(beside * bit_x == 1)(lambda: send_beside(0))
        pl.when(beside * bit_y == 1)(lambda: send_beside(1))
    for k in range(CHUNKS):
        for half in range(2):
            core_copy(half, k).start()
    u_copy.wait()
    cz_copy.wait()

    def entry(qubit, row, col):
        return u_ref[row * 2 + col, qubit], u_ref[4 + row * 2 + col, qubit]

    def matrix(qubit, flip=0):
        return [entry(qubit, row + flip * plus_minus(row), col + flip * plus_minus(col)) for row in range(2) for col in range(2)]

    lane = lax.broadcasted_iota(jnp.int32, (SUB, LANES), 1)
    sub = lax.broadcasted_iota(jnp.int32, (SUB, LANES), 0)

    def build(t, carry):
        row = sub + SUB * t
        for base, left in ((6, True), (13, False)):
            re = im = None
            for j in range(7):
                shift = 6 - j
                row_bit = ((row >> shift) & 1) == 1
                col_bit = ((lane >> shift) & 1) == 1
                fac = []
                for ri in range(2):
                    u00, u01, u10, u11 = [u_ref[4 * ri + k, base + j] for k in range(4)]
                    if not left:
                        u01, u10 = u10, u01
                    fac.append(jnp.where(row_bit, jnp.where(col_bit, u11, u10), jnp.where(col_bit, u01, u00)))
                if re is None:
                    re, im = fac
                else:
                    re, im = cmul((re, im), fac)
            low, high = tile(t), tile(t, LANES)
            dest, upper, lower = (GM, -im, im) if left else (KM, im, -im)
            dest[low, LOW] = re
            dest[low, HIGH] = upper
            dest[high, LOW] = lower
            dest[high, HIGH] = re
        return carry

    with scope('build'):
        lax.fori_loop(0, TILES, build, 0)

    shifts = [[QUBITS - 1 - cz_ref[side, k] for side in range(2)] for k in range(QUBITS // 2)]

    def build_signs(t, carry):
        flat = (me * DEVICES * ROWS + sub + SUB * t) * LANES + lane
        parity = jnp.zeros_like(flat)
        for shift_a, shift_b in shifts:
            parity = parity ^ ((flat >> shift_a) & (flat >> shift_b))
        SG[tile(t), :] = plus_minus(parity & 1).astype(F32)
        return carry

    with scope('signs'):
        lax.fori_loop(0, DEVICES * TILES, build_signs, 0, unroll=4)

    def strided(ref, at):
        return [ref[pl.ds(at + part, SUB, stride=2), :] for part in range(2)]

    zero_tile = jnp.zeros((SUB, LANES), F32)
    zero_pair = (zero_tile, zero_tile)

    def raw_sums(t, carry):
        total, sums = carry
        value = [strided(X, pl.multiple_of(block * CHUNK + 2 * SUB * t, 2 * SUB)) for block in range(DEVICES)]
        dens = [norm(v) for v in value]
        done = []
        for (diff, cross), bit in zip(sums, (4, 2, 1)):
            for block in range(DEVICES):
                if block & bit:
                    diff = diff - dens[block]
                else:
                    diff = diff + dens[block]
                    cross = cadd(cross, conj_mul(value[block], value[block + bit]))
            done.append((diff, cross))
        for part in dens:
            total = total + part
        return total, tuple(done)

    with scope('raw'):
        raw_total, raw = lax.fori_loop(0, TILES, raw_sums, (zero_tile, ((zero_tile, zero_pair),) * 3))

    def fold(part):
        return jnp.sum(part, axis=0, keepdims=True)

    def pair_weights(mat):
        u00, u01, u10, u11 = mat
        (a_re, a_im), (b_re, b_im) = conj_mul(u00, u01), conj_mul(u10, u11)
        return norm(u00) - norm(u10), norm(u01) - norm(u11), 2 * (a_re - b_re), 2 * (b_im - a_im)

    raw_rows = []
    raw_total = fold(raw_total)
    for qubit, (diff, (re, im)) in zip((3, 4, 5), raw):
        weight_0, weight_1, mix_re, mix_im = pair_weights(matrix(qubit))
        even, odd = raw_total + fold(diff), raw_total - fold(diff)
        raw_rows.append((weight_0 * even + weight_1 * odd) / 2 + mix_re * fold(re) + mix_im * fold(im))

    def gate_pair(qubit, own_bit):
        return entry(qubit, own_bit, own_bit), entry(qubit, own_bit, 1 - own_bit)

    coef_y = gate_pair(0, bit_y)
    coef_x = gate_pair(1, bit_x)
    coef_c = gate_pair(2, bit_c)
    stage1_coefs = [[cmul(top, core) for core in coef_c for top in coef] for coef in (coef_x, coef_y)]

    norms = zero_pair
    for k in range(CHUNKS):
        with scope('w_s1'):
            wait_bytes(RB.at[0:2 * CHUNK], s1r.at[k])
        for half in range(2):
            forward(half, k).start()
        if k == 0:
            pl.when(bit_c == 1)(lambda: send_rest((0, 1)))
        else:
            for half in range(2):
                stage2(half, k - 1).start()
        if k == 0:
            wait_bytes(XP, cpr)
        with scope('w_fw'):
            wait_bytes(RP.at[0:2 * CHUNK], fwr.at[k])

        for half in range(2):
            coefs = stage1_coefs[half]
            base = (half * CHUNKS + sent(half, k)) * CHUNK

            def combine(t, carry, base=base, coefs=coefs, half=half):
                at = pl.multiple_of(base + 2 * SUB * t, 2 * SUB)
                re, im = mix(coefs, [strided(ref, at) for ref in (X, RB, XP, RP)])
                XC[tile(t), (LOW, HIGH)[half]] = re
                XC[tile(t, LANES), (LOW, HIGH)[half]] = im
                return carry

            with scope('comb'):
                lax.fori_loop(0, TILES, combine, 0, unroll=2)
        with scope('mm'):
            left = lax.dot(GM[...], XC[...], precision=lax.Precision.HIGHEST, preferred_element_type=F32)
            for rows in (LOW, HIGH):
                for cols in (LOW, HIGH):
                    ZC[cols, rows] = left[rows, cols]
            both = lax.dot(ZC[...], KM[...], precision=lax.Precision.HIGHEST, preferred_element_type=F32)
            for half in range(2):
                for part in range(2):
                    S[half, sent(half, k), part] = both[(LOW, HIGH)[half], (LOW, HIGH)[part]]

        def mid_sums(t, sums, k=k):
            dens = [norm(planes(S, half, sent(half, k), tile(t))) for half in range(2)]
            row = dens[0] + dens[1]
            TP[tile(t), :] = row if k == 0 else TP[tile(t), :] + row
            return tuple(a + b for a, b in zip(sums, dens))

        with scope('dens'):
            norms = lax.fori_loop(0, TILES, mid_sums, norms, unroll=2)

    flips = (1 - bit_y, 1 - bit_x)
    u3 = matrix(3)
    u4 = [matrix(4, flip) for flip in flips]
    u5 = [matrix(5, flip) for flip in flips]
    second_coef = (coef_y, coef_x)

    def weights(k):
        table = {}
        for half in range(2):
            index = received(half, k)
            for chunk in range(CHUNKS):
                inner = cmul(entry(4, chunk // 2, index // 2), entry(5, chunk % 2, index % 2))
                inner = cmul(second_coef[half][1], inner)
                for side in range(2):
                    table[side, chunk, half] = cmul(u3[2 * side + half], inner)
        return table

    def add_cross(k):
        def body(t, cross):
            done = []
            for half in range(2):
                chunk = received(half, k)
                part = conj_mul(planes(S, half, chunk, tile(t)), planes(R2, half, chunk, tile(t)))
                done.append(cadd(cross[half], part))
            return tuple(done)
        return body

    def step_own(t, carry):
        rows = tile(t)
        for half in range(2):
            own, other = second_coef[half]
            value = []
            for k in range(CHUNKS):
                chunk = received(half, k)
                part = cmul(own, planes(S, half, chunk, rows))
                value.append(cadd(part, cmul(other, planes(R2, half, chunk, rows))) if k < 2 else part)
            value = [v for pair in (value[:2], value[2:]) for v in gate(u5[half], *pair)]
            value = [gate(u4[half], value[k], value[k + 2]) for k in range(2)]
            for k in range(CHUNKS):
                put(T, half, received(half, k), rows, value[k % 2][k // 2])
        return carry

    def step_mix(t, carry):
        rows = tile(t)
        for chunk in range(CHUNKS):
            for half, value in enumerate(gate(u3, planes(T, 0, chunk, rows), planes(T, 1, chunk, rows))):
                put(T, half, chunk, rows, value)
        return carry

    def add_received(k, table, store):
        def body(t, carry):
            rows = tile(t)
            other = [planes(R2, half, received(half, k), rows) for half in range(2)]
            for side in range(2):
                for chunk in range(CHUNKS):
                    value = planes(T, side, chunk, rows)
                    for half in range(2):
                        value = cadd(value, cmul(table[side, chunk, half], other[half]))
                    store(side, chunk, t, value)
            return carry
        return body

    def store_partial(side, chunk, t, value):
        put(T, side, chunk, tile(t), value)

    def store_out(side, chunk, t, value):
        block = side * CHUNKS + chunk
        sign = SG[tile(t, block * ROWS), :]
        at = pl.multiple_of(block * CHUNK + 2 * SUB * t, 2 * SUB)
        for part in range(2):
            OUT[pl.ds(at + part, SUB, stride=2), :] = value[part] * sign

    tables = {k: weights(k) for k in (2, 3)}
    cross = (zero_pair, zero_pair)
    with scope('w_s2'):
        wait_bytes(R2.at[:, 0], s2r.at[0])
    for piece in range(EARLY):
        for half in range(2):
            stage2(half, 3, piece).start()
    with scope('x0'):
        cross = lax.fori_loop(0, TILES, add_cross(0), cross, unroll=2)
    with scope('w_s2'):
        wait_bytes(R2.at[:, 0], s2r.at[1])
    with scope('x1'):
        cross = lax.fori_loop(0, TILES, add_cross(1), cross, unroll=2)

    def signed(parts, bit):
        acc = parts[0]
        for index, part in enumerate(parts[1:], 1):
            acc = acc - part if (index >> bit) & 1 else acc + part
        return acc

    def z_part():
        return remote(V, VP, zs, zp, dev_c)

    def z_copy(chip, core):
        dev = me + (chip // 2) * step_y + (chip % 2) * step_x + core * step_c
        return remote(V, VR.at[chip], zs, zr, dev)

    def send_sum():
        with scope('w_zp'):
            wait_bytes(VP, zp)
        total = V[...] + VP[...]
        V[...] = total
        VR[0] = total

    def spread_sum():
        for chip in reversed(range(CHIPS)):
            for core in reversed(range(2)):
                if chip or core:
                    z_copy(chip, core).start()

    row_index = lax.broadcasted_iota(jnp.int32, (3 * SUB, LANES), 0)
    col_index = lax.broadcasted_iota(jnp.int32, (3 * SUB, LANES), 1)
    with scope('zsum'):
        signs = [plus_minus(bit).astype(F32) for bit in (bit_y, bit_x, bit_c)]
        norm_rows = [fold(part) for part in norms]
        tot_row = norm_rows[0] + norm_rows[1]
        rows = []
        for half, bit in enumerate(second_bit):
            weight_0, weight_1, mix_re, mix_im = pair_weights(matrix(half))
            re, im = cross[half]
            rows.append(jnp.where(bit == 1, weight_1, weight_0) * norm_rows[half] + mix_re * fold(re)
                        + (mix_im * signs[half]) * fold(im) + signs[half] * norm_rows[1 - half])
        rows += [signs[2] * tot_row] + raw_rows
        parts = [TP[tile(t), :] for t in range(TILES)]
        rows += [fold(signed(parts, bit)) for bit in reversed(range(4))]
        total = norms[0] + norms[1]
        rows += [fold(total * plus_minus((sub >> bit) & 1).astype(F32)) for bit in reversed(range(3))]
        rows += [tot_row * plus_minus((lane[:1] >> bit) & 1).astype(F32) for bit in reversed(range(7))]
        rows += [jnp.zeros_like(tot_row)] * 4
        column = jnp.sum(jnp.concatenate(rows, axis=0), axis=1, keepdims=True)
        mine = jnp.sum(jnp.where(row_index == col_index, column, 0.0), axis=0, keepdims=True)
        V[...] = mine
    pl.when(bit_c == 1)(send_sum)
    pl.when(bit_c == 0)(lambda: z_part().start())
    pl.when(bit_c == 1)(spread_sum)
    def send_pieces(low, high):
        for piece in range(low, high):
            for half in range(2):
                stage2(half, 3, piece).start()

    send_pieces(EARLY, len(PIECES) - 1)
    with scope('own'):
        lax.fori_loop(0, TILES, step_own, 0)
        lax.fori_loop(0, TILES, step_mix, 0)
    with scope('w_s2'):
        wait_bytes(R2.at[:, 0], s2r.at[2])
    with scope('st2'):
        lax.fori_loop(0, TILES, add_received(2, tables[2], store_partial), 0)

    for piece in range(len(PIECES) - 1):
        low, high = PIECES[piece], PIECES[piece + 1]
        with scope('w_s2'):
            wait_bytes(R2.at[:, 0, :, low:high], s2r.at[3 + piece])
        with scope('tail'):
            lax.fori_loop(low // SUB, high // SUB, add_received(3, tables[3], store_out), 0)
        if piece == len(PIECES) - 3:
            with scope('w_z'):
                pl.when(bit_c == 0)(lambda: wait_bytes(VR, zr))
                pl.when(bit_c == 1)(lambda: wait_bytes(VR.at[1:CHIPS], zr))
            acc = VR[0]
            for chip in range(1, CHIPS):
                acc = acc + VR[chip]
            z_ref[...] = acc[:, :QUBITS] / 2 ** QUBITS

    with scope('w_send'):
        wait_bytes(BIG, sent_sem)
        pl.when(bit_c == 0)(lambda: wait_bytes(VP, zs))
        pl.when(bit_c == 1)(lambda: wait_bytes(V7, zs))


def writer(state_ref, z_ref, state_out, z_out, sems):
    copies = [pltpu.make_async_copy(state_ref, state_out, sems.at[0]), pltpu.make_async_copy(z_ref, z_out, sems.at[1])]
    for copy in copies:
        copy.start()
    for copy in copies:
        copy.wait()


def solution(mesh):
    def local_layer(state_local, unitaries, cz_pairs):
        size = state_local.shape[1]
        rows = 2 * size // LANES
        x = state_local.reshape(2, -1, LANES).swapaxes(0, 1).reshape(rows, LANES)
        u = unitaries.transpose(0, 2, 3, 1).reshape(SUB, QUBITS)
        cz = cz_pairs.T
        x, u, cz = [pltpu.with_memory_space_constraint(v, pltpu.HBM) for v in (x, u, cz)]
        vm = pltpu.VMEM
        dma = pltpu.SemaphoreType.DMA
        halves = vm((2, CHUNKS, 2, ROWS, LANES), F32)
        square = vm((2 * LANES, 2 * LANES), F32)
        any_spec = pl.BlockSpec(memory_space=pl.ANY)
        shapes = (jax.ShapeDtypeStruct((rows, LANES), F32), jax.ShapeDtypeStruct((1, QUBITS), F32))
        out, z = pl.pallas_call(
            kernel,
            out_shape=shapes,
            in_specs=[pl.BlockSpec(memory_space=pltpu.HBM)] * 3,
            out_specs=(pl.BlockSpec(memory_space=pltpu.VMEM), pl.BlockSpec(memory_space=pltpu.VMEM)),
            scratch_shapes=[
                vm((4, rows, LANES), F32), pltpu.SMEM(u.shape, F32), pltpu.SMEM(cz.shape, jnp.int32), halves, halves, halves,
                vm((rows // 2, LANES), F32), square, square, square, square, vm((ROWS, LANES), F32),
                vm((1, LANES), F32), vm((1, LANES), F32), vm((CHIPS, 1, LANES), F32), vm((2 * CHIPS - 1, 1, LANES), F32),
                dma((5,)), dma, dma((4,)), dma, dma((4,)), dma((3 + len(PIECES) - 1,)), dma, dma, dma, pltpu.SemaphoreType.REGULAR,
            ],
            compiler_params=pltpu.CompilerParams(collective_id=0, has_side_effects=True, vmem_limit_bytes=40 * 2 ** 20),
        )(x, u, cz)
        out, z = pl.pallas_call(
            writer, out_shape=shapes, in_specs=[any_spec] * 2, out_specs=(any_spec,) * 2, scratch_shapes=[dma((2,))],
            compiler_params=pltpu.CompilerParams(vmem_limit_bytes=2 ** 20),
        )(out, z)
        state = out.reshape(-1, 2, LANES).swapaxes(0, 1).reshape(2, size)
        return state, z.reshape(QUBITS)

    return jax.shard_map(local_layer, mesh=mesh, in_specs=(P(None, 'q'), P(), P()), out_specs=(P(None, 'q'), P()), check_vma=False)
```

```python
import jax
import jax.numpy as jnp
from jax import lax
from jax.experimental import pallas as pl
from jax.experimental.pallas import tpu as pltpu
from jax.sharding import PartitionSpec as P

MESH = pl.DeviceIdType.MESH
F32 = jnp.float32
LANES = 128
SUB = 8
TILES = 16
LOW, HIGH = slice(0, LANES), slice(LANES, 2 * LANES)
ROWS = SUB * TILES
CHUNK = 2 * ROWS
CHUNKS = 4
PIECES = (0, 16, 64, 112, 128)
FIRST = CHUNK // 4
DEVICES = 8
CHIPS = 4
QUBITS = 20
scope = jax.named_scope


def cmul(a, b):
    (a_re, a_im), (b_re, b_im) = a, b
    return a_re * b_re - a_im * b_im, a_re * b_im + a_im * b_re


def cadd(a, b):
    (a_re, a_im), (b_re, b_im) = a, b
    return a_re + b_re, a_im + b_im


def conj_mul(a, b):
    (a_re, a_im), (b_re, b_im) = a, b
    return a_re * b_re + a_im * b_im, a_re * b_im - a_im * b_re


def mix(coefs, values):
    total = None
    for coef, value in zip(coefs, values):
        part = cmul(coef, value)
        total = part if total is None else cadd(total, part)
    return total


def gate(mat, zero, one):
    u00, u01, u10, u11 = mat
    return mix((u00, u01), (zero, one)), mix((u10, u11), (zero, one))


def norm(a):
    re, im = a
    return re * re + im * im


def plus_minus(bit):
    return 1 - 2 * bit


def planes(ref, half, chunk, rows):
    return [ref[half, chunk, part, rows, :] for part in range(2)]


def put(ref, half, chunk, rows, value):
    for part in range(2):
        ref[half, chunk, part, rows, :] = value[part]


def tile(t, first=0):
    return pl.ds(pl.multiple_of(first + SUB * t, SUB), SUB)


def kernel(x_hbm, u_hbm, cz_hbm, OUT, z_ref,
           BIG, u_ref, cz_ref, S, R2, T, SG, GM, KM, XC, ZC, TP, V, VP, VR, V7,
           ld, sent_sem, s1r, fwr, s2r, zs, zp, ready):
    zr = ld.at[2]
    piece_sems = [s1r.at[0], s1r.at[1], s1r.at[2], fwr.at[0]]
    size = BIG.shape[0] // 4
    X, RB, XP, RP = [BIG.at[pl.ds(part * size, size)] for part in range(4)]
    me = lax.axis_index('q')
    bit_y = me // 4
    bit_x = (me // 2) % 2
    bit_c = me % 2
    step_y, step_x, step_c = 4 * plus_minus(bit_y), 2 * plus_minus(bit_x), plus_minus(bit_c)
    dev_y, dev_x, dev_c = me + step_y, me + step_x, me + step_c
    first_dev = (dev_x, dev_y)
    second_dev = (dev_y, dev_x)
    second_bit = (bit_y, bit_x)

    def sent(half, k):
        return k + second_bit[half] * (3 - 2 * k)

    def received(half, k):
        return 3 - k + second_bit[half] * (2 * k - 3)

    def block_rows(half, chunk):
        return pl.ds(pl.multiple_of((half * CHUNKS + chunk) * CHUNK, CHUNK), CHUNK)

    def remote(src, dst, send, recv, dev):
        return pltpu.make_async_remote_copy(src_ref=src, dst_ref=dst, send_sem=send, recv_sem=recv,
                                            device_id=(dev,), device_id_type=MESH)

    def wait_bytes(ref, sem):
        pltpu.make_async_copy(ref, ref, sem).wait()

    def part_rows(half, k, part):
        low, size = ((0, FIRST), (FIRST, CHUNK - FIRST))[part] if k == 0 else (0, CHUNK)
        return pl.ds(pl.multiple_of((half * CHUNKS + sent(half, k)) * CHUNK + low, SUB), size)

    def load_copy(half, k, part=0):
        rows = part_rows(half, k, part)
        return pltpu.make_async_copy(x_hbm.at[rows], X.at[rows], ld.at[min(2, k + 1) if k else part])

    def stage1(half, k, part=0):
        rows = part_rows(half, k, part)
        return remote(X.at[rows], RB.at[rows], sent_sem, s1r.at[k], first_dev[half])

    def core_copy(half, k):
        rows = block_rows(half, sent(half, k))
        return remote(X.at[rows], XP.at[rows], sent_sem, fwr.at[0], dev_c)

    def forward(half, k):
        rows = block_rows(half, sent(half, k))
        return remote(RB.at[rows], RP.at[rows], sent_sem, fwr.at[k], dev_c)

    def stage2(half, k, piece=None):
        chunk = sent(half, k)
        if piece is None:
            return remote(S.at[half, chunk], R2.at[half, chunk], sent_sem, s2r.at[k], second_dev[half])
        rows = pl.ds(PIECES[piece], PIECES[piece + 1] - PIECES[piece])
        return remote(S.at[half, chunk, :, rows], R2.at[half, chunk, :, rows], sent_sem, piece_sems[piece], second_dev[half])

    u_copy = pltpu.make_async_copy(u_hbm, u_ref, zs)
    cz_copy = pltpu.make_async_copy(cz_hbm, cz_ref, zp)
    last_chip = bit_y * bit_x
    beside = bit_y + bit_x - 2 * last_chip
    barrier = pltpu.get_barrier_semaphore()

    def signal(sem, devices):
        for dev in devices:
            pl.semaphore_signal(sem, inc=1, device_id=(dev,), device_id_type=MESH)

    signal(barrier, (dev_c,))
    pl.when(last_chip == 0)(lambda: signal(barrier, (dev_x, dev_y)))
    order = [(k, part) for k in range(CHUNKS) for part in range(1 if k else 2)]
    for k, part in order:
        for half in range(2):
            load_copy(half, k, part).start()
    u_copy.start()
    cz_copy.start()

    waits = {(0, 0): (0, 2 * FIRST), (0, 1): (1, 2 * (CHUNK - FIRST)), (1, 0): (2, 6 * CHUNK)}

    def send_first(halves, wait):
        for k, part in order:
            if wait and (k, part) in waits:
                index, size = waits[k, part]
                wait_bytes(X.at[:size], ld.at[index])
            if k == 0:
                for half in halves:
                    stage1(half, k, part).start()
        pl.when(bit_c == 0)(lambda: send_rest(halves))

    def send_rest(halves):
        for k in range(1, CHUNKS):
            for half in halves:
                stage1(half, k).start()

    def send_beside(half):
        send_first((half,), True)
        with scope('w_rdy'):
            pl.semaphore_wait(ready, 1)
        send_first((1 - half,), False)

    with scope('bar'):
        pl.when(beside == 1)(lambda: pl.semaphore_wait(barrier, 2))
        pl.when(beside == 0)(lambda: pl.semaphore_wait(barrier, 3))
    pl.when(last_chip == 1)(lambda: signal(ready, (dev_x, dev_y)))
    with scope('first'):
        pl.when(beside == 0)(lambda: send_first((0, 1), True))
        pl.when(beside * bit_x == 1)(lambda: send_beside(0))
        pl.when(beside * bit_y == 1)(lambda: send_beside(1))
    for k in range(CHUNKS):
        for half in range(2):
            core_copy(half, k).start()
    u_copy.wait()
    cz_copy.wait()

    def entry(qubit, row, col):
        return u_ref[row * 2 + col, qubit], u_ref[4 + row * 2 + col, qubit]

    def matrix(qubit, flip=0):
        return [entry(qubit, row + flip * plus_minus(row), col + flip * plus_minus(col)) for row in range(2) for col in range(2)]

    lane = lax.broadcasted_iota(jnp.int32, (SUB, LANES), 1)
    sub = lax.broadcasted_iota(jnp.int32, (SUB, LANES), 0)

    def build(t, carry):
        row = sub + SUB * t
        for base, left in ((6, True), (13, False)):
            re = im = None
            for j in range(7):
                shift = 6 - j
                row_bit = ((row >> shift) & 1) == 1
                col_bit = ((lane >> shift) & 1) == 1
                fac = []
                for ri in range(2):
                    u00, u01, u10, u11 = [u_ref[4 * ri + k, base + j] for k in range(4)]
                    if not left:
                        u01, u10 = u10, u01
                    fac.append(jnp.where(row_bit, jnp.where(col_bit, u11, u10), jnp.where(col_bit, u01, u00)))
                if re is None:
                    re, im = fac
                else:
                    re, im = cmul((re, im), fac)
            low, high = tile(t), tile(t, LANES)
            dest, upper, lower = (GM, -im, im) if left else (KM, im, -im)
            dest[low, LOW] = re
            dest[low, HIGH] = upper
            dest[high, LOW] = lower
            dest[high, HIGH] = re
        return carry

    with scope('build'):
        lax.fori_loop(0, TILES, build, 0)

    shifts = [[QUBITS - 1 - cz_ref[side, k] for side in range(2)] for k in range(QUBITS // 2)]

    def build_signs(t, carry):
        flat = (me * DEVICES * ROWS + sub + SUB * t) * LANES + lane
        parity = jnp.zeros_like(flat)
        for shift_a, shift_b in shifts:
            parity = parity ^ ((flat >> shift_a) & (flat >> shift_b))
        SG[tile(t), :] = plus_minus(parity & 1).astype(F32)
        return carry

    with scope('signs'):
        lax.fori_loop(0, DEVICES * TILES, build_signs, 0, unroll=4)

    def strided(ref, at):
        return [ref[pl.ds(at + part, SUB, stride=2), :] for part in range(2)]

    zero_tile = jnp.zeros((SUB, LANES), F32)
    zero_pair = (zero_tile, zero_tile)

    def raw_sums(t, carry):
        total, sums = carry
        value = [strided(X, pl.multiple_of(block * CHUNK + 2 * SUB * t, 2 * SUB)) for block in range(DEVICES)]
        dens = [norm(v) for v in value]
        done = []
        for (diff, cross), bit in zip(sums, (4, 2, 1)):
            for block in range(DEVICES):
                if block & bit:
                    diff = diff - dens[block]
                else:
                    diff = diff + dens[block]
                    cross = cadd(cross, conj_mul(value[block], value[block + bit]))
            done.append((diff, cross))
        for part in dens:
            total = total + part
        return total, tuple(done)

    with scope('raw'):
        raw_total, raw = lax.fori_loop(0, TILES, raw_sums, (zero_tile, ((zero_tile, zero_pair),) * 3))

    def fold(part):
        return jnp.sum(part, axis=0, keepdims=True)

    def pair_weights(mat):
        u00, u01, u10, u11 = mat
        (a_re, a_im), (b_re, b_im) = conj_mul(u00, u01), conj_mul(u10, u11)
        return norm(u00) - norm(u10), norm(u01) - norm(u11), 2 * (a_re - b_re), 2 * (b_im - a_im)

    raw_rows = []
    raw_total = fold(raw_total)
    for qubit, (diff, (re, im)) in zip((3, 4, 5), raw):
        weight_0, weight_1, mix_re, mix_im = pair_weights(matrix(qubit))
        even, odd = raw_total + fold(diff), raw_total - fold(diff)
        raw_rows.append((weight_0 * even + weight_1 * odd) / 2 + mix_re * fold(re) + mix_im * fold(im))

    def gate_pair(qubit, own_bit):
        return entry(qubit, own_bit, own_bit), entry(qubit, own_bit, 1 - own_bit)

    coef_y = gate_pair(0, bit_y)
    coef_x = gate_pair(1, bit_x)
    coef_c = gate_pair(2, bit_c)
    stage1_coefs = [[cmul(top, core) for core in coef_c for top in coef] for coef in (coef_x, coef_y)]

    norms = zero_pair
    for k in range(CHUNKS):
        with scope('w_s1'):
            wait_bytes(RB.at[0:2 * CHUNK], s1r.at[k])
        for half in range(2):
            forward(half, k).start()
        if k == 0:
            pl.when(bit_c == 1)(lambda: send_rest((0, 1)))
        else:
            for half in range(2):
                stage2(half, k - 1).start()
        with scope('w_fw'):
            wait_bytes(BIG.at[0:2 * CHUNK + (0 if k else size)], fwr.at[k])

        for half in range(2):
            coefs = stage1_coefs[half]
            base = (half * CHUNKS + sent(half, k)) * CHUNK

            def combine(t, carry, base=base, coefs=coefs, half=half):
                at = pl.multiple_of(base + 2 * SUB * t, 2 * SUB)
                re, im = mix(coefs, [strided(ref, at) for ref in (X, RB, XP, RP)])
                XC[tile(t), (LOW, HIGH)[half]] = re
                XC[tile(t, LANES), (LOW, HIGH)[half]] = im
                return carry

            with scope('comb'):
                lax.fori_loop(0, TILES, combine, 0, unroll=2)
        with scope('mm'):
            left = lax.dot(GM[...], XC[...], precision=lax.Precision.HIGHEST, preferred_element_type=F32)
            for rows in (LOW, HIGH):
                for cols in (LOW, HIGH):
                    ZC[cols, rows] = left[rows, cols]
            both = lax.dot(ZC[...], KM[...], precision=lax.Precision.HIGHEST, preferred_element_type=F32)
            for half in range(2):
                for part in range(2):
                    S[half, sent(half, k), part] = both[(LOW, HIGH)[half], (LOW, HIGH)[part]]

        def mid_sums(t, sums, k=k):
            dens = [norm(planes(S, half, sent(half, k), tile(t))) for half in range(2)]
            row = dens[0] + dens[1]
            TP[tile(t), :] = row if k == 0 else TP[tile(t), :] + row
            return tuple(a + b for a, b in zip(sums, dens))

        with scope('dens'):
            norms = lax.fori_loop(0, TILES, mid_sums, norms, unroll=2)

    flips = (1 - bit_y, 1 - bit_x)
    u3 = matrix(3)
    u4 = [matrix(4, flip) for flip in flips]
    u5 = [matrix(5, flip) for flip in flips]
    second_coef = (coef_y, coef_x)

    def weights(k):
        table = {}
        for half in range(2):
            index = received(half, k)
            for chunk in range(CHUNKS):
                inner = cmul(entry(4, chunk // 2, index // 2), entry(5, chunk % 2, index % 2))
                inner = cmul(second_coef[half][1], inner)
                for side in range(2):
                    table[side, chunk, half] = cmul(u3[2 * side + half], inner)
        return table

    def add_cross(k):
        def body(t, cross):
            done = []
            for half in range(2):
                chunk = received(half, k)
                part = conj_mul(planes(S, half, chunk, tile(t)), planes(R2, half, chunk, tile(t)))
                done.append(cadd(cross[half], part))
            return tuple(done)
        return body

    def step_own(t, carry):
        rows = tile(t)
        for half in range(2):
            own, other = second_coef[half]
            value = []
            for k in range(CHUNKS):
                chunk = received(half, k)
                part = cmul(own, planes(S, half, chunk, rows))
                value.append(cadd(part, cmul(other, planes(R2, half, chunk, rows))) if k < 2 else part)
            value = [v for pair in (value[:2], value[2:]) for v in gate(u5[half], *pair)]
            value = [gate(u4[half], value[k], value[k + 2]) for k in range(2)]
            for k in range(CHUNKS):
                put(T, half, received(half, k), rows, value[k % 2][k // 2])
        return carry

    def step_mix(t, carry):
        rows = tile(t)
        for chunk in range(CHUNKS):
            for half, value in enumerate(gate(u3, planes(T, 0, chunk, rows), planes(T, 1, chunk, rows))):
                put(T, half, chunk, rows, value)
        return carry

    def add_received(k, table, store):
        def body(t, carry):
            rows = tile(t)
            other = [planes(R2, half, received(half, k), rows) for half in range(2)]
            for side in range(2):
                for chunk in range(CHUNKS):
                    value = planes(T, side, chunk, rows)
                    for half in range(2):
                        value = cadd(value, cmul(table[side, chunk, half], other[half]))
                    store(side, chunk, t, value)
            return carry
        return body

    def store_partial(side, chunk, t, value):
        put(T, side, chunk, tile(t), value)

    def store_out(side, chunk, t, value):
        block = side * CHUNKS + chunk
        sign = SG[tile(t, block * ROWS), :]
        at = pl.multiple_of(block * CHUNK + 2 * SUB * t, 2 * SUB)
        for part in range(2):
            OUT[pl.ds(at + part, SUB, stride=2), :] = value[part] * sign

    tables = {k: weights(k) for k in (2, 3)}
    cross = (zero_pair, zero_pair)
    with scope('w_s2'):
        wait_bytes(R2.at[:, 0], s2r.at[0])
    with scope('x0'):
        cross = lax.fori_loop(0, TILES, add_cross(0), cross, unroll=2)
    with scope('w_s2'):
        wait_bytes(R2.at[:, 0], s2r.at[1])
    with scope('x1'):
        cross = lax.fori_loop(0, TILES, add_cross(1), cross, unroll=2)

    def signed(parts, bit):
        acc = parts[0]
        for index, part in enumerate(parts[1:], 1):
            acc = acc - part if (index >> bit) & 1 else acc + part
        return acc

    def z_part():
        return remote(V, VP, zs, zp, dev_c)

    def z_copy(chip, core):
        dev = me + (chip // 2) * step_y + (chip % 2) * step_x + core * step_c
        return remote(V, VR.at[chip], zs, zr, dev)

    def send_sum():
        with scope('w_zp'):
            wait_bytes(VP, zp)
        total = V[...] + VP[...]
        V[...] = total
        VR[0] = total

    def spread_sum():
        for chip in reversed(range(CHIPS)):
            for core in reversed(range(2)):
                if chip or core:
                    z_copy(chip, core).start()

    row_index = lax.broadcasted_iota(jnp.int32, (3 * SUB, LANES), 0)
    col_index = lax.broadcasted_iota(jnp.int32, (3 * SUB, LANES), 1)
    with scope('zsum'):
        signs = [plus_minus(bit).astype(F32) for bit in (bit_y, bit_x, bit_c)]
        norm_rows = [fold(part) for part in norms]
        tot_row = norm_rows[0] + norm_rows[1]
        rows = []
        for half, bit in enumerate(second_bit):
            weight_0, weight_1, mix_re, mix_im = pair_weights(matrix(half))
            re, im = cross[half]
            rows.append(jnp.where(bit == 1, weight_1, weight_0) * norm_rows[half] + mix_re * fold(re)
                        + (mix_im * signs[half]) * fold(im) + signs[half] * norm_rows[1 - half])
        rows += [signs[2] * tot_row] + raw_rows
        parts = [TP[tile(t), :] for t in range(TILES)]
        rows += [fold(signed(parts, bit)) for bit in reversed(range(4))]
        total = norms[0] + norms[1]
        rows += [fold(total * plus_minus((sub >> bit) & 1).astype(F32)) for bit in reversed(range(3))]
        rows += [tot_row * plus_minus((lane[:1] >> bit) & 1).astype(F32) for bit in reversed(range(7))]
        rows += [jnp.zeros_like(tot_row)] * 4
        column = jnp.sum(jnp.concatenate(rows, axis=0), axis=1, keepdims=True)
        mine = jnp.sum(jnp.where(row_index == col_index, column, 0.0), axis=0, keepdims=True)
        V[...] = mine
    pl.when(bit_c == 1)(send_sum)
    pl.when(bit_c == 0)(lambda: z_part().start())
    pl.when(bit_c == 1)(spread_sum)
    for piece in range(len(PIECES) - 1):
        for half in range(2):
            stage2(half, 3, piece).start()
    with scope('own'):
        lax.fori_loop(0, TILES, step_own, 0)
        lax.fori_loop(0, TILES, step_mix, 0)
    with scope('w_s2'):
        wait_bytes(R2.at[:, 0], s2r.at[2])
    with scope('st2'):
        lax.fori_loop(0, TILES, add_received(2, tables[2], store_partial), 0)

    for piece in range(len(PIECES) - 1):
        low, high = PIECES[piece], PIECES[piece + 1]
        with scope('w_s2'):
            wait_bytes(R2.at[:, 0, :, low:high], piece_sems[piece])
        with scope('tail'):
            lax.fori_loop(low // SUB, high // SUB, add_received(3, tables[3], store_out), 0)
        if piece == len(PIECES) - 3:
            with scope('w_z'):
                pl.when(bit_c == 0)(lambda: wait_bytes(VR, zr))
                pl.when(bit_c == 1)(lambda: wait_bytes(VR.at[1:CHIPS], zr))
            acc = VR[0]
            for chip in range(1, CHIPS):
                acc = acc + VR[chip]
            z_ref[...] = acc[:, :QUBITS] / 2 ** QUBITS

    with scope('w_send'):
        wait_bytes(BIG, sent_sem)
        pl.when(bit_c == 0)(lambda: wait_bytes(VP, zs))
        pl.when(bit_c == 1)(lambda: wait_bytes(V7, zs))


def writer(state_ref, z_ref, state_out, z_out, sems):
    copies = [pltpu.make_async_copy(state_ref, state_out, sems.at[0]), pltpu.make_async_copy(z_ref, z_out, sems.at[1])]
    for copy in copies:
        copy.start()
    for copy in copies:
        copy.wait()


def solution(mesh):
    def local_layer(state_local, unitaries, cz_pairs):
        size = state_local.shape[1]
        rows = 2 * size // LANES
        x = state_local.reshape(2, -1, LANES).swapaxes(0, 1).reshape(rows, LANES)
        u = unitaries.transpose(0, 2, 3, 1).reshape(SUB, QUBITS)
        cz = cz_pairs.T
        x, u, cz = [pltpu.with_memory_space_constraint(v, pltpu.HBM) for v in (x, u, cz)]
        vm = pltpu.VMEM
        dma = pltpu.SemaphoreType.DMA
        halves = vm((2, CHUNKS, 2, ROWS, LANES), F32)
        square = vm((2 * LANES, 2 * LANES), F32)
        any_spec = pl.BlockSpec(memory_space=pl.ANY)
        shapes = (jax.ShapeDtypeStruct((rows, LANES), F32), jax.ShapeDtypeStruct((1, QUBITS), F32))
        out, z = pl.pallas_call(
            kernel,
            out_shape=shapes,
            in_specs=[pl.BlockSpec(memory_space=pltpu.HBM)] * 3,
            out_specs=(pl.BlockSpec(memory_space=pltpu.VMEM), pl.BlockSpec(memory_space=pltpu.VMEM)),
            scratch_shapes=[
                vm((4 * rows, LANES), F32), pltpu.SMEM(u.shape, F32), pltpu.SMEM(cz.shape, jnp.int32), halves, halves, halves,
                vm((rows // 2, LANES), F32), square, square, square, square, vm((ROWS, LANES), F32),
                vm((1, LANES), F32), vm((1, LANES), F32), vm((CHIPS, 1, LANES), F32), vm((2 * CHIPS - 1, 1, LANES), F32),
                dma((3,)), dma, dma((4,)), dma((4,)), dma((3,)), dma, dma, pltpu.SemaphoreType.REGULAR,
            ],
            compiler_params=pltpu.CompilerParams(collective_id=0, has_side_effects=True, vmem_limit_bytes=40 * 2 ** 20),
        )(x, u, cz)
        out, z = pl.pallas_call(
            writer, out_shape=shapes, in_specs=[any_spec] * 2, out_specs=(any_spec,) * 2, scratch_shapes=[dma((2,))],
            compiler_params=pltpu.CompilerParams(vmem_limit_bytes=2 ** 20),
        )(out, z)
        state = out.reshape(-1, 2, LANES).swapaxes(0, 1).reshape(2, size)
        return state, z.reshape(QUBITS)

    return jax.shard_map(local_layer, mesh=mesh, in_specs=(P(None, 'q'), P(), P()), out_specs=(P(None, 'q'), P()), check_vma=False)
```

```python
import jax
import jax.numpy as jnp
from jax import lax
from jax.experimental import pallas as pl
from jax.experimental.pallas import tpu as pltpu
from jax.sharding import PartitionSpec as P

MESH = pl.DeviceIdType.MESH
F32 = jnp.float32
LANES = 128
SUB = 8
TILES = 16
LOW, HIGH = slice(0, LANES), slice(LANES, 2 * LANES)
ROWS = SUB * TILES
CHUNK = 2 * ROWS
CHUNKS = 4
PIECES = (0, 16, 64, 112, 128)
FIRST = CHUNK // 4
DEVICES = 8
CHIPS = 4
OUT_PARTS = 32
QUBITS = 20
scope = jax.named_scope


def cmul(a, b):
    (a_re, a_im), (b_re, b_im) = a, b
    return a_re * b_re - a_im * b_im, a_re * b_im + a_im * b_re


def cadd(a, b):
    (a_re, a_im), (b_re, b_im) = a, b
    return a_re + b_re, a_im + b_im


def conj_mul(a, b):
    (a_re, a_im), (b_re, b_im) = a, b
    return a_re * b_re + a_im * b_im, a_re * b_im - a_im * b_re


def mix(coefs, values):
    total = None
    for coef, value in zip(coefs, values):
        part = cmul(coef, value)
        total = part if total is None else cadd(total, part)
    return total


def gate(mat, zero, one):
    u00, u01, u10, u11 = mat
    return mix((u00, u01), (zero, one)), mix((u10, u11), (zero, one))


def norm(a):
    re, im = a
    return re * re + im * im


def plus_minus(bit):
    return 1 - 2 * bit


def planes(ref, half, chunk, rows):
    return [ref[half, chunk, part, rows, :] for part in range(2)]


def put(ref, half, chunk, rows, value):
    for part in range(2):
        ref[half, chunk, part, rows, :] = value[part]


def tile(t, first=0):
    return pl.ds(pl.multiple_of(first + SUB * t, SUB), SUB)


def kernel(x_hbm, u_hbm, cz_hbm, OUT, z_ref,
           BIG, u_ref, cz_ref, S, R2, T, SG, GM, KM, XC, ZC, TP, V, VP, VR, V7,
           ld, sent_sem, s1r, fw, s2r, zs, zp, ready):
    zr = ld.at[2]
    fwr = [fw, ld.at[0], ld.at[1], fw]
    piece_sems = [s1r.at[0], s1r.at[1], s1r.at[2], ld.at[0]]
    size = BIG.shape[0] // 4
    X, RB, XP, RP = [BIG.at[pl.ds(part * size, size)] for part in range(4)]
    me = lax.axis_index('q')
    bit_y = me // 4
    bit_x = (me // 2) % 2
    bit_c = me % 2
    step_y, step_x, step_c = 4 * plus_minus(bit_y), 2 * plus_minus(bit_x), plus_minus(bit_c)
    dev_y, dev_x, dev_c = me + step_y, me + step_x, me + step_c
    first_dev = (dev_x, dev_y)
    second_dev = (dev_y, dev_x)
    second_bit = (bit_y, bit_x)

    def sent(half, k):
        return k + second_bit[half] * (3 - 2 * k)

    def received(half, k):
        return 3 - k + second_bit[half] * (2 * k - 3)

    def block_rows(half, chunk):
        return pl.ds(pl.multiple_of((half * CHUNKS + chunk) * CHUNK, CHUNK), CHUNK)

    def remote(src, dst, send, recv, dev):
        return pltpu.make_async_remote_copy(src_ref=src, dst_ref=dst, send_sem=send, recv_sem=recv,
                                            device_id=(dev,), device_id_type=MESH)

    def wait_bytes(ref, sem):
        pltpu.make_async_copy(ref, ref, sem).wait()

    def part_rows(half, k, part):
        low, size = ((0, FIRST), (FIRST, CHUNK - FIRST))[part] if k == 0 else (0, CHUNK)
        return pl.ds(pl.multiple_of((half * CHUNKS + sent(half, k)) * CHUNK + low, SUB), size)

    def load_copy(half, k, part=0):
        rows = part_rows(half, k, part)
        return pltpu.make_async_copy(x_hbm.at[rows], X.at[rows], ld.at[min(2, k + 1) if k else part])

    def stage1(half, k, part=0):
        rows = part_rows(half, k, part)
        return remote(X.at[rows], RB.at[rows], sent_sem, s1r.at[k], first_dev[half])

    def core_copy(half, k):
        rows = block_rows(half, sent(half, k))
        return remote(X.at[rows], XP.at[rows], sent_sem, fw, dev_c)

    def forward(half, k):
        rows = block_rows(half, sent(half, k))
        return remote(RB.at[rows], RP.at[rows], sent_sem, fwr[k], dev_c)

    def stage2(half, k, piece=None):
        chunk = sent(half, k)
        if piece is None:
            return remote(S.at[half, chunk], R2.at[half, chunk], sent_sem, s2r.at[k], second_dev[half])
        rows = pl.ds(PIECES[piece], PIECES[piece + 1] - PIECES[piece])
        return remote(S.at[half, chunk, :, rows], R2.at[half, chunk, :, rows], sent_sem, piece_sems[piece], second_dev[half])

    u_copy = pltpu.make_async_copy(u_hbm, u_ref, zs)
    cz_copy = pltpu.make_async_copy(cz_hbm, cz_ref, zp)
    order = [(k, part) for k in range(CHUNKS) for part in range(1 if k else 2)]
    for k, part in order:
        for half in range(2):
            load_copy(half, k, part).start()

    last_chip = bit_y * bit_x
    beside = bit_y + bit_x - 2 * last_chip
    barrier = pltpu.get_barrier_semaphore()

    def signal(sem, devices):
        for dev in devices:
            pl.semaphore_signal(sem, inc=1, device_id=(dev,), device_id_type=MESH)

    signal(barrier, (dev_c,))
    pl.when(last_chip == 0)(lambda: signal(barrier, (dev_x, dev_y)))
    u_copy.start()
    cz_copy.start()

    waits = {(0, 0): (0, 2 * FIRST), (0, 1): (1, 2 * (CHUNK - FIRST)), (1, 0): (2, 6 * CHUNK)}

    def send_first(halves, wait):
        for k, part in order:
            if wait and (k, part) in waits:
                index, size = waits[k, part]
                wait_bytes(X.at[:size], ld.at[index])
            if k == 0:
                for half in halves:
                    stage1(half, k, part).start()
        pl.when(bit_c == 0)(lambda: send_rest(halves))

    def send_rest(halves):
        for k in range(1, CHUNKS):
            for half in halves:
                stage1(half, k).start()

    def send_beside(half):
        send_first((half,), True)
        with scope('w_rdy'):
            pl.semaphore_wait(ready, 1)
        send_first((1 - half,), False)

    with scope('bar'):
        pl.when(beside == 1)(lambda: pl.semaphore_wait(barrier, 2))
        pl.when(beside == 0)(lambda: pl.semaphore_wait(barrier, 3))
    pl.when(last_chip == 1)(lambda: signal(ready, (dev_x, dev_y)))
    with scope('first'):
        pl.when(beside == 0)(lambda: send_first((0, 1), True))
        pl.when(beside * bit_x == 1)(lambda: send_beside(0))
        pl.when(beside * bit_y == 1)(lambda: send_beside(1))
    for k in range(CHUNKS):
        for half in range(2):
            core_copy(half, k).start()
    u_copy.wait()
    cz_copy.wait()

    def entry(qubit, row, col):
        return u_ref[row * 2 + col, qubit], u_ref[4 + row * 2 + col, qubit]

    def matrix(qubit, flip=0):
        return [entry(qubit, row + flip * plus_minus(row), col + flip * plus_minus(col)) for row in range(2) for col in range(2)]

    lane = lax.broadcasted_iota(jnp.int32, (SUB, LANES), 1)
    sub = lax.broadcasted_iota(jnp.int32, (SUB, LANES), 0)

    def build(t, carry):
        row = sub + SUB * t
        for base, left in ((6, True), (13, False)):
            re = im = None
            for j in range(7):
                shift = 6 - j
                row_bit = ((row >> shift) & 1) == 1
                col_bit = ((lane >> shift) & 1) == 1
                fac = []
                for ri in range(2):
                    u00, u01, u10, u11 = [u_ref[4 * ri + k, base + j] for k in range(4)]
                    if not left:
                        u01, u10 = u10, u01
                    fac.append(jnp.where(row_bit, jnp.where(col_bit, u11, u10), jnp.where(col_bit, u01, u00)))
                if re is None:
                    re, im = fac
                else:
                    re, im = cmul((re, im), fac)
            low, high = tile(t), tile(t, LANES)
            dest, upper, lower = (GM, -im, im) if left else (KM, im, -im)
            dest[low, LOW] = re
            dest[low, HIGH] = upper
            dest[high, LOW] = lower
            dest[high, HIGH] = re
        return carry

    with scope('build'):
        lax.fori_loop(0, TILES, build, 0)

    shifts = [[QUBITS - 1 - cz_ref[side, k] for side in range(2)] for k in range(QUBITS // 2)]

    def build_signs(t, carry):
        flat = (me * DEVICES * ROWS + sub + SUB * t) * LANES + lane
        parity = jnp.zeros_like(flat)
        for shift_a, shift_b in shifts:
            parity = parity ^ ((flat >> shift_a) & (flat >> shift_b))
        SG[tile(t), :] = plus_minus(parity & 1).astype(F32)
        return carry

    with scope('signs'):
        lax.fori_loop(0, DEVICES * TILES, build_signs, 0, unroll=4)

    def strided(ref, at):
        return [ref[pl.ds(at + part, SUB, stride=2), :] for part in range(2)]

    zero_tile = jnp.zeros((SUB, LANES), F32)
    zero_pair = (zero_tile, zero_tile)

    def raw_sums(t, carry):
        total, sums = carry
        value = [strided(X, pl.multiple_of(block * CHUNK + 2 * SUB * t, 2 * SUB)) for block in range(DEVICES)]
        dens = [norm(v) for v in value]
        done = []
        for (diff, cross), bit in zip(sums, (4, 2, 1)):
            for block in range(DEVICES):
                if block & bit:
                    diff = diff - dens[block]
                else:
                    diff = diff + dens[block]
                    cross = cadd(cross, conj_mul(value[block], value[block + bit]))
            done.append((diff, cross))
        for part in dens:
            total = total + part
        return total, tuple(done)

    with scope('raw'):
        raw_total, raw = lax.fori_loop(0, TILES, raw_sums, (zero_tile, ((zero_tile, zero_pair),) * 3))

    def fold(part):
        return jnp.sum(part, axis=0, keepdims=True)

    def pair_weights(mat):
        u00, u01, u10, u11 = mat
        (a_re, a_im), (b_re, b_im) = conj_mul(u00, u01), conj_mul(u10, u11)
        return norm(u00) - norm(u10), norm(u01) - norm(u11), 2 * (a_re - b_re), 2 * (b_im - a_im)

    raw_rows = []
    raw_total = fold(raw_total)
    for qubit, (diff, (re, im)) in zip((3, 4, 5), raw):
        weight_0, weight_1, mix_re, mix_im = pair_weights(matrix(qubit))
        even, odd = raw_total + fold(diff), raw_total - fold(diff)
        raw_rows.append((weight_0 * even + weight_1 * odd) / 2 + mix_re * fold(re) + mix_im * fold(im))

    def gate_pair(qubit, own_bit):
        return entry(qubit, own_bit, own_bit), entry(qubit, own_bit, 1 - own_bit)

    coef_y = gate_pair(0, bit_y)
    coef_x = gate_pair(1, bit_x)
    coef_c = gate_pair(2, bit_c)
    stage1_coefs = [[cmul(top, core) for core in coef_c for top in coef] for coef in (coef_x, coef_y)]

    norms = zero_pair
    for k in range(CHUNKS):
        with scope('w_s1'):
            wait_bytes(RB.at[0:2 * CHUNK], s1r.at[k])
        for half in range(2):
            forward(half, k).start()
        if k == 0:
            pl.when(bit_c == 1)(lambda: send_rest((0, 1)))
        else:
            for half in range(2):
                stage2(half, k - 1).start()
        with scope('w_fw'):
            wait_bytes(BIG.at[0:2 * CHUNK + (0 if k else size)], fwr[k])

        for half in range(2):
            coefs = stage1_coefs[half]
            base = (half * CHUNKS + sent(half, k)) * CHUNK

            def combine(t, carry, base=base, coefs=coefs, half=half):
                at = pl.multiple_of(base + 2 * SUB * t, 2 * SUB)
                re, im = mix(coefs, [strided(ref, at) for ref in (X, RB, XP, RP)])
                XC[tile(t), (LOW, HIGH)[half]] = re
                XC[tile(t, LANES), (LOW, HIGH)[half]] = im
                return carry

            with scope('comb'):
                lax.fori_loop(0, TILES, combine, 0, unroll=2)
        with scope('mm'):
            left = lax.dot(GM[...], XC[...], precision=lax.Precision.HIGHEST, preferred_element_type=F32)
            for rows in (LOW, HIGH):
                for cols in (LOW, HIGH):
                    ZC[cols, rows] = left[rows, cols]
            both = lax.dot(ZC[...], KM[...], precision=lax.Precision.HIGHEST, preferred_element_type=F32)
            for half in range(2):
                for part in range(2):
                    S[half, sent(half, k), part] = both[(LOW, HIGH)[half], (LOW, HIGH)[part]]

        def mid_sums(t, sums, k=k):
            dens = [norm(planes(S, half, sent(half, k), tile(t))) for half in range(2)]
            row = dens[0] + dens[1]
            TP[tile(t), :] = row if k == 0 else TP[tile(t), :] + row
            return tuple(a + b for a, b in zip(sums, dens))

        with scope('dens'):
            norms = lax.fori_loop(0, TILES, mid_sums, norms, unroll=2)

    flips = (1 - bit_y, 1 - bit_x)
    u3 = matrix(3)
    u4 = [matrix(4, flip) for flip in flips]
    u5 = [matrix(5, flip) for flip in flips]
    second_coef = (coef_y, coef_x)

    def weights(k):
        table = {}
        for half in range(2):
            index = received(half, k)
            for chunk in range(CHUNKS):
                inner = cmul(entry(4, chunk // 2, index // 2), entry(5, chunk % 2, index % 2))
                inner = cmul(second_coef[half][1], inner)
                for side in range(2):
                    table[side, chunk, half] = cmul(u3[2 * side + half], inner)
        return table

    def add_cross(k):
        def body(t, cross):
            done = []
            for half in range(2):
                chunk = received(half, k)
                part = conj_mul(planes(S, half, chunk, tile(t)), planes(R2, half, chunk, tile(t)))
                done.append(cadd(cross[half], part))
            return tuple(done)
        return body

    def step_own(t, carry):
        rows = tile(t)
        for half in range(2):
            own, other = second_coef[half]
            value = []
            for k in range(CHUNKS):
                chunk = received(half, k)
                part = cmul(own, planes(S, half, chunk, rows))
                value.append(cadd(part, cmul(other, planes(R2, half, chunk, rows))) if k < 2 else part)
            value = [v for pair in (value[:2], value[2:]) for v in gate(u5[half], *pair)]
            value = [gate(u4[half], value[k], value[k + 2]) for k in range(2)]
            for k in range(CHUNKS):
                put(T, half, received(half, k), rows, value[k % 2][k // 2])
        return carry

    def step_mix(t, carry):
        rows = tile(t)
        for chunk in range(CHUNKS):
            for half, value in enumerate(gate(u3, planes(T, 0, chunk, rows), planes(T, 1, chunk, rows))):
                put(T, half, chunk, rows, value)
        return carry

    def add_received(k, table, store):
        def body(t, carry):
            rows = tile(t)
            other = [planes(R2, half, received(half, k), rows) for half in range(2)]
            for side in range(2):
                for chunk in range(CHUNKS):
                    value = planes(T, side, chunk, rows)
                    for half in range(2):
                        value = cadd(value, cmul(table[side, chunk, half], other[half]))
                    store(side, chunk, t, value)
            return carry
        return body

    def store_partial(side, chunk, t, value):
        put(T, side, chunk, tile(t), value)

    def store_out(side, chunk, t, value):
        block = side * CHUNKS + chunk
        sign = SG[tile(t, block * ROWS), :]
        at = pl.multiple_of(block * CHUNK + 2 * SUB * t, 2 * SUB)
        for part in range(2):
            OUT[pl.ds(at + part, SUB, stride=2), :] = value[part] * sign

    tables = {k: weights(k) for k in (2, 3)}
    cross = (zero_pair, zero_pair)
    with scope('w_s2'):
        wait_bytes(R2.at[:, 0], s2r.at[0])
    with scope('x0'):
        cross = lax.fori_loop(0, TILES, add_cross(0), cross, unroll=2)
    with scope('w_s2'):
        wait_bytes(R2.at[:, 0], s2r.at[1])
    with scope('x1'):
        cross = lax.fori_loop(0, TILES, add_cross(1), cross, unroll=2)

    def signed(parts, bit):
        acc = parts[0]
        for index, part in enumerate(parts[1:], 1):
            acc = acc - part if (index >> bit) & 1 else acc + part
        return acc

    def z_part():
        return remote(V, VP, zs, zp, dev_c)

    def z_copy(chip, core):
        dev = me + (chip // 2) * step_y + (chip % 2) * step_x + core * step_c
        return remote(V, VR.at[chip], zs, zr, dev)

    def send_sum():
        with scope('w_zp'):
            wait_bytes(VP, zp)
        total = V[...] + VP[...]
        V[...] = total
        VR[0] = total

    def spread_sum():
        for chip in reversed(range(CHIPS)):
            for core in reversed(range(2)):
                if chip or core:
                    z_copy(chip, core).start()

    row_index = lax.broadcasted_iota(jnp.int32, (3 * SUB, LANES), 0)
    col_index = lax.broadcasted_iota(jnp.int32, (3 * SUB, LANES), 1)
    with scope('zsum'):
        signs = [plus_minus(bit).astype(F32) for bit in (bit_y, bit_x, bit_c)]
        norm_rows = [fold(part) for part in norms]
        tot_row = norm_rows[0] + norm_rows[1]
        rows = []
        for half, bit in enumerate(second_bit):
            weight_0, weight_1, mix_re, mix_im = pair_weights(matrix(half))
            re, im = cross[half]
            rows.append(jnp.where(bit == 1, weight_1, weight_0) * norm_rows[half] + mix_re * fold(re)
                        + (mix_im * signs[half]) * fold(im) + signs[half] * norm_rows[1 - half])
        rows += [signs[2] * tot_row] + raw_rows
        parts = [TP[tile(t), :] for t in range(TILES)]
        rows += [fold(signed(parts, bit)) for bit in reversed(range(4))]
        total = norms[0] + norms[1]
        rows += [fold(total * plus_minus((sub >> bit) & 1).astype(F32)) for bit in reversed(range(3))]
        rows += [tot_row * plus_minus((lane[:1] >> bit) & 1).astype(F32) for bit in reversed(range(7))]
        rows += [jnp.zeros_like(tot_row)] * 4
        column = jnp.sum(jnp.concatenate(rows, axis=0), axis=1, keepdims=True)
        mine = jnp.sum(jnp.where(row_index == col_index, column, 0.0), axis=0, keepdims=True)
        V[...] = mine
    pl.when(bit_c == 1)(send_sum)
    pl.when(bit_c == 0)(lambda: z_part().start())
    pl.when(bit_c == 1)(spread_sum)
    for piece in range(len(PIECES) - 1):
        for half in range(2):
            stage2(half, 3, piece).start()
    with scope('own'):
        lax.fori_loop(0, TILES, step_own, 0)
        lax.fori_loop(0, TILES, step_mix, 0)
    with scope('w_s2'):
        wait_bytes(R2.at[:, 0], s2r.at[2])
    with scope('st2'):
        lax.fori_loop(0, TILES, add_received(2, tables[2], store_partial), 0)

    for piece in range(len(PIECES) - 1):
        low, high = PIECES[piece], PIECES[piece + 1]
        with scope('w_s2'):
            wait_bytes(R2.at[:, 0, :, low:high], piece_sems[piece])
        with scope('tail'):
            lax.fori_loop(low // SUB, high // SUB, add_received(3, tables[3], store_out), 0)
        if piece == len(PIECES) - 3:
            with scope('w_z'):
                pl.when(bit_c == 0)(lambda: wait_bytes(VR, zr))
                pl.when(bit_c == 1)(lambda: wait_bytes(VR.at[1:CHIPS], zr))
            acc = VR[0]
            for chip in range(1, CHIPS):
                acc = acc + VR[chip]
            z_ref[...] = acc[:, :QUBITS] / 2 ** QUBITS

    with scope('w_send'):
        wait_bytes(BIG, sent_sem)
        pl.when(bit_c == 0)(lambda: wait_bytes(VP, zs))
        pl.when(bit_c == 1)(lambda: wait_bytes(V7, zs))


def writer(state_ref, z_ref, state_out, z_out, sems):
    size = state_ref.shape[0] // OUT_PARTS
    for part in range(OUT_PARTS):
        rows = pl.ds(part * size, size)
        pltpu.make_async_copy(state_ref.at[rows], state_out.at[rows], sems.at[0]).start(priority=part % 2)
    copy = pltpu.make_async_copy(z_ref, z_out, sems.at[1])
    copy.start()
    pltpu.make_async_copy(state_ref, state_out, sems.at[0]).wait()
    copy.wait()


def solution(mesh):
    def local_layer(state_local, unitaries, cz_pairs):
        size = state_local.shape[1]
        rows = 2 * size // LANES
        x = state_local.reshape(2, -1, LANES).swapaxes(0, 1).reshape(rows, LANES)
        u = unitaries.transpose(0, 2, 3, 1).reshape(SUB, QUBITS)
        cz = cz_pairs.T
        x, u, cz = [pltpu.with_memory_space_constraint(v, pltpu.HBM) for v in (x, u, cz)]
        vm = pltpu.VMEM
        dma = pltpu.SemaphoreType.DMA
        halves = vm((2, CHUNKS, 2, ROWS, LANES), F32)
        square = vm((2 * LANES, 2 * LANES), F32)
        any_spec = pl.BlockSpec(memory_space=pl.ANY)
        shapes = (jax.ShapeDtypeStruct((rows, LANES), F32), jax.ShapeDtypeStruct((1, QUBITS), F32))
        out, z = pl.pallas_call(
            kernel,
            out_shape=shapes,
            in_specs=[pl.BlockSpec(memory_space=pltpu.HBM)] * 3,
            out_specs=(pl.BlockSpec(memory_space=pltpu.VMEM), pl.BlockSpec(memory_space=pltpu.VMEM)),
            scratch_shapes=[
                vm((4 * rows, LANES), F32), pltpu.SMEM(u.shape, F32), pltpu.SMEM(cz.shape, jnp.int32), halves, halves, halves,
                vm((rows // 2, LANES), F32), square, square, square, square, vm((ROWS, LANES), F32),
                vm((1, LANES), F32), vm((1, LANES), F32), vm((CHIPS, 1, LANES), F32), vm((2 * CHIPS - 1, 1, LANES), F32),
                dma((3,)), dma, dma((4,)), dma, dma((3,)), dma, dma, pltpu.SemaphoreType.REGULAR,
            ],
            compiler_params=pltpu.CompilerParams(collective_id=0, has_side_effects=True, vmem_limit_bytes=40 * 2 ** 20),
        )(x, u, cz)
        out, z = pl.pallas_call(
            writer, out_shape=shapes, in_specs=[any_spec] * 2, out_specs=(any_spec,) * 2, scratch_shapes=[dma((2,))],
            compiler_params=pltpu.CompilerParams(vmem_limit_bytes=2 ** 20),
        )(out, z)
        state = out.reshape(-1, 2, LANES).swapaxes(0, 1).reshape(2, size)
        return state, z.reshape(QUBITS)

    return jax.shard_map(local_layer, mesh=mesh, in_specs=(P(None, 'q'), P(), P()), out_specs=(P(None, 'q'), P()), check_vma=False)
```

```python
import jax
import jax.numpy as jnp
from jax import lax
from jax.experimental import pallas as pl
from jax.experimental.pallas import tpu as pltpu
from jax.sharding import PartitionSpec as P

MESH = pl.DeviceIdType.MESH
F32 = jnp.float32
LANES = 128
SUB = 8
TILES = 16
LOW, HIGH = slice(0, LANES), slice(LANES, 2 * LANES)
ROWS = SUB * TILES
CHUNK = 2 * ROWS
CHUNKS = 4
PIECES = (0, 24, 96, 120, 128)
FIRST = 3 * CHUNK // 16
DEVICES = 8
CHIPS = 4
OUT_PARTS = 32
QUBITS = 20
scope = jax.named_scope


def cmul(a, b):
    (a_re, a_im), (b_re, b_im) = a, b
    return a_re * b_re - a_im * b_im, a_re * b_im + a_im * b_re


def cadd(a, b):
    (a_re, a_im), (b_re, b_im) = a, b
    return a_re + b_re, a_im + b_im


def conj_mul(a, b):
    (a_re, a_im), (b_re, b_im) = a, b
    return a_re * b_re + a_im * b_im, a_re * b_im - a_im * b_re


def mix(coefs, values):
    total = None
    for coef, value in zip(coefs, values):
        part = cmul(coef, value)
        total = part if total is None else cadd(total, part)
    return total


def gate(mat, zero, one):
    u00, u01, u10, u11 = mat
    return mix((u00, u01), (zero, one)), mix((u10, u11), (zero, one))


def norm(a):
    re, im = a
    return re * re + im * im


def plus_minus(bit):
    return 1 - 2 * bit


def planes(ref, half, chunk, rows):
    return [ref[half, chunk, part, rows, :] for part in range(2)]


def put(ref, half, chunk, rows, value):
    for part in range(2):
        ref[half, chunk, part, rows, :] = value[part]


def tile(t, first=0):
    return pl.ds(pl.multiple_of(first + SUB * t, SUB), SUB)


def kernel(x_hbm, u_hbm, cz_hbm, OUT, z_ref,
           BIG, u_ref, cz_ref, S, R2, T, SG, GM, KM, XC, ZC, TP, V, VP, VR, V7,
           ld, sent_sem, s1r, fw, s2r, zs, zp, ready):
    zr = ld.at[2]
    fwr = [fw, ld.at[0], ld.at[1], fw]
    piece_sems = [s1r.at[0], s1r.at[1], s1r.at[2], ld.at[0]]
    size = BIG.shape[0] // 4
    X, RB, XP, RP = [BIG.at[pl.ds(part * size, size)] for part in range(4)]
    me = lax.axis_index('q')
    bit_y = me // 4
    bit_x = (me // 2) % 2
    bit_c = me % 2
    step_y, step_x, step_c = 4 * plus_minus(bit_y), 2 * plus_minus(bit_x), plus_minus(bit_c)
    dev_y, dev_x, dev_c = me + step_y, me + step_x, me + step_c
    first_dev = (dev_x, dev_y)
    second_dev = (dev_y, dev_x)
    second_bit = (bit_y, bit_x)

    def sent(half, k):
        return k + second_bit[half] * (3 - 2 * k)

    def received(half, k):
        return 3 - k + second_bit[half] * (2 * k - 3)

    def block_rows(half, chunk):
        return pl.ds(pl.multiple_of((half * CHUNKS + chunk) * CHUNK, CHUNK), CHUNK)

    def remote(src, dst, send, recv, dev):
        return pltpu.make_async_remote_copy(src_ref=src, dst_ref=dst, send_sem=send, recv_sem=recv,
                                            device_id=(dev,), device_id_type=MESH)

    def wait_bytes(ref, sem):
        pltpu.make_async_copy(ref, ref, sem).wait()

    def part_rows(half, k, part):
        low, size = ((0, FIRST), (FIRST, CHUNK - FIRST))[part] if k == 0 else (0, CHUNK)
        return pl.ds(pl.multiple_of((half * CHUNKS + sent(half, k)) * CHUNK + low, SUB), size)

    def load_copy(half, k, part=0):
        rows = part_rows(half, k, part)
        return pltpu.make_async_copy(x_hbm.at[rows], X.at[rows], ld.at[min(2, k + 1) if k else part])

    def stage1(half, k, part=0):
        rows = part_rows(half, k, part)
        return remote(X.at[rows], RB.at[rows], sent_sem, s1r.at[k], first_dev[half])

    def core_copy(half, k):
        rows = block_rows(half, sent(half, k))
        return remote(X.at[rows], XP.at[rows], sent_sem, fw, dev_c)

    def forward(half, k):
        rows = block_rows(half, sent(half, k))
        return remote(RB.at[rows], RP.at[rows], sent_sem, fwr[k], dev_c)

    def stage2(half, k, piece=None):
        chunk = sent(half, k)
        if piece is None:
            return remote(S.at[half, chunk], R2.at[half, chunk], sent_sem, s2r.at[k], second_dev[half])
        rows = pl.ds(PIECES[piece], PIECES[piece + 1] - PIECES[piece])
        return remote(S.at[half, chunk, :, rows], R2.at[half, chunk, :, rows], sent_sem, piece_sems[piece], second_dev[half])

    u_copy = pltpu.make_async_copy(u_hbm, u_ref, zs)
    cz_copy = pltpu.make_async_copy(cz_hbm, cz_ref, zp)
    order = [(k, part) for k in range(CHUNKS) for part in range(1 if k else 2)]
    for k, part in order:
        for half in range(2):
            load_copy(half, k, part).start()

    last_chip = bit_y * bit_x
    beside = bit_y + bit_x - 2 * last_chip
    barrier = pltpu.get_barrier_semaphore()

    def signal(sem, devices):
        for dev in devices:
            pl.semaphore_signal(sem, inc=1, device_id=(dev,), device_id_type=MESH)

    signal(barrier, (dev_c,))
    pl.when(last_chip == 0)(lambda: signal(barrier, (dev_x, dev_y)))
    u_copy.start()
    cz_copy.start()

    waits = {(0, 0): (0, 2 * FIRST), (0, 1): (1, 2 * (CHUNK - FIRST)), (1, 0): (2, 6 * CHUNK)}

    def send_first(halves, wait):
        for k, part in order:
            if wait and (k, part) in waits:
                index, size = waits[k, part]
                wait_bytes(X.at[:size], ld.at[index])
            if k == 0:
                for half in halves:
                    stage1(half, k, part).start()
        pl.when(bit_c == 0)(lambda: send_rest(halves))

    def send_rest(halves):
        for k in range(1, CHUNKS):
            for half in halves:
                stage1(half, k).start()

    def send_beside(half):
        send_first((half,), True)
        with scope('w_rdy'):
            pl.semaphore_wait(ready, 1)
        send_first((1 - half,), False)

    with scope('bar'):
        pl.when(beside == 1)(lambda: pl.semaphore_wait(barrier, 2))
        pl.when(beside == 0)(lambda: pl.semaphore_wait(barrier, 3))
    pl.when(last_chip == 1)(lambda: signal(ready, (dev_x, dev_y)))
    with scope('first'):
        pl.when(beside == 0)(lambda: send_first((0, 1), True))
        pl.when(beside * bit_x == 1)(lambda: send_beside(0))
        pl.when(beside * bit_y == 1)(lambda: send_beside(1))
    for k in range(CHUNKS):
        for half in range(2):
            core_copy(half, k).start()
    u_copy.wait()
    cz_copy.wait()

    def entry(qubit, row, col):
        return u_ref[row * 2 + col, qubit], u_ref[4 + row * 2 + col, qubit]

    def matrix(qubit, flip=0):
        return [entry(qubit, row + flip * plus_minus(row), col + flip * plus_minus(col)) for row in range(2) for col in range(2)]

    lane = lax.broadcasted_iota(jnp.int32, (SUB, LANES), 1)
    sub = lax.broadcasted_iota(jnp.int32, (SUB, LANES), 0)

    def build(t, carry):
        row = sub + SUB * t
        for base, left in ((6, True), (13, False)):
            re = im = None
            for j in range(7):
                shift = 6 - j
                row_bit = ((row >> shift) & 1) == 1
                col_bit = ((lane >> shift) & 1) == 1
                fac = []
                for ri in range(2):
                    u00, u01, u10, u11 = [u_ref[4 * ri + k, base + j] for k in range(4)]
                    if not left:
                        u01, u10 = u10, u01
                    fac.append(jnp.where(row_bit, jnp.where(col_bit, u11, u10), jnp.where(col_bit, u01, u00)))
                if re is None:
                    re, im = fac
                else:
                    re, im = cmul((re, im), fac)
            low, high = tile(t), tile(t, LANES)
            dest, upper, lower = (GM, -im, im) if left else (KM, im, -im)
            dest[low, LOW] = re
            dest[low, HIGH] = upper
            dest[high, LOW] = lower
            dest[high, HIGH] = re
        return carry

    with scope('build'):
        lax.fori_loop(0, TILES, build, 0)

    shifts = [[QUBITS - 1 - cz_ref[side, k] for side in range(2)] for k in range(QUBITS // 2)]

    def build_signs(t, carry):
        flat = (me * DEVICES * ROWS + sub + SUB * t) * LANES + lane
        parity = jnp.zeros_like(flat)
        for shift_a, shift_b in shifts:
            parity = parity ^ ((flat >> shift_a) & (flat >> shift_b))
        SG[tile(t), :] = plus_minus(parity & 1).astype(F32)
        return carry

    with scope('signs'):
        lax.fori_loop(0, DEVICES * TILES, build_signs, 0, unroll=4)

    def strided(ref, at):
        return [ref[pl.ds(at + part, SUB, stride=2), :] for part in range(2)]

    zero_tile = jnp.zeros((SUB, LANES), F32)
    zero_pair = (zero_tile, zero_tile)

    def raw_sums(t, carry):
        total, sums = carry
        value = [strided(X, pl.multiple_of(block * CHUNK + 2 * SUB * t, 2 * SUB)) for block in range(DEVICES)]
        dens = [norm(v) for v in value]
        done = []
        for (diff, cross), bit in zip(sums, (4, 2, 1)):
            for block in range(DEVICES):
                if block & bit:
                    diff = diff - dens[block]
                else:
                    diff = diff + dens[block]
                    cross = cadd(cross, conj_mul(value[block], value[block + bit]))
            done.append((diff, cross))
        for part in dens:
            total = total + part
        return total, tuple(done)

    with scope('raw'):
        raw_total, raw = lax.fori_loop(0, TILES, raw_sums, (zero_tile, ((zero_tile, zero_pair),) * 3))

    def fold(part):
        return jnp.sum(part, axis=0, keepdims=True)

    def pair_weights(mat):
        u00, u01, u10, u11 = mat
        (a_re, a_im), (b_re, b_im) = conj_mul(u00, u01), conj_mul(u10, u11)
        return norm(u00) - norm(u10), norm(u01) - norm(u11), 2 * (a_re - b_re), 2 * (b_im - a_im)

    raw_rows = []
    raw_total = fold(raw_total)
    for qubit, (diff, (re, im)) in zip((3, 4, 5), raw):
        weight_0, weight_1, mix_re, mix_im = pair_weights(matrix(qubit))
        even, odd = raw_total + fold(diff), raw_total - fold(diff)
        raw_rows.append((weight_0 * even + weight_1 * odd) / 2 + mix_re * fold(re) + mix_im * fold(im))

    def gate_pair(qubit, own_bit):
        return entry(qubit, own_bit, own_bit), entry(qubit, own_bit, 1 - own_bit)

    coef_y = gate_pair(0, bit_y)
    coef_x = gate_pair(1, bit_x)
    coef_c = gate_pair(2, bit_c)
    stage1_coefs = [[cmul(top, core) for core in coef_c for top in coef] for coef in (coef_x, coef_y)]

    norms = zero_pair
    for k in range(CHUNKS):
        with scope('w_s1'):
            wait_bytes(RB.at[0:2 * CHUNK], s1r.at[k])
        for half in range(2):
            forward(half, k).start()
        if k == 0:
            pl.when(bit_c == 1)(lambda: send_rest((0, 1)))
        else:
            for half in range(2):
                stage2(half, k - 1).start()
        with scope('w_fw'):
            wait_bytes(BIG.at[0:2 * CHUNK + (0 if k else size)], fwr[k])

        for half in range(2):
            coefs = stage1_coefs[half]
            base = (half * CHUNKS + sent(half, k)) * CHUNK

            def combine(t, carry, base=base, coefs=coefs, half=half):
                at = pl.multiple_of(base + 2 * SUB * t, 2 * SUB)
                re, im = mix(coefs, [strided(ref, at) for ref in (X, RB, XP, RP)])
                XC[tile(t), (LOW, HIGH)[half]] = re
                XC[tile(t, LANES), (LOW, HIGH)[half]] = im
                return carry

            with scope('comb'):
                lax.fori_loop(0, TILES, combine, 0, unroll=2)
        with scope('mm'):
            left = lax.dot(GM[...], XC[...], precision=lax.Precision.HIGHEST, preferred_element_type=F32)
            for rows in (LOW, HIGH):
                for cols in (LOW, HIGH):
                    ZC[cols, rows] = left[rows, cols]
            both = lax.dot(ZC[...], KM[...], precision=lax.Precision.HIGHEST, preferred_element_type=F32)
            for half in range(2):
                for part in range(2):
                    S[half, sent(half, k), part] = both[(LOW, HIGH)[half], (LOW, HIGH)[part]]

        def mid_sums(t, sums, k=k):
            dens = [norm(planes(S, half, sent(half, k), tile(t))) for half in range(2)]
            row = dens[0] + dens[1]
            TP[tile(t), :] = row if k == 0 else TP[tile(t), :] + row
            return tuple(a + b for a, b in zip(sums, dens))

        with scope('dens'):
            norms = lax.fori_loop(0, TILES, mid_sums, norms, unroll=2)

    flips = (1 - bit_y, 1 - bit_x)
    u3 = matrix(3)
    u4 = [matrix(4, flip) for flip in flips]
    u5 = [matrix(5, flip) for flip in flips]
    second_coef = (coef_y, coef_x)

    def weights(k):
        table = {}
        for half in range(2):
            index = received(half, k)
            for chunk in range(CHUNKS):
                inner = cmul(entry(4, chunk // 2, index // 2), entry(5, chunk % 2, index % 2))
                inner = cmul(second_coef[half][1], inner)
                for side in range(2):
                    table[side, chunk, half] = cmul(u3[2 * side + half], inner)
        return table

    def add_cross(k):
        def body(t, cross):
            done = []
            for half in range(2):
                chunk = received(half, k)
                part = conj_mul(planes(S, half, chunk, tile(t)), planes(R2, half, chunk, tile(t)))
                done.append(cadd(cross[half], part))
            return tuple(done)
        return body

    def step_own(t, carry):
        rows = tile(t)
        for half in range(2):
            own, other = second_coef[half]
            value = []
            for k in range(CHUNKS):
                chunk = received(half, k)
                part = cmul(own, planes(S, half, chunk, rows))
                value.append(cadd(part, cmul(other, planes(R2, half, chunk, rows))) if k < 2 else part)
            value = [v for pair in (value[:2], value[2:]) for v in gate(u5[half], *pair)]
            value = [gate(u4[half], value[k], value[k + 2]) for k in range(2)]
            for k in range(CHUNKS):
                put(T, half, received(half, k), rows, value[k % 2][k // 2])
        return carry

    def step_mix(t, carry):
        rows = tile(t)
        for chunk in range(CHUNKS):
            for half, value in enumerate(gate(u3, planes(T, 0, chunk, rows), planes(T, 1, chunk, rows))):
                put(T, half, chunk, rows, value)
        return carry

    def add_received(k, table, store):
        def body(t, carry):
            rows = tile(t)
            other = [planes(R2, half, received(half, k), rows) for half in range(2)]
            for side in range(2):
                for chunk in range(CHUNKS):
                    value = planes(T, side, chunk, rows)
                    for half in range(2):
                        value = cadd(value, cmul(table[side, chunk, half], other[half]))
                    store(side, chunk, t, value)
            return carry
        return body

    def store_partial(side, chunk, t, value):
        put(T, side, chunk, tile(t), value)

    def store_out(side, chunk, t, value):
        block = side * CHUNKS + chunk
        sign = SG[tile(t, block * ROWS), :]
        at = pl.multiple_of(block * CHUNK + 2 * SUB * t, 2 * SUB)
        for part in range(2):
            OUT[pl.ds(at + part, SUB, stride=2), :] = value[part] * sign

    tables = {k: weights(k) for k in (2, 3)}
    cross = (zero_pair, zero_pair)
    with scope('w_s2'):
        wait_bytes(R2.at[:, 0], s2r.at[0])
    with scope('x0'):
        cross = lax.fori_loop(0, TILES, add_cross(0), cross, unroll=2)
    with scope('w_s2'):
        wait_bytes(R2.at[:, 0], s2r.at[1])
    with scope('x1'):
        cross = lax.fori_loop(0, TILES, add_cross(1), cross, unroll=2)

    def signed(parts, bit):
        acc = parts[0]
        for index, part in enumerate(parts[1:], 1):
            acc = acc - part if (index >> bit) & 1 else acc + part
        return acc

    def z_part():
        return remote(V, VP, zs, zp, dev_c)

    def z_copy(chip, core):
        dev = me + (chip // 2) * step_y + (chip % 2) * step_x + core * step_c
        return remote(V, VR.at[chip], zs, zr, dev)

    def send_sum():
        with scope('w_zp'):
            wait_bytes(VP, zp)
        total = V[...] + VP[...]
        V[...] = total
        VR[0] = total

    def spread_sum():
        for chip in reversed(range(CHIPS)):
            for core in reversed(range(2)):
                if chip or core:
                    z_copy(chip, core).start()

    row_index = lax.broadcasted_iota(jnp.int32, (3 * SUB, LANES), 0)
    col_index = lax.broadcasted_iota(jnp.int32, (3 * SUB, LANES), 1)
    with scope('zsum'):
        signs = [plus_minus(bit).astype(F32) for bit in (bit_y, bit_x, bit_c)]
        norm_rows = [fold(part) for part in norms]
        tot_row = norm_rows[0] + norm_rows[1]
        rows = []
        for half, bit in enumerate(second_bit):
            weight_0, weight_1, mix_re, mix_im = pair_weights(matrix(half))
            re, im = cross[half]
            rows.append(jnp.where(bit == 1, weight_1, weight_0) * norm_rows[half] + mix_re * fold(re)
                        + (mix_im * signs[half]) * fold(im) + signs[half] * norm_rows[1 - half])
        rows += [signs[2] * tot_row] + raw_rows
        parts = [TP[tile(t), :] for t in range(TILES)]
        rows += [fold(signed(parts, bit)) for bit in reversed(range(4))]
        total = norms[0] + norms[1]
        rows += [fold(total * plus_minus((sub >> bit) & 1).astype(F32)) for bit in reversed(range(3))]
        rows += [tot_row * plus_minus((lane[:1] >> bit) & 1).astype(F32) for bit in reversed(range(7))]
        rows += [jnp.zeros_like(tot_row)] * 4
        column = jnp.sum(jnp.concatenate(rows, axis=0), axis=1, keepdims=True)
        mine = jnp.sum(jnp.where(row_index == col_index, column, 0.0), axis=0, keepdims=True)
        V[...] = mine
    pl.when(bit_c == 1)(send_sum)
    pl.when(bit_c == 0)(lambda: z_part().start())
    pl.when(bit_c == 1)(spread_sum)
    for piece in range(len(PIECES) - 1):
        for half in range(2):
            stage2(half, 3, piece).start()
    with scope('own'):
        lax.fori_loop(0, TILES, step_own, 0)
        lax.fori_loop(0, TILES, step_mix, 0)
    with scope('w_s2'):
        wait_bytes(R2.at[:, 0], s2r.at[2])
    with scope('st2'):
        lax.fori_loop(0, TILES, add_received(2, tables[2], store_partial), 0)

    for piece in range(len(PIECES) - 1):
        low, high = PIECES[piece], PIECES[piece + 1]
        with scope('w_s2'):
            wait_bytes(R2.at[:, 0, :, low:high], piece_sems[piece])
        with scope('tail'):
            lax.fori_loop(low // SUB, high // SUB, add_received(3, tables[3], store_out), 0, unroll=2)
        if piece == len(PIECES) - 3:
            with scope('w_z'):
                pl.when(bit_c == 0)(lambda: wait_bytes(VR, zr))
                pl.when(bit_c == 1)(lambda: wait_bytes(VR.at[1:CHIPS], zr))
            acc = VR[0]
            for chip in range(1, CHIPS):
                acc = acc + VR[chip]
            z_ref[...] = acc[:, :QUBITS] / 2 ** QUBITS

    with scope('w_send'):
        wait_bytes(BIG, sent_sem)
        pl.when(bit_c == 0)(lambda: wait_bytes(VP, zs))
        pl.when(bit_c == 1)(lambda: wait_bytes(V7, zs))


def writer(state_ref, z_ref, state_out, z_out, sems):
    size = state_ref.shape[0] // OUT_PARTS
    for part in range(OUT_PARTS):
        rows = pl.ds(part * size, size)
        pltpu.make_async_copy(state_ref.at[rows], state_out.at[rows], sems.at[0]).start(priority=part % 2)
    copy = pltpu.make_async_copy(z_ref, z_out, sems.at[1])
    copy.start()
    pltpu.make_async_copy(state_ref, state_out, sems.at[0]).wait()
    copy.wait()


def solution(mesh):
    def local_layer(state_local, unitaries, cz_pairs):
        size = state_local.shape[1]
        rows = 2 * size // LANES
        x = state_local.reshape(2, -1, LANES).swapaxes(0, 1).reshape(rows, LANES)
        u = unitaries.transpose(0, 2, 3, 1).reshape(SUB, QUBITS)
        cz = cz_pairs.T
        x, u, cz = [pltpu.with_memory_space_constraint(v, pltpu.HBM) for v in (x, u, cz)]
        vm = pltpu.VMEM
        dma = pltpu.SemaphoreType.DMA
        halves = vm((2, CHUNKS, 2, ROWS, LANES), F32)
        square = vm((2 * LANES, 2 * LANES), F32)
        any_spec = pl.BlockSpec(memory_space=pl.ANY)
        shapes = (jax.ShapeDtypeStruct((rows, LANES), F32), jax.ShapeDtypeStruct((1, QUBITS), F32))
        out, z = pl.pallas_call(
            kernel,
            out_shape=shapes,
            in_specs=[pl.BlockSpec(memory_space=pltpu.HBM)] * 3,
            out_specs=(pl.BlockSpec(memory_space=pltpu.VMEM), pl.BlockSpec(memory_space=pltpu.VMEM)),
            scratch_shapes=[
                vm((4 * rows, LANES), F32), pltpu.SMEM(u.shape, F32), pltpu.SMEM(cz.shape, jnp.int32), halves, halves, halves,
                vm((rows // 2, LANES), F32), square, square, square, square, vm((ROWS, LANES), F32),
                vm((1, LANES), F32), vm((1, LANES), F32), vm((CHIPS, 1, LANES), F32), vm((2 * CHIPS - 1, 1, LANES), F32),
                dma((3,)), dma, dma((4,)), dma, dma((3,)), dma, dma, pltpu.SemaphoreType.REGULAR,
            ],
            compiler_params=pltpu.CompilerParams(collective_id=0, has_side_effects=True, vmem_limit_bytes=40 * 2 ** 20),
        )(x, u, cz)
        out, z = pl.pallas_call(
            writer, out_shape=shapes, in_specs=[any_spec] * 2, out_specs=(any_spec,) * 2, scratch_shapes=[dma((2,))],
            compiler_params=pltpu.CompilerParams(vmem_limit_bytes=2 ** 20),
        )(out, z)
        state = out.reshape(-1, 2, LANES).swapaxes(0, 1).reshape(2, size)
        return state, z.reshape(QUBITS)

    return jax.shard_map(local_layer, mesh=mesh, in_specs=(P(None, 'q'), P(), P()), out_specs=(P(None, 'q'), P()), check_vma=False)
```

```python
import jax
import jax.numpy as jnp
from jax import lax
from jax.experimental import pallas as pl
from jax.experimental.pallas import tpu as pltpu
from jax.sharding import PartitionSpec as P

MESH = pl.DeviceIdType.MESH
F32 = jnp.float32
LANES = 128
SUB = 8
TILES = 16
LOW, HIGH = slice(0, LANES), slice(LANES, 2 * LANES)
ROWS = SUB * TILES
CHUNK = 2 * ROWS
CHUNKS = 4
PIECES = (0, 24, 96, 120, 128)
FIRST = 3 * CHUNK // 16
DEVICES = 8
CHIPS = 4
OUT_PARTS = 32
QUBITS = 20
scope = jax.named_scope


def cmul(a, b):
    (a_re, a_im), (b_re, b_im) = a, b
    return a_re * b_re - a_im * b_im, a_re * b_im + a_im * b_re


def cadd(a, b):
    (a_re, a_im), (b_re, b_im) = a, b
    return a_re + b_re, a_im + b_im


def conj_mul(a, b):
    (a_re, a_im), (b_re, b_im) = a, b
    return a_re * b_re + a_im * b_im, a_re * b_im - a_im * b_re


def mix(coefs, values):
    total = None
    for coef, value in zip(coefs, values):
        part = cmul(coef, value)
        total = part if total is None else cadd(total, part)
    return total


def gate(mat, zero, one):
    u00, u01, u10, u11 = mat
    return mix((u00, u01), (zero, one)), mix((u10, u11), (zero, one))


def norm(a):
    re, im = a
    return re * re + im * im


def plus_minus(bit):
    return 1 - 2 * bit


def planes(ref, half, chunk, rows):
    return [ref[half, chunk, part, rows, :] for part in range(2)]


def put(ref, half, chunk, rows, value):
    for part in range(2):
        ref[half, chunk, part, rows, :] = value[part]


def tile(t, first=0):
    return pl.ds(pl.multiple_of(first + SUB * t, SUB), SUB)


def kernel(x_hbm, u_hbm, cz_hbm, OUT, z_ref,
           BIG, u_ref, cz_ref, S, R2, T, SG, GM, KM, XC, ZC, TP, V, VP, VR, V7,
           ld, sent_sem, s1r, fw, s2r, ready):
    zr, zs, zp = ld.at[2], ld.at[1], s1r.at[3]
    fwr = [fw, ld.at[0], ld.at[1], fw]
    piece_sems = [s1r.at[0], s1r.at[1], s1r.at[2], ld.at[0]]
    size = BIG.shape[0] // 4
    X, RB, XP, RP = [BIG.at[pl.ds(part * size, size)] for part in range(4)]
    me = lax.axis_index('q')
    bit_y = me // 4
    bit_x = (me // 2) % 2
    bit_c = me % 2
    step_y, step_x, step_c = 4 * plus_minus(bit_y), 2 * plus_minus(bit_x), plus_minus(bit_c)
    dev_y, dev_x, dev_c = me + step_y, me + step_x, me + step_c
    first_dev = (dev_x, dev_y)
    second_dev = (dev_y, dev_x)
    second_bit = (bit_y, bit_x)

    def sent(half, k):
        return k + second_bit[half] * (3 - 2 * k)

    def received(half, k):
        return 3 - k + second_bit[half] * (2 * k - 3)

    def block_rows(half, chunk):
        return pl.ds(pl.multiple_of((half * CHUNKS + chunk) * CHUNK, CHUNK), CHUNK)

    def remote(src, dst, send, recv, dev):
        return pltpu.make_async_remote_copy(src_ref=src, dst_ref=dst, send_sem=send, recv_sem=recv,
                                            device_id=(dev,), device_id_type=MESH)

    def wait_bytes(ref, sem):
        pltpu.make_async_copy(ref, ref, sem).wait()

    def part_rows(half, k, part):
        low, size = ((0, FIRST), (FIRST, CHUNK - FIRST))[part] if k == 0 else (0, CHUNK)
        return pl.ds(pl.multiple_of((half * CHUNKS + sent(half, k)) * CHUNK + low, SUB), size)

    def load_copy(half, k, part=0):
        rows = part_rows(half, k, part)
        return pltpu.make_async_copy(x_hbm.at[rows], X.at[rows], ld.at[min(2, k + 1) if k else part])

    def stage1(half, k, part=0):
        rows = part_rows(half, k, part)
        return remote(X.at[rows], RB.at[rows], sent_sem, s1r.at[k], first_dev[half])

    def core_copy(half, k):
        rows = block_rows(half, sent(half, k))
        return remote(X.at[rows], XP.at[rows], sent_sem, fw, dev_c)

    def forward(half, k):
        rows = block_rows(half, sent(half, k))
        return remote(RB.at[rows], RP.at[rows], sent_sem, fwr[k], dev_c)

    def stage2(half, k, piece=None):
        chunk = sent(half, k)
        if piece is None:
            return remote(S.at[half, chunk], R2.at[half, chunk], sent_sem, s2r.at[k], second_dev[half])
        rows = pl.ds(PIECES[piece], PIECES[piece + 1] - PIECES[piece])
        return remote(S.at[half, chunk, :, rows], R2.at[half, chunk, :, rows], sent_sem, piece_sems[piece], second_dev[half])

    u_copy = pltpu.make_async_copy(u_hbm, u_ref, s2r.at[0])
    cz_copy = pltpu.make_async_copy(cz_hbm, cz_ref, s2r.at[1])
    order = [(k, part) for k in range(CHUNKS) for part in range(1 if k else 2)]
    for k, part in order:
        for half in range(2):
            load_copy(half, k, part).start()

    last_chip = bit_y * bit_x
    beside = bit_y + bit_x - 2 * last_chip
    barrier = pltpu.get_barrier_semaphore()

    def signal(sem, devices):
        for dev in devices:
            pl.semaphore_signal(sem, inc=1, device_id=(dev,), device_id_type=MESH)

    signal(barrier, (dev_c,))
    pl.when(last_chip == 0)(lambda: signal(barrier, (dev_x, dev_y)))
    u_copy.start()
    cz_copy.start()

    waits = {(0, 0): (0, 2 * FIRST), (0, 1): (1, 2 * (CHUNK - FIRST)), (1, 0): (2, 6 * CHUNK)}

    def send_first(halves, wait):
        for k, part in order:
            if wait and (k, part) in waits:
                index, size = waits[k, part]
                wait_bytes(X.at[:size], ld.at[index])
                if k:
                    u_copy.wait()
                    cz_copy.wait()
            if k == 0:
                for half in halves:
                    stage1(half, k, part).start()
        pl.when(bit_c == 0)(lambda: send_rest(halves))

    def send_rest(halves):
        for k in range(1, CHUNKS):
            for half in halves:
                stage1(half, k).start()

    def send_beside(half):
        send_first((half,), True)
        with scope('w_rdy'):
            pl.semaphore_wait(ready, 1)
        send_first((1 - half,), False)

    with scope('bar'):
        pl.when(beside == 1)(lambda: pl.semaphore_wait(barrier, 2))
        pl.when(beside == 0)(lambda: pl.semaphore_wait(barrier, 3))
    pl.when(last_chip == 1)(lambda: signal(ready, (dev_x, dev_y)))
    with scope('first'):
        pl.when(beside == 0)(lambda: send_first((0, 1), True))
        pl.when(beside * bit_x == 1)(lambda: send_beside(0))
        pl.when(beside * bit_y == 1)(lambda: send_beside(1))
    for k in range(CHUNKS):
        for half in range(2):
            core_copy(half, k).start()

    def entry(qubit, row, col):
        return u_ref[row * 2 + col, qubit], u_ref[4 + row * 2 + col, qubit]

    def matrix(qubit, flip=0):
        return [entry(qubit, row + flip * plus_minus(row), col + flip * plus_minus(col)) for row in range(2) for col in range(2)]

    lane = lax.broadcasted_iota(jnp.int32, (SUB, LANES), 1)
    sub = lax.broadcasted_iota(jnp.int32, (SUB, LANES), 0)

    def build(t, carry):
        row = sub + SUB * t
        for base, left in ((6, True), (13, False)):
            re = im = None
            for j in range(7):
                shift = 6 - j
                row_bit = ((row >> shift) & 1) == 1
                col_bit = ((lane >> shift) & 1) == 1
                fac = []
                for ri in range(2):
                    u00, u01, u10, u11 = [u_ref[4 * ri + k, base + j] for k in range(4)]
                    if not left:
                        u01, u10 = u10, u01
                    fac.append(jnp.where(row_bit, jnp.where(col_bit, u11, u10), jnp.where(col_bit, u01, u00)))
                if re is None:
                    re, im = fac
                else:
                    re, im = cmul((re, im), fac)
            low, high = tile(t), tile(t, LANES)
            dest, upper, lower = (GM, -im, im) if left else (KM, im, -im)
            dest[low, LOW] = re
            dest[low, HIGH] = upper
            dest[high, LOW] = lower
            dest[high, HIGH] = re
        return carry

    with scope('build'):
        lax.fori_loop(0, TILES, build, 0)

    shifts = [[QUBITS - 1 - cz_ref[side, k] for side in range(2)] for k in range(QUBITS // 2)]

    def build_signs(t, carry):
        flat = (me * DEVICES * ROWS + sub + SUB * t) * LANES + lane
        parity = jnp.zeros_like(flat)
        for shift_a, shift_b in shifts:
            parity = parity ^ ((flat >> shift_a) & (flat >> shift_b))
        SG[tile(t), :] = plus_minus(parity & 1).astype(F32)
        return carry

    with scope('signs'):
        lax.fori_loop(0, DEVICES * TILES, build_signs, 0, unroll=4)

    def strided(ref, at):
        return [ref[pl.ds(at + part, SUB, stride=2), :] for part in range(2)]

    zero_tile = jnp.zeros((SUB, LANES), F32)
    zero_pair = (zero_tile, zero_tile)

    def raw_sums(t, carry):
        total, sums = carry
        value = [strided(X, pl.multiple_of(block * CHUNK + 2 * SUB * t, 2 * SUB)) for block in range(DEVICES)]
        dens = [norm(v) for v in value]
        done = []
        for (diff, cross), bit in zip(sums, (4, 2, 1)):
            for block in range(DEVICES):
                if block & bit:
                    diff = diff - dens[block]
                else:
                    diff = diff + dens[block]
                    cross = cadd(cross, conj_mul(value[block], value[block + bit]))
            done.append((diff, cross))
        for part in dens:
            total = total + part
        return total, tuple(done)

    with scope('raw'):
        raw_total, raw = lax.fori_loop(0, TILES, raw_sums, (zero_tile, ((zero_tile, zero_pair),) * 3))

    def fold(part):
        return jnp.sum(part, axis=0, keepdims=True)

    def pair_weights(mat):
        u00, u01, u10, u11 = mat
        (a_re, a_im), (b_re, b_im) = conj_mul(u00, u01), conj_mul(u10, u11)
        return norm(u00) - norm(u10), norm(u01) - norm(u11), 2 * (a_re - b_re), 2 * (b_im - a_im)

    raw_rows = []
    raw_total = fold(raw_total)
    for qubit, (diff, (re, im)) in zip((3, 4, 5), raw):
        weight_0, weight_1, mix_re, mix_im = pair_weights(matrix(qubit))
        even, odd = raw_total + fold(diff), raw_total - fold(diff)
        raw_rows.append((weight_0 * even + weight_1 * odd) / 2 + mix_re * fold(re) + mix_im * fold(im))

    def gate_pair(qubit, own_bit):
        return entry(qubit, own_bit, own_bit), entry(qubit, own_bit, 1 - own_bit)

    coef_y = gate_pair(0, bit_y)
    coef_x = gate_pair(1, bit_x)
    coef_c = gate_pair(2, bit_c)
    stage1_coefs = [[cmul(top, core) for core in coef_c for top in coef] for coef in (coef_x, coef_y)]

    norms = zero_pair
    for k in range(CHUNKS):
        with scope('w_s1'):
            wait_bytes(RB.at[0:2 * CHUNK], s1r.at[k])
        for half in range(2):
            forward(half, k).start()
        if k == 0:
            pl.when(bit_c == 1)(lambda: send_rest((0, 1)))
        else:
            for half in range(2):
                stage2(half, k - 1).start()
        with scope('w_fw'):
            wait_bytes(BIG.at[0:2 * CHUNK + (0 if k else size)], fwr[k])

        for half in range(2):
            coefs = stage1_coefs[half]
            base = (half * CHUNKS + sent(half, k)) * CHUNK

            def combine(t, carry, base=base, coefs=coefs, half=half):
                at = pl.multiple_of(base + 2 * SUB * t, 2 * SUB)
                re, im = mix(coefs, [strided(ref, at) for ref in (X, RB, XP, RP)])
                XC[tile(t), (LOW, HIGH)[half]] = re
                XC[tile(t, LANES), (LOW, HIGH)[half]] = im
                return carry

            with scope('comb'):
                lax.fori_loop(0, TILES, combine, 0, unroll=2)
        with scope('mm'):
            left = lax.dot(GM[...], XC[...], precision=lax.Precision.HIGHEST, preferred_element_type=F32)
            for rows in (LOW, HIGH):
                for cols in (LOW, HIGH):
                    ZC[cols, rows] = left[rows, cols]
            both = lax.dot(ZC[...], KM[...], precision=lax.Precision.HIGHEST, preferred_element_type=F32)
            for half in range(2):
                for part in range(2):
                    S[half, sent(half, k), part] = both[(LOW, HIGH)[half], (LOW, HIGH)[part]]

        def mid_sums(t, sums, k=k):
            dens = [norm(planes(S, half, sent(half, k), tile(t))) for half in range(2)]
            row = dens[0] + dens[1]
            TP[tile(t), :] = row if k == 0 else TP[tile(t), :] + row
            return tuple(a + b for a, b in zip(sums, dens))

        with scope('dens'):
            norms = lax.fori_loop(0, TILES, mid_sums, norms, unroll=2)

    flips = (1 - bit_y, 1 - bit_x)
    u3 = matrix(3)
    u4 = [matrix(4, flip) for flip in flips]
    u5 = [matrix(5, flip) for flip in flips]
    second_coef = (coef_y, coef_x)

    def weights(k):
        table = {}
        for half in range(2):
            index = received(half, k)
            for chunk in range(CHUNKS):
                inner = cmul(entry(4, chunk // 2, index // 2), entry(5, chunk % 2, index % 2))
                inner = cmul(second_coef[half][1], inner)
                for side in range(2):
                    table[side, chunk, half] = cmul(u3[2 * side + half], inner)
        return table

    def add_cross(k):
        def body(t, cross):
            done = []
            for half in range(2):
                chunk = received(half, k)
                part = conj_mul(planes(S, half, chunk, tile(t)), planes(R2, half, chunk, tile(t)))
                done.append(cadd(cross[half], part))
            return tuple(done)
        return body

    def step_own(t, carry):
        rows = tile(t)
        for half in range(2):
            own, other = second_coef[half]
            value = []
            for k in range(CHUNKS):
                chunk = received(half, k)
                part = cmul(own, planes(S, half, chunk, rows))
                value.append(cadd(part, cmul(other, planes(R2, half, chunk, rows))) if k < 2 else part)
            value = [v for pair in (value[:2], value[2:]) for v in gate(u5[half], *pair)]
            value = [gate(u4[half], value[k], value[k + 2]) for k in range(2)]
            for k in range(CHUNKS):
                put(T, half, received(half, k), rows, value[k % 2][k // 2])
        return carry

    def step_mix(t, carry):
        rows = tile(t)
        for chunk in range(CHUNKS):
            for half, value in enumerate(gate(u3, planes(T, 0, chunk, rows), planes(T, 1, chunk, rows))):
                put(T, half, chunk, rows, value)
        return carry

    def add_received(k, table, store):
        def body(t, carry):
            rows = tile(t)
            other = [planes(R2, half, received(half, k), rows) for half in range(2)]
            for side in range(2):
                for chunk in range(CHUNKS):
                    value = planes(T, side, chunk, rows)
                    for half in range(2):
                        value = cadd(value, cmul(table[side, chunk, half], other[half]))
                    store(side, chunk, t, value)
            return carry
        return body

    def store_partial(side, chunk, t, value):
        put(T, side, chunk, tile(t), value)

    def store_out(side, chunk, t, value):
        block = side * CHUNKS + chunk
        sign = SG[tile(t, block * ROWS), :]
        at = pl.multiple_of(block * CHUNK + 2 * SUB * t, 2 * SUB)
        for part in range(2):
            OUT[pl.ds(at + part, SUB, stride=2), :] = value[part] * sign

    tables = {k: weights(k) for k in (2, 3)}
    cross = (zero_pair, zero_pair)
    with scope('w_s2'):
        wait_bytes(R2.at[:, 0], s2r.at[0])
    with scope('x0'):
        cross = lax.fori_loop(0, TILES, add_cross(0), cross, unroll=2)
    with scope('w_s2'):
        wait_bytes(R2.at[:, 0], s2r.at[1])
    with scope('x1'):
        cross = lax.fori_loop(0, TILES, add_cross(1), cross, unroll=2)

    def signed(parts, bit):
        acc = parts[0]
        for index, part in enumerate(parts[1:], 1):
            acc = acc - part if (index >> bit) & 1 else acc + part
        return acc

    def z_part():
        return remote(V, VP, zs, zp, dev_c)

    def z_copy(chip, core):
        dev = me + (chip // 2) * step_y + (chip % 2) * step_x + core * step_c
        return remote(V, VR.at[chip], zs, zr, dev)

    def send_sum():
        with scope('w_zp'):
            wait_bytes(VP, zp)
        total = V[...] + VP[...]
        V[...] = total
        VR[0] = total

    def spread_sum():
        for chip in reversed(range(CHIPS)):
            for core in reversed(range(2)):
                if chip or core:
                    z_copy(chip, core).start()

    row_index = lax.broadcasted_iota(jnp.int32, (3 * SUB, LANES), 0)
    col_index = lax.broadcasted_iota(jnp.int32, (3 * SUB, LANES), 1)
    with scope('zsum'):
        signs = [plus_minus(bit).astype(F32) for bit in (bit_y, bit_x, bit_c)]
        norm_rows = [fold(part) for part in norms]
        tot_row = norm_rows[0] + norm_rows[1]
        rows = []
        for half, bit in enumerate(second_bit):
            weight_0, weight_1, mix_re, mix_im = pair_weights(matrix(half))
            re, im = cross[half]
            rows.append(jnp.where(bit == 1, weight_1, weight_0) * norm_rows[half] + mix_re * fold(re)
                        + (mix_im * signs[half]) * fold(im) + signs[half] * norm_rows[1 - half])
        rows += [signs[2] * tot_row] + raw_rows
        parts = [TP[tile(t), :] for t in range(TILES)]
        rows += [fold(signed(parts, bit)) for bit in reversed(range(4))]
        total = norms[0] + norms[1]
        rows += [fold(total * plus_minus((sub >> bit) & 1).astype(F32)) for bit in reversed(range(3))]
        rows += [tot_row * plus_minus((lane[:1] >> bit) & 1).astype(F32) for bit in reversed(range(7))]
        rows += [jnp.zeros_like(tot_row)] * 4
        column = jnp.sum(jnp.concatenate(rows, axis=0), axis=1, keepdims=True)
        mine = jnp.sum(jnp.where(row_index == col_index, column, 0.0), axis=0, keepdims=True)
        V[...] = mine
    pl.when(bit_c == 1)(send_sum)
    pl.when(bit_c == 0)(lambda: z_part().start())
    pl.when(bit_c == 1)(spread_sum)
    for piece in range(len(PIECES) - 1):
        for half in range(2):
            stage2(half, 3, piece).start()
    with scope('own'):
        lax.fori_loop(0, TILES, step_own, 0)
        lax.fori_loop(0, TILES, step_mix, 0)
    with scope('w_s2'):
        wait_bytes(R2.at[:, 0], s2r.at[2])
    with scope('st2'):
        lax.fori_loop(0, TILES, add_received(2, tables[2], store_partial), 0)

    for piece in range(len(PIECES) - 1):
        low, high = PIECES[piece], PIECES[piece + 1]
        with scope('w_s2'):
            wait_bytes(R2.at[:, 0, :, low:high], piece_sems[piece])
        with scope('tail'):
            lax.fori_loop(low // SUB, high // SUB, add_received(3, tables[3], store_out), 0, unroll=2)
        if piece == len(PIECES) - 3:
            with scope('w_z'):
                pl.when(bit_c == 0)(lambda: wait_bytes(VR, zr))
                pl.when(bit_c == 1)(lambda: wait_bytes(VR.at[1:CHIPS], zr))
            acc = VR[0]
            for chip in range(1, CHIPS):
                acc = acc + VR[chip]
            z_ref[...] = acc[:, :QUBITS] / 2 ** QUBITS

    with scope('w_send'):
        wait_bytes(BIG, sent_sem)
        pl.when(bit_c == 0)(lambda: wait_bytes(VP, zs))
        pl.when(bit_c == 1)(lambda: wait_bytes(V7, zs))


def writer(state_ref, z_ref, state_out, z_out, sems):
    size = state_ref.shape[0] // OUT_PARTS
    for part in range(OUT_PARTS):
        rows = pl.ds(part * size, size)
        pltpu.make_async_copy(state_ref.at[rows], state_out.at[rows], sems.at[0]).start(priority=part % 2)
    copy = pltpu.make_async_copy(z_ref, z_out, sems.at[1])
    copy.start()
    pltpu.make_async_copy(state_ref, state_out, sems.at[0]).wait()
    copy.wait()


def solution(mesh):
    def local_layer(state_local, unitaries, cz_pairs):
        size = state_local.shape[1]
        rows = 2 * size // LANES
        x = state_local.reshape(2, -1, LANES).swapaxes(0, 1).reshape(rows, LANES)
        u = unitaries.transpose(0, 2, 3, 1).reshape(SUB, QUBITS)
        cz = cz_pairs.T
        x, u, cz = [pltpu.with_memory_space_constraint(v, pltpu.HBM) for v in (x, u, cz)]
        vm = pltpu.VMEM
        dma = pltpu.SemaphoreType.DMA
        halves = vm((2, CHUNKS, 2, ROWS, LANES), F32)
        square = vm((2 * LANES, 2 * LANES), F32)
        any_spec = pl.BlockSpec(memory_space=pl.ANY)
        shapes = (jax.ShapeDtypeStruct((rows, LANES), F32), jax.ShapeDtypeStruct((1, QUBITS), F32))
        out, z = pl.pallas_call(
            kernel,
            out_shape=shapes,
            in_specs=[pl.BlockSpec(memory_space=pltpu.HBM)] * 3,
            out_specs=(pl.BlockSpec(memory_space=pltpu.VMEM), pl.BlockSpec(memory_space=pltpu.VMEM)),
            scratch_shapes=[
                vm((4 * rows, LANES), F32), pltpu.SMEM(u.shape, F32), pltpu.SMEM(cz.shape, jnp.int32), halves, halves, halves,
                vm((rows // 2, LANES), F32), square, square, square, square, vm((ROWS, LANES), F32),
                vm((1, LANES), F32), vm((1, LANES), F32), vm((CHIPS, 1, LANES), F32), vm((2 * CHIPS - 1, 1, LANES), F32),
                dma((3,)), dma, dma((4,)), dma, dma((3,)), pltpu.SemaphoreType.REGULAR,
            ],
            compiler_params=pltpu.CompilerParams(collective_id=0, has_side_effects=True, vmem_limit_bytes=40 * 2 ** 20),
        )(x, u, cz)
        out, z = pl.pallas_call(
            writer, out_shape=shapes, in_specs=[any_spec] * 2, out_specs=(any_spec,) * 2, scratch_shapes=[dma((2,))],
            compiler_params=pltpu.CompilerParams(vmem_limit_bytes=2 ** 20),
        )(out, z)
        state = out.reshape(-1, 2, LANES).swapaxes(0, 1).reshape(2, size)
        return state, z.reshape(QUBITS)

    return jax.shard_map(local_layer, mesh=mesh, in_specs=(P(None, 'q'), P(), P()), out_specs=(P(None, 'q'), P()), check_vma=False)
```

```python
import jax
import jax.numpy as jnp
from jax import lax
from jax.experimental import pallas as pl
from jax.experimental.pallas import tpu as pltpu
from jax.sharding import PartitionSpec as P

MESH = pl.DeviceIdType.MESH
F32 = jnp.float32
LANES = 128
SUB = 8
TILES = 16
LOW, HIGH = slice(0, LANES), slice(LANES, 2 * LANES)
ROWS = SUB * TILES
CHUNK = 2 * ROWS
CHUNKS = 4
PIECES = (0, 56, 104, 120, 128)
FIRST = 3 * CHUNK // 16
DEVICES = 8
CHIPS = 4
OUT_PARTS = 32
QUBITS = 20
scope = jax.named_scope


def cmul(a, b):
    (a_re, a_im), (b_re, b_im) = a, b
    return a_re * b_re - a_im * b_im, a_re * b_im + a_im * b_re


def cadd(a, b):
    (a_re, a_im), (b_re, b_im) = a, b
    return a_re + b_re, a_im + b_im


def conj_mul(a, b):
    (a_re, a_im), (b_re, b_im) = a, b
    return a_re * b_re + a_im * b_im, a_re * b_im - a_im * b_re


def mix(coefs, values):
    total = None
    for coef, value in zip(coefs, values):
        part = cmul(coef, value)
        total = part if total is None else cadd(total, part)
    return total


def gate(mat, zero, one):
    u00, u01, u10, u11 = mat
    return mix((u00, u01), (zero, one)), mix((u10, u11), (zero, one))


def norm(a):
    re, im = a
    return re * re + im * im


def plus_minus(bit):
    return 1 - 2 * bit


def planes(ref, half, chunk, rows):
    return [ref[half, chunk, part, rows, :] for part in range(2)]


def put(ref, half, chunk, rows, value):
    for part in range(2):
        ref[half, chunk, part, rows, :] = value[part]


def tile(t, first=0):
    return pl.ds(pl.multiple_of(first + SUB * t, SUB), SUB)


def kernel(x_hbm, u_hbm, cz_hbm, OUT, z_ref,
           BIG, u_ref, cz_ref, S, R2, T, SG, GM, KM, XC, ZC, TP, V, VP, VR, V7,
           ld, sent_sem, s1r, fw, s2r, ready):
    zr, zs, zp = ld.at[2], ld.at[1], s1r.at[3]
    fwr = [fw, ld.at[0], ld.at[1], fw]
    piece_sems = [s1r.at[0], s1r.at[1], s1r.at[2], ld.at[0]]
    size = BIG.shape[0] // 4
    X, RB, XP, RP = [BIG.at[pl.ds(part * size, size)] for part in range(4)]
    me = lax.axis_index('q')
    bit_y = me // 4
    bit_x = (me // 2) % 2
    bit_c = me % 2
    step_y, step_x, step_c = 4 * plus_minus(bit_y), 2 * plus_minus(bit_x), plus_minus(bit_c)
    dev_y, dev_x, dev_c = me + step_y, me + step_x, me + step_c
    first_dev = (dev_x, dev_y)
    second_dev = (dev_y, dev_x)
    second_bit = (bit_y, bit_x)

    def sent(half, k):
        return k + second_bit[half] * (3 - 2 * k)

    def received(half, k):
        return 3 - k + second_bit[half] * (2 * k - 3)

    def block_rows(half, chunk):
        return pl.ds(pl.multiple_of((half * CHUNKS + chunk) * CHUNK, CHUNK), CHUNK)

    def remote(src, dst, send, recv, dev):
        return pltpu.make_async_remote_copy(src_ref=src, dst_ref=dst, send_sem=send, recv_sem=recv,
                                            device_id=(dev,), device_id_type=MESH)

    def wait_bytes(ref, sem):
        pltpu.make_async_copy(ref, ref, sem).wait()

    def part_rows(half, k, part):
        low, size = ((0, FIRST), (FIRST, CHUNK - FIRST))[part] if k == 0 else (0, CHUNK)
        return pl.ds(pl.multiple_of((half * CHUNKS + sent(half, k)) * CHUNK + low, SUB), size)

    def load_copy(half, k, part=0):
        rows = part_rows(half, k, part)
        return pltpu.make_async_copy(x_hbm.at[rows], X.at[rows], ld.at[min(2, k + 1) if k else part])

    def stage1(half, k, part=0):
        rows = part_rows(half, k, part)
        return remote(X.at[rows], RB.at[rows], sent_sem, s1r.at[k], first_dev[half])

    def core_copy(half, k):
        rows = block_rows(half, sent(half, k))
        return remote(X.at[rows], XP.at[rows], sent_sem, fw, dev_c)

    def forward(half, k):
        rows = block_rows(half, sent(half, k))
        return remote(RB.at[rows], RP.at[rows], sent_sem, fwr[k], dev_c)

    def stage2(half, k, piece=None):
        chunk = sent(half, k)
        if piece is None:
            return remote(S.at[half, chunk], R2.at[half, chunk], sent_sem, s2r.at[k], second_dev[half])
        rows = pl.ds(PIECES[piece], PIECES[piece + 1] - PIECES[piece])
        return remote(S.at[half, chunk, :, rows], R2.at[half, chunk, :, rows], sent_sem, piece_sems[piece], second_dev[half])

    u_copy = pltpu.make_async_copy(u_hbm, u_ref, s2r.at[0])
    cz_copy = pltpu.make_async_copy(cz_hbm, cz_ref, s2r.at[1])
    order = [(k, part) for k in range(CHUNKS) for part in range(1 if k else 2)]
    for k, part in order:
        for half in range(2):
            load_copy(half, k, part).start()

    last_chip = bit_y * bit_x
    beside = bit_y + bit_x - 2 * last_chip
    barrier = pltpu.get_barrier_semaphore()

    def signal(sem, devices):
        for dev in devices:
            pl.semaphore_signal(sem, inc=1, device_id=(dev,), device_id_type=MESH)

    signal(barrier, (dev_c,))
    pl.when(last_chip == 0)(lambda: signal(barrier, (dev_x, dev_y)))
    u_copy.start()
    cz_copy.start()

    waits = {(0, 0): (0, 2 * FIRST), (0, 1): (1, 2 * (CHUNK - FIRST)), (1, 0): (2, 6 * CHUNK)}

    def send_first(halves, wait):
        for k, part in order:
            if wait and (k, part) in waits:
                index, size = waits[k, part]
                wait_bytes(X.at[:size], ld.at[index])
                if k:
                    u_copy.wait()
                    cz_copy.wait()
            if k == 0:
                for half in halves:
                    stage1(half, k, part).start()
        pl.when(bit_c == 0)(lambda: send_rest(halves))

    def send_rest(halves):
        for k in range(1, CHUNKS):
            for half in halves:
                stage1(half, k).start()

    def send_beside(half):
        send_first((half,), True)
        with scope('w_rdy'):
            pl.semaphore_wait(ready, 1)
        send_first((1 - half,), False)

    with scope('bar'):
        pl.when(beside == 1)(lambda: pl.semaphore_wait(barrier, 2))
        pl.when(beside == 0)(lambda: pl.semaphore_wait(barrier, 3))
    pl.when(last_chip == 1)(lambda: signal(ready, (dev_x, dev_y)))
    with scope('first'):
        pl.when(beside == 0)(lambda: send_first((0, 1), True))
        pl.when(beside * bit_x == 1)(lambda: send_beside(0))
        pl.when(beside * bit_y == 1)(lambda: send_beside(1))
    for k in range(CHUNKS):
        for half in range(2):
            core_copy(half, k).start()

    def entry(qubit, row, col):
        return u_ref[row * 2 + col, qubit], u_ref[4 + row * 2 + col, qubit]

    def matrix(qubit, flip=0):
        return [entry(qubit, row + flip * plus_minus(row), col + flip * plus_minus(col)) for row in range(2) for col in range(2)]

    lane = lax.broadcasted_iota(jnp.int32, (SUB, LANES), 1)
    sub = lax.broadcasted_iota(jnp.int32, (SUB, LANES), 0)

    def build(t, carry):
        row = sub + SUB * t
        for base, left in ((6, True), (13, False)):
            re = im = None
            for j in range(7):
                shift = 6 - j
                row_bit = ((row >> shift) & 1) == 1
                col_bit = ((lane >> shift) & 1) == 1
                fac = []
                for ri in range(2):
                    u00, u01, u10, u11 = [u_ref[4 * ri + k, base + j] for k in range(4)]
                    if not left:
                        u01, u10 = u10, u01
                    fac.append(jnp.where(row_bit, jnp.where(col_bit, u11, u10), jnp.where(col_bit, u01, u00)))
                if re is None:
                    re, im = fac
                else:
                    re, im = cmul((re, im), fac)
            low, high = tile(t), tile(t, LANES)
            dest, upper, lower = (GM, -im, im) if left else (KM, im, -im)
            dest[low, LOW] = re
            dest[low, HIGH] = upper
            dest[high, LOW] = lower
            dest[high, HIGH] = re
        return carry

    with scope('build'):
        lax.fori_loop(0, TILES, build, 0)

    shifts = [[QUBITS - 1 - cz_ref[side, k] for side in range(2)] for k in range(QUBITS // 2)]

    def build_signs(t, carry):
        flat = (me * DEVICES * ROWS + sub + SUB * t) * LANES + lane
        parity = jnp.zeros_like(flat)
        for shift_a, shift_b in shifts:
            parity = parity ^ ((flat >> shift_a) & (flat >> shift_b))
        SG[tile(t), :] = plus_minus(parity & 1).astype(F32)
        return carry

    with scope('signs'):
        lax.fori_loop(0, DEVICES * TILES, build_signs, 0, unroll=4)

    def strided(ref, at):
        return [ref[pl.ds(at + part, SUB, stride=2), :] for part in range(2)]

    zero_tile = jnp.zeros((SUB, LANES), F32)
    zero_pair = (zero_tile, zero_tile)

    def raw_sums(t, carry):
        total, sums = carry
        value = [strided(X, pl.multiple_of(block * CHUNK + 2 * SUB * t, 2 * SUB)) for block in range(DEVICES)]
        dens = [norm(v) for v in value]
        done = []
        for (diff, cross), bit in zip(sums, (4, 2, 1)):
            for block in range(DEVICES):
                if block & bit:
                    diff = diff - dens[block]
                else:
                    diff = diff + dens[block]
                    cross = cadd(cross, conj_mul(value[block], value[block + bit]))
            done.append((diff, cross))
        for part in dens:
            total = total + part
        return total, tuple(done)

    with scope('raw'):
        raw_total, raw = lax.fori_loop(0, TILES, raw_sums, (zero_tile, ((zero_tile, zero_pair),) * 3))

    def fold(part):
        return jnp.sum(part, axis=0, keepdims=True)

    def pair_weights(mat):
        u00, u01, u10, u11 = mat
        (a_re, a_im), (b_re, b_im) = conj_mul(u00, u01), conj_mul(u10, u11)
        return norm(u00) - norm(u10), norm(u01) - norm(u11), 2 * (a_re - b_re), 2 * (b_im - a_im)

    raw_rows = []
    raw_total = fold(raw_total)
    for qubit, (diff, (re, im)) in zip((3, 4, 5), raw):
        weight_0, weight_1, mix_re, mix_im = pair_weights(matrix(qubit))
        even, odd = raw_total + fold(diff), raw_total - fold(diff)
        raw_rows.append((weight_0 * even + weight_1 * odd) / 2 + mix_re * fold(re) + mix_im * fold(im))

    def gate_pair(qubit, own_bit):
        return entry(qubit, own_bit, own_bit), entry(qubit, own_bit, 1 - own_bit)

    coef_y = gate_pair(0, bit_y)
    coef_x = gate_pair(1, bit_x)
    coef_c = gate_pair(2, bit_c)
    stage1_coefs = [[cmul(top, core) for core in coef_c for top in coef] for coef in (coef_x, coef_y)]

    norms = zero_pair
    for k in range(CHUNKS):
        with scope('w_s1'):
            wait_bytes(RB.at[0:2 * CHUNK], s1r.at[k])
        if k == 0:
            pl.when(bit_c == 1)(lambda: send_rest((0, 1)))
        for half in range(2):
            forward(half, k).start()
        if k:
            for half in range(2):
                stage2(half, k - 1).start()
        with scope('w_fw'):
            wait_bytes(BIG.at[0:2 * CHUNK + (0 if k else size)], fwr[k])

        for half in range(2):
            coefs = stage1_coefs[half]
            base = (half * CHUNKS + sent(half, k)) * CHUNK

            def combine(t, carry, base=base, coefs=coefs, half=half):
                at = pl.multiple_of(base + 2 * SUB * t, 2 * SUB)
                re, im = mix(coefs, [strided(ref, at) for ref in (X, RB, XP, RP)])
                XC[tile(t), (LOW, HIGH)[half]] = re
                XC[tile(t, LANES), (LOW, HIGH)[half]] = im
                return carry

            with scope('comb'):
                lax.fori_loop(0, TILES, combine, 0, unroll=2)
        with scope('mm'):
            left = lax.dot(GM[...], XC[...], precision=lax.Precision.HIGHEST, preferred_element_type=F32)
            for rows in (LOW, HIGH):
                for cols in (LOW, HIGH):
                    ZC[cols, rows] = left[rows, cols]
            both = lax.dot(ZC[...], KM[...], precision=lax.Precision.HIGHEST, preferred_element_type=F32)
            for half in range(2):
                for part in range(2):
                    S[half, sent(half, k), part] = both[(LOW, HIGH)[half], (LOW, HIGH)[part]]

        def mid_sums(t, sums, k=k):
            dens = [norm(planes(S, half, sent(half, k), tile(t))) for half in range(2)]
            row = dens[0] + dens[1]
            TP[tile(t), :] = row if k == 0 else TP[tile(t), :] + row
            return tuple(a + b for a, b in zip(sums, dens))

        with scope('dens'):
            norms = lax.fori_loop(0, TILES, mid_sums, norms, unroll=2)

    flips = (1 - bit_y, 1 - bit_x)
    u3 = matrix(3)
    u4 = [matrix(4, flip) for flip in flips]
    u5 = [matrix(5, flip) for flip in flips]
    second_coef = (coef_y, coef_x)

    def weights(k):
        table = {}
        for half in range(2):
            index = received(half, k)
            for chunk in range(CHUNKS):
                inner = cmul(entry(4, chunk // 2, index // 2), entry(5, chunk % 2, index % 2))
                inner = cmul(second_coef[half][1], inner)
                for side in range(2):
                    table[side, chunk, half] = cmul(u3[2 * side + half], inner)
        return table

    def add_cross(k):
        def body(t, cross):
            done = []
            for half in range(2):
                chunk = received(half, k)
                part = conj_mul(planes(S, half, chunk, tile(t)), planes(R2, half, chunk, tile(t)))
                done.append(cadd(cross[half], part))
            return tuple(done)
        return body

    def step_own(t, carry):
        rows = tile(t)
        for half in range(2):
            own, other = second_coef[half]
            value = []
            for k in range(CHUNKS):
                chunk = received(half, k)
                part = cmul(own, planes(S, half, chunk, rows))
                value.append(cadd(part, cmul(other, planes(R2, half, chunk, rows))) if k < 2 else part)
            value = [v for pair in (value[:2], value[2:]) for v in gate(u5[half], *pair)]
            value = [gate(u4[half], value[k], value[k + 2]) for k in range(2)]
            for k in range(CHUNKS):
                put(T, half, received(half, k), rows, value[k % 2][k // 2])
        return carry

    def step_mix(t, carry):
        rows = tile(t)
        for chunk in range(CHUNKS):
            for half, value in enumerate(gate(u3, planes(T, 0, chunk, rows), planes(T, 1, chunk, rows))):
                put(T, half, chunk, rows, value)
        return carry

    def add_received(k, table, store):
        def body(t, carry):
            rows = tile(t)
            other = [planes(R2, half, received(half, k), rows) for half in range(2)]
            for side in range(2):
                for chunk in range(CHUNKS):
                    value = planes(T, side, chunk, rows)
                    for half in range(2):
                        value = cadd(value, cmul(table[side, chunk, half], other[half]))
                    store(side, chunk, t, value)
            return carry
        return body

    def store_partial(side, chunk, t, value):
        put(T, side, chunk, tile(t), value)

    def store_out(side, chunk, t, value):
        block = side * CHUNKS + chunk
        sign = SG[tile(t, block * ROWS), :]
        at = pl.multiple_of(block * CHUNK + 2 * SUB * t, 2 * SUB)
        for part in range(2):
            OUT[pl.ds(at + part, SUB, stride=2), :] = value[part] * sign

    tables = {k: weights(k) for k in (2, 3)}
    cross = (zero_pair, zero_pair)
    with scope('w_s2'):
        wait_bytes(R2.at[:, 0], s2r.at[0])
    with scope('x0'):
        cross = lax.fori_loop(0, TILES, add_cross(0), cross, unroll=2)
    with scope('w_s2'):
        wait_bytes(R2.at[:, 0], s2r.at[1])
    with scope('x1'):
        cross = lax.fori_loop(0, TILES, add_cross(1), cross, unroll=2)

    def signed(parts, bit):
        acc = parts[0]
        for index, part in enumerate(parts[1:], 1):
            acc = acc - part if (index >> bit) & 1 else acc + part
        return acc

    def z_part():
        return remote(V, VP, zs, zp, dev_c)

    def z_copy(chip, core):
        dev = me + (chip // 2) * step_y + (chip % 2) * step_x + core * step_c
        return remote(V, VR.at[chip], zs, zr, dev)

    def send_sum():
        with scope('w_zp'):
            wait_bytes(VP, zp)
        total = V[...] + VP[...]
        V[...] = total
        VR[0] = total

    def spread_sum():
        for chip in reversed(range(CHIPS)):
            for core in reversed(range(2)):
                if chip or core:
                    z_copy(chip, core).start()

    row_index = lax.broadcasted_iota(jnp.int32, (3 * SUB, LANES), 0)
    col_index = lax.broadcasted_iota(jnp.int32, (3 * SUB, LANES), 1)
    with scope('zsum'):
        signs = [plus_minus(bit).astype(F32) for bit in (bit_y, bit_x, bit_c)]
        norm_rows = [fold(part) for part in norms]
        tot_row = norm_rows[0] + norm_rows[1]
        rows = []
        for half, bit in enumerate(second_bit):
            weight_0, weight_1, mix_re, mix_im = pair_weights(matrix(half))
            re, im = cross[half]
            rows.append(jnp.where(bit == 1, weight_1, weight_0) * norm_rows[half] + mix_re * fold(re)
                        + (mix_im * signs[half]) * fold(im) + signs[half] * norm_rows[1 - half])
        rows += [signs[2] * tot_row] + raw_rows
        parts = [TP[tile(t), :] for t in range(TILES)]
        rows += [fold(signed(parts, bit)) for bit in reversed(range(4))]
        total = norms[0] + norms[1]
        rows += [fold(total * plus_minus((sub >> bit) & 1).astype(F32)) for bit in reversed(range(3))]
        rows += [tot_row * plus_minus((lane[:1] >> bit) & 1).astype(F32) for bit in reversed(range(7))]
        rows += [jnp.zeros_like(tot_row)] * 4
        column = jnp.sum(jnp.concatenate(rows, axis=0), axis=1, keepdims=True)
        mine = jnp.sum(jnp.where(row_index == col_index, column, 0.0), axis=0, keepdims=True)
        V[...] = mine
    pl.when(bit_c == 1)(send_sum)
    pl.when(bit_c == 0)(lambda: z_part().start())
    pl.when(bit_c == 1)(spread_sum)
    for piece in range(len(PIECES) - 1):
        for half in range(2):
            stage2(half, 3, piece).start()
    with scope('own'):
        lax.fori_loop(0, TILES, step_own, 0)
        lax.fori_loop(0, TILES, step_mix, 0)
    with scope('w_s2'):
        wait_bytes(R2.at[:, 0], s2r.at[2])
    with scope('st2'):
        lax.fori_loop(0, TILES, add_received(2, tables[2], store_partial), 0)

    for piece in range(len(PIECES) - 1):
        low, high = PIECES[piece], PIECES[piece + 1]
        with scope('w_s2'):
            wait_bytes(R2.at[:, 0, :, low:high], piece_sems[piece])
        with scope('tail'):
            lax.fori_loop(low // SUB, high // SUB, add_received(3, tables[3], store_out), 0, unroll=2)
        if piece == len(PIECES) - 3:
            with scope('w_z'):
                pl.when(bit_c == 0)(lambda: wait_bytes(VR, zr))
                pl.when(bit_c == 1)(lambda: wait_bytes(VR.at[1:CHIPS], zr))
            acc = VR[0]
            for chip in range(1, CHIPS):
                acc = acc + VR[chip]
            z_ref[...] = acc[:, :QUBITS] / 2 ** QUBITS

    with scope('w_send'):
        wait_bytes(BIG, sent_sem)
        pl.when(bit_c == 0)(lambda: wait_bytes(VP, zs))
        pl.when(bit_c == 1)(lambda: wait_bytes(V7, zs))


def writer(state_ref, z_ref, state_out, z_out, sems):
    size = state_ref.shape[0] // OUT_PARTS
    for part in range(OUT_PARTS):
        rows = pl.ds(part * size, size)
        pltpu.make_async_copy(state_ref.at[rows], state_out.at[rows], sems.at[0]).start(priority=part % 2)
    copy = pltpu.make_async_copy(z_ref, z_out, sems.at[1])
    copy.start()
    pltpu.make_async_copy(state_ref, state_out, sems.at[0]).wait()
    copy.wait()


def solution(mesh):
    def local_layer(state_local, unitaries, cz_pairs):
        size = state_local.shape[1]
        rows = 2 * size // LANES
        x = state_local.reshape(2, -1, LANES).swapaxes(0, 1).reshape(rows, LANES)
        u = unitaries.transpose(0, 2, 3, 1).reshape(SUB, QUBITS)
        cz = cz_pairs.T
        x, u, cz = [pltpu.with_memory_space_constraint(v, pltpu.HBM) for v in (x, u, cz)]
        vm = pltpu.VMEM
        dma = pltpu.SemaphoreType.DMA
        halves = vm((2, CHUNKS, 2, ROWS, LANES), F32)
        square = vm((2 * LANES, 2 * LANES), F32)
        any_spec = pl.BlockSpec(memory_space=pl.ANY)
        shapes = (jax.ShapeDtypeStruct((rows, LANES), F32), jax.ShapeDtypeStruct((1, QUBITS), F32))
        out, z = pl.pallas_call(
            kernel,
            out_shape=shapes,
            in_specs=[pl.BlockSpec(memory_space=pltpu.HBM)] * 3,
            out_specs=(pl.BlockSpec(memory_space=pltpu.VMEM), pl.BlockSpec(memory_space=pltpu.VMEM)),
            scratch_shapes=[
                vm((4 * rows, LANES), F32), pltpu.SMEM(u.shape, F32), pltpu.SMEM(cz.shape, jnp.int32), halves, halves, halves,
                vm((rows // 2, LANES), F32), square, square, square, square, vm((ROWS, LANES), F32),
                vm((1, LANES), F32), vm((1, LANES), F32), vm((CHIPS, 1, LANES), F32), vm((2 * CHIPS - 1, 1, LANES), F32),
                dma((3,)), dma, dma((4,)), dma, dma((3,)), pltpu.SemaphoreType.REGULAR,
            ],
            compiler_params=pltpu.CompilerParams(collective_id=0, has_side_effects=True, vmem_limit_bytes=40 * 2 ** 20),
        )(x, u, cz)
        out, z = pl.pallas_call(
            writer, out_shape=shapes, in_specs=[any_spec] * 2, out_specs=(any_spec,) * 2, scratch_shapes=[dma((2,))],
            compiler_params=pltpu.CompilerParams(vmem_limit_bytes=2 ** 20),
        )(out, z)
        state = out.reshape(-1, 2, LANES).swapaxes(0, 1).reshape(2, size)
        return state, z.reshape(QUBITS)

    return jax.shard_map(local_layer, mesh=mesh, in_specs=(P(None, 'q'), P(), P()), out_specs=(P(None, 'q'), P()), check_vma=False)
```
